32 devices in a mesh: dom: 8 (over z, x), feat: 4 (over y, core).
Axes of the slice: x: 2, y: 2, z: 4, core: 2. Of those that a mesh axis runs over, the one named last changes fastest.
Arguments:
- feats: bfloat16 [256, 4096], P('feat', 'dom'), may hold values from -6 to 6
- self_weight: bfloat16 [256, 256], P(None, 'feat'), may hold values from -0.375 to 0.375
- bases: bfloat16 [30, 256, 256], P(None, 'feat'), may hold values from -0.375 to 0.375
- coef: float32 [237, 30], replicated, may hold values from -1.2 to 1.2
- src_part: int32 [8192, 1], P('dom'), may hold values from 0 to 7; in each aligned block of 1024 rows (0 to 1023, 1024 to 2047, ...) at most 256 rows name the same one
- src_row: int32 [8192], P('dom'), may hold values from 0 to 511
- edge_dst: int32 [8192], P('dom'), may hold values from 0 to 511
- edge_rel: int32 [8192], P('dom'), may hold values from 0 to 236
- block_owner: int32 [64, 1], P('dom'), may hold values from 0 to 7; in each aligned block of 8 rows (0 to 7, 8 to 15, ...) at most 2 rows name the same one
- block_valid: int32 [8, 8], P('dom'), may hold values from 1 to 128, 896 in all within a row
- cotangent: bfloat16 [256, 4096], P('feat', 'dom'), may hold values from -6 to 6
Outputs:
- output: bfloat16 [256, 4096], P('feat', 'dom')
- grad_feats: bfloat16 [256, 4096], P('feat', 'dom')
- grad_bases: float32 [30, 256, 256], P(None, 'feat')
- grad_self: float32 [256, 256], P(None, 'feat')
- grad_coef: float32 [237, 30], replicated
The draws below stay inside these ranges and needn't reach their ends.
Inputs may be any that keep to these rules, and one draw needn't show every extreme that they name: `src_part`: among the edge rows of one index of dom, no partition is the source partition of more than 256 rows, and some partition of exactly 256. `block_owner`: among the blocks of one index of dom, no partition owns more than 2, a bound that some block reaches. `block_valid`: the valid rows of a block come first; the counts of one index of dom sum to 896.
All inputs are finite; a program needn't handle non-finite values.
Results may differ from the reference program's by a relative error of at most 0.0055.
Values may be sent and summed in bfloat16 or wider, within the bound.
No kernel may reach another device: no remote copies, remote signals or barrier semaphores. Data moves between devices by JAX's collectives and lax.ppermute only.
A program may use at most 64 MiB of HBM per device.

```python
import math
import jax
import jax.numpy as jnp
import numpy as np
from jax import lax

D = 256
BASES = 30
RELS = 237
ROWS = 128
ENT_DEV = 512
NB = 8
EDGE_DEV = 1024
ENTITIES = 4096
EDGES = 8192
BLOCKS = 64
SCAP = 256
BCAP = 2
VALID_DEV = 896
N_DOM = 8


def set_ends(result, own_key, smallest, top_value):
    longest = result.shape.index(max(result.shape))
    spots = []
    for shift in (0, 1):
        where = [jax.random.randint(jax.random.fold_in(own_key, axis), (), 0, length) for axis, length in enumerate(result.shape)]
        where[longest] = (where[longest] + shift) % result.shape[longest]
        spots.append(tuple(where))
    return result.at[spots[0]].set(smallest).at[spots[1]].set(top_value)


def shard_levels(own_key, extent, pieces, least, high):
    factor_of = 1.0
    for position, shards_of in pieces:
        steps = jax.random.uniform(jax.random.fold_in(jax.random.fold_in(own_key, 6), position), (shards_of,), jnp.float32, least / len(pieces), high / len(pieces))
        factor_of = factor_of * jnp.repeat(jnp.exp(steps), extent[position] // shards_of).reshape((-1,) + (1,) * (len(extent) - 1 - position))
    return factor_of


def rank_bounds(amount, lean):
    loads = [(1 << 20) // math.isqrt(rank ** lean) + 1 for rank in range(1, amount + 1)]
    scale = 1 + sum(loads) // (1 << 30)
    return np.cumsum(np.array([max(1, weight // scale) for weight in loads]))


def skewed_ids(rng, extent, number_of, skew):
    grid = rank_bounds(number_of, skew)
    lot = jax.random.randint(jax.random.fold_in(rng, 1), extent, 0, int(grid[number_of - 1]))
    grade = jnp.searchsorted(jnp.asarray(grid, jnp.int32), lot, side="right")
    return jax.random.permutation(jax.random.fold_in(rng, 2), number_of)[grade].astype(jnp.int32)


def length_profile(amount, total, most, skew):
    loads = [(1 << 20) // math.isqrt(grade ** skew) + 1 for grade in range(2, amount + 1)]
    rest, given = total - most - (amount - 1), [1] * (amount - 1)
    while rest > 0:
        movable = [i for i in range(amount - 1) if given[i] < most]
        whole, remaining = sum([loads[i] for i in movable]), rest
        for i in movable:
            addition = min(most - given[i], max(1, remaining * loads[i] // whole), rest)
            given[i] = given[i] + addition
            rest = rest - addition
    return np.array([most] + given)


def uneven_parts(own_key, count, total, bound, slope):
    if count == 2:
        one = jax.random.randint(own_key, (), max(1, total - bound), min(bound, total - 1) + 1)
        return jnp.stack([one, total - one])
    sizes = jnp.asarray(length_profile(count, total, bound, slope), jnp.int32)
    couples = (count - 1) // 2
    source_of, sink = sizes[1:1 + 2 * couples:2], sizes[2:2 + 2 * couples:2]
    margin = jnp.minimum(source_of - 1, bound - sink)
    shifted = jax.random.randint(jax.random.fold_in(own_key, 1), (couples,), 0, 1 << 20) % (margin + 1)
    sizes = sizes.at[1:1 + 2 * couples:2].set(source_of - shifted).at[2:2 + 2 * couples:2].set(sink + shifted)
    return sizes[jax.random.permutation(jax.random.fold_in(own_key, 2), count)]


def deal_out(own_key, own, number, rows, number_of, top, limit, slope):
    order = jax.random.permutation(own_key, number_of)
    packed, ordinary = load_shares(number_of, rows * top, limit, slope, True), load_shares(number_of, rows * top, limit, slope, False)
    places = jnp.arange(number_of)

    def named(tallies, rotation):
        used = int((tallies > 0).sum())
        fixed = max(1, used // 4)
        moved = fixed + (places - fixed + rotation * (used - fixed)) % max(1, number_of - fixed)
        return jnp.zeros((number_of,), jnp.int32).at[order[jnp.where(places < fixed, places, moved)]].set(jnp.asarray(tallies, jnp.int32))

    tallies = jnp.where(number % 4 == 0, named(packed, number // 4), named(ordinary, number - number // 4 - 1))
    mixed = jax.random.permutation(jax.random.fold_in(own, 3), number_of)
    giver, receiver = mixed[0:number_of // 2 * 2:2], mixed[1:number_of // 2 * 2:2]
    room = jnp.minimum(tallies[giver] - 1, limit - tallies[receiver]) // 2
    room = jnp.where((giver == order[0]) | (receiver == order[0]) | (tallies[receiver] == 0), 0, jnp.maximum(room, 0))
    moved = jax.random.randint(jax.random.fold_in(own, 4), (number_of // 2,), 0, 1 << 20) % (room + 1)
    tallies = tallies.at[giver].add(-moved).at[receiver].add(moved)
    labels = jnp.searchsorted(jnp.cumsum(tallies), jnp.arange(rows * top), side="right").astype(jnp.int32)
    grid = labels.reshape(top, rows).T
    grid = grid[jax.random.permutation(jax.random.fold_in(own, 1), rows)]
    rotation = jax.random.randint(jax.random.fold_in(own, 2), (rows, 1), 0, top)
    return jnp.take_along_axis(grid, (jnp.arange(top)[None, :] + rotation) % top, axis=1)


def load_shares(count, total, bound, skew, full):
    loads = [(1 << 20) // math.isqrt(standing ** skew) + 1 for standing in range(1, count + 1)]
    largest = bound if full else min(bound, max(-(-total // count), total * loads[0] // sum(loads)))
    least = 1 if total - largest >= count - 1 else 0
    given, rest = [largest] + [least] * (count - 1), total - largest - least * (count - 1)
    while rest > 0:
        free = [i for i in range(1, count) if given[i] < largest] or [i for i in range(1, count) if given[i] < bound]
        mass, remaining = sum([loads[i] for i in free]), rest
        for i in free:
            extra = min(bound - given[i], max(1, remaining * loads[i] // mass), rest)
            given[i] = given[i] + extra
            rest = rest - extra
    return np.array(given)


def normal_values(stream_key, extent, width, bound, pieces=(), held_as=jnp.bfloat16):
    array = jax.random.normal(stream_key, extent, jnp.float32) * width
    if len(pieces) > 0:
        array = shard_levels(stream_key, extent, pieces, -0.22, 0.18) * array
    return jnp.clip(array, min=-bound, max=bound).astype(held_as)


def setup_inputs(seed: int = 0) -> dict:
    key_list = jax.random.split(jax.random.key(seed), 12)
    feats = normal_values(key_list[0], (D, ENTITIES), 1.0, 6.0, ((0, 4), (1, 8)))
    self_weight = normal_values(key_list[1], (D, D), D ** -0.5, 0.375, ((1, 4),))
    bases = normal_values(key_list[2], (BASES, D, D), D ** -0.5, 0.375, ((1, 4),))
    coef = normal_values(key_list[3], (RELS, BASES), 0.2, 1.2, (), jnp.float32)
    src_part_keys = jax.random.split(jax.random.fold_in(key_list[4], 1), EDGES // EDGE_DEV)
    src_part_turns = jax.random.permutation(jax.random.fold_in(key_list[4], 3), EDGES // EDGE_DEV)
    src_part = jax.vmap(lambda own, number: deal_out(jax.random.fold_in(key_list[4], 2), own, number, EDGE_DEV, N_DOM, 1, SCAP, 2))(src_part_keys, src_part_turns).reshape((EDGES, 1))
    src_row = set_ends(jax.random.randint(key_list[5], (EDGES,), 0, ENT_DEV), jax.random.fold_in(key_list[5], 1), 0, ENT_DEV - 1).astype(jnp.int32)
    edge_dst = set_ends(jax.random.randint(key_list[6], (EDGES,), 0, ENT_DEV), jax.random.fold_in(key_list[6], 1), 0, ENT_DEV - 1).astype(jnp.int32)
    edge_rel = set_ends(skewed_ids(key_list[7], (EDGES,), RELS, 2), jax.random.fold_in(key_list[7], 3), 0, RELS - 1).astype(jnp.int32)
    block_owner_keys = jax.random.split(jax.random.fold_in(key_list[8], 1), BLOCKS // NB)
    block_owner_turns = jax.random.permutation(jax.random.fold_in(key_list[8], 3), BLOCKS // NB)
    block_owner = jax.vmap(lambda own, number: deal_out(jax.random.fold_in(key_list[8], 2), own, number, NB, N_DOM, 1, BCAP, 2))(block_owner_keys, block_owner_turns).reshape((BLOCKS, 1))
    block_valid = jax.vmap(lambda own: uneven_parts(own, NB, VALID_DEV, ROWS, 2))(jax.random.split(key_list[9], N_DOM)).reshape((N_DOM, NB)).astype(jnp.int32)
    cotangent = normal_values(key_list[10], (D, ENTITIES), 1.0, 6.0, ((0, 4), (1, 8)))
    return dict(feats=feats, self_weight=self_weight, bases=bases, coef=coef, src_part=src_part, src_row=src_row, edge_dst=edge_dst, edge_rel=edge_rel, block_owner=block_owner, block_valid=block_valid, cotangent=cotangent)


def float_dot(left, right):
    return jnp.dot(left.astype(jnp.float32), right.astype(jnp.float32), precision=lax.Precision.HIGHEST)


def reference(feats, self_weight, bases, coef, src_part, src_row, edge_dst, edge_rel, block_owner, block_valid, cotangent):
    entity_total = ENT_DEV * N_DOM
    edge_total = EDGE_DEV * N_DOM
    source_ids = (src_part[:, 0] * ENT_DEV + src_row).astype(jnp.int32)
    owners = jnp.repeat(block_owner[:, 0], ROWS)
    live_rows = (jnp.arange(ROWS, dtype=jnp.int32)[None, :] < block_valid.reshape(-1)[:, None]).reshape(-1)
    target_ids = (owners * ENT_DEV + edge_dst).astype(jnp.int32)
    live_float = live_rows.astype(jnp.float32)
    degree = jnp.zeros((entity_total,), jnp.float32).at[target_ids].add(live_float)
    inverse_degree = 1.0 / jnp.maximum(degree, 1.0)
    edge_coef = coef[edge_rel]
    bases_flat = jnp.transpose(bases, (2, 0, 1)).reshape(D, BASES * D).astype(jnp.float32)
    grouped = (source_ids.reshape(N_DOM, EDGE_DEV), target_ids.reshape(N_DOM, EDGE_DEV),
               edge_coef.reshape(N_DOM, EDGE_DEV, BASES), live_float.reshape(N_DOM, EDGE_DEV),
               edge_rel.reshape(N_DOM, EDGE_DEV))

    def basis_products(src_ids):
        source_feats = feats[:, src_ids].astype(jnp.float32)
        products = jnp.dot(source_feats.T, bases_flat, precision=lax.Precision.HIGHEST)
        return source_feats, products.reshape(-1, BASES, D)

    def forward_group(aggregate, group):
        src_ids, dst_ids, weights, live, rels = group
        source_feats, products = basis_products(src_ids)
        message = jnp.einsum("eb,ebo->eo", weights, products, precision=lax.Precision.HIGHEST)
        message = (message * live[:, None]).astype(jnp.bfloat16)
        return aggregate.at[dst_ids].add(message.astype(jnp.float32)), jnp.zeros((), jnp.float32)

    aggregate, ignored = lax.scan(forward_group, jnp.zeros((entity_total, D), jnp.float32), grouped)
    preact = float_dot(feats.T, self_weight) + inverse_degree[:, None] * aggregate
    output = jax.nn.silu(preact).astype(jnp.bfloat16)
    sigmoid_pre = jax.nn.sigmoid(preact)
    grad_pre = (cotangent.T.astype(jnp.float32) * sigmoid_pre * (1.0 + preact * (1.0 - sigmoid_pre))).astype(jnp.bfloat16)

    def backward_group(totals_now, group):
        grad_bases, grad_coef, edge_grads = totals_now
        src_ids, dst_ids, weights, live, rels = group
        source_feats, products = basis_products(src_ids)
        grad_message = inverse_degree[dst_ids][:, None] * grad_pre[dst_ids].astype(jnp.float32) * live[:, None]
        grad_message = grad_message.astype(jnp.bfloat16).astype(jnp.float32)
        scaled = jnp.einsum("ebo,eo->eb", products, grad_message, precision=lax.Precision.HIGHEST)
        grad_coef = grad_coef + jax.ops.segment_sum(scaled, rels, num_segments=RELS)
        combined = (weights[:, :, None] * grad_message[:, None, :]).astype(jnp.bfloat16).reshape(-1, BASES * D)
        grad_bases = grad_bases + float_dot(source_feats, combined)
        edge_part = float_dot(combined, bases_flat.T)
        edge_grads = edge_grads.at[src_ids].add(edge_part)
        return (grad_bases, grad_coef, edge_grads), jnp.zeros((), jnp.float32)

    start_state = (jnp.zeros((D, BASES * D), jnp.float32), jnp.zeros((RELS, BASES), jnp.float32),
                   jnp.zeros((entity_total, D), jnp.float32))
    final_state, ignored = lax.scan(backward_group, start_state, grouped)
    grad_bases, grad_coef, edge_grads = final_state
    self_part = float_dot(grad_pre, self_weight.T)
    grad_feats = (self_part + edge_grads).astype(jnp.bfloat16).T
    grad_self = float_dot(feats, grad_pre)
    scale = float(edge_total) ** -0.5
    grad_bases = jnp.transpose((grad_bases * scale).reshape(D, BASES, D), (1, 2, 0))
    return (output.T, grad_feats, grad_bases, grad_self * scale, grad_coef * scale)
```

```python
import functools

import jax
import jax.numpy as jnp
from jax import lax
from jax.experimental import pallas as pl
from jax.experimental.pallas import tpu as pltpu
from jax.sharding import PartitionSpec as P

BF = jnp.bfloat16
F32 = jnp.float32
I32 = jnp.int32
LANES = 128
NN = (((1,), (0,)), ((), ()))
NT = (((1,), (1,)), ((), ()))


def iota(shape, dim):
    return lax.broadcasted_iota(I32, shape, dim)


def hot(mask):
    return jnp.where(mask, 1.0, 0.0).astype(BF)


def dot(left, right, dims=NN):
    return lax.dot_general(left, right, dims, preferred_element_type=F32)


def call(kernel, out_shape, smem=(), scratch=(), count=0):
    specs = [
        pl.BlockSpec(memory_space=pltpu.SMEM if k in smem else pltpu.VMEM) for k in range(count)
    ]
    single = not isinstance(out_shape, (tuple, list))
    outs = pl.BlockSpec(memory_space=pltpu.VMEM)
    return pl.pallas_call(
        kernel,
        out_shape=out_shape,
        in_specs=specs,
        out_specs=outs if single else tuple(outs for _ in out_shape),
        scratch_shapes=scratch,
    )


def block_slots(owners, block_count, block_cap):
    slots = []
    for j in range(block_count):
        rank = jnp.int32(0)
        for k in range(j):
            rank = rank + jnp.where(owners[k] == owners[j], 1, 0)
        slots.append(owners[j] * block_cap + rank)
    return slots


def each(count, step):
    if count <= 8:
        for k in range(count):
            step(k)
    else:
        lax.fori_loop(0, count, lambda k, c: (step(k), c)[1], 0)


def plan_kernel(
    entities, slot_cap, block_cap, owners, valid, part, row, dst, send, slot_out, hot_scratch
):
    dom_count = send.shape[0]
    edge_count = part.shape[1]
    block_count = dst.shape[0]
    chunks = slot_cap // LANES
    before = hot(iota((LANES, LANES), 0) < iota((LANES, LANES), 1))
    ones = jnp.ones((LANES, LANES), BF)
    offset = jnp.zeros((dom_count, LANES), F32)
    for c in range(edge_count // LANES):
        lanes = slice(c * LANES, (c + 1) * LANES)
        here = part[:, lanes]
        mask = iota((dom_count, LANES), 0) == here
        chosen = hot(mask)
        rank = jnp.sum(jnp.where(mask, dot(chosen, before) + offset, 0.0), axis=0, keepdims=True)
        offset = offset + dot(chosen, ones)
        slot_out[:, lanes] = here * slot_cap + rank.astype(I32)
    rows = row[...]
    digits = jnp.concatenate(
        [
            (rows >> 8).astype(F32),
            (rows & 255).astype(F32),
            jnp.ones((1, edge_count), F32),
            jnp.zeros((13, edge_count), F32),
        ],
        axis=0,
    ).astype(BF)

    def ask(p):
        near = slot_out[...] - p * slot_cap
        hot_scratch[...] = hot(iota((slot_cap, edge_count), 0) == near)
        found = dot(digits, hot_scratch[...], NT)
        wanted = found[0:1] * 256.0 + found[1:2] + (1.0 - found[2:3]) * float(entities)
        wanted = wanted.astype(I32)
        for k in range(chunks):
            send[p, k : k + 1, :] = wanted[:, k * LANES : (k + 1) * LANES]
        for t in range(block_cap):
            send[p, chunks + t : chunks + t + 1, :] = jnp.full((1, LANES), entities, I32)

    each(dom_count, ask)
    for j in range(block_count):
        rank = jnp.int32(0)
        for k in range(j):
            rank = rank + jnp.where(owners[k] == owners[j], 1, 0)
        live = iota((1, LANES), 1) < valid[j]
        send[owners[j], pl.ds(chunks + rank, 1), :] = jnp.where(live, dst[j : j + 1, :], entities)


def asked_row(arrived, g, chunks):
    rows = [arrived[g, k : k + 1, :] for k in range(chunks)]
    return rows[0] if chunks == 1 else jnp.concatenate(rows, axis=1)


def serve_kernel(slot_cap, arrived, feats, served):
    chunks = slot_cap // LANES
    entities = feats.shape[1]

    def step(g):
        asked = asked_row(arrived, g, chunks)
        chosen = hot(iota((entities, slot_cap), 0) == asked)
        served[g] = dot(feats[...], chosen).astype(BF)

    each(served.shape[0], step)


def unslot_kernel(fetched, slot, feats, out, total):
    dom_count, quarter, slot_cap = fetched.shape
    edge_count = slot.shape[1]
    total[...] = jnp.zeros_like(total)

    def step(p):
        near = slot[...] - p * slot_cap
        chosen = hot(iota((slot_cap, edge_count), 0) == near)
        total[...] += dot(fetched[p], chosen)

    each(dom_count, step)
    out[:, :edge_count] = total[...].astype(BF)
    out[:, edge_count:] = feats[...]


def rel_hot(rel, width):
    return hot(iota((width, rel.shape[1]), 0) == rel)


def forward_kernel(block_cap, owners, gathered, bases, coef, rel, send, weights):
    slots, quarter, rows = send.shape
    edge_count = rel.shape[1]
    block_count = edge_count // rows
    basis_count = bases.shape[0] // quarter
    span = 2 * rows if block_count % 2 == 0 else rows
    group = 5
    send[...] = jnp.zeros_like(send)
    table = coef[...]
    high = table.astype(BF)
    rest = table - high.astype(F32)
    middle = rest.astype(BF)
    low = (rest - middle.astype(F32)).astype(BF)
    where = block_slots(owners, block_count, block_cap)
    for t in range(edge_count // span):
        lanes = slice(t * span, (t + 1) * span)
        chosen = rel_hot(rel[:, lanes], coef.shape[1])
        mix = dot(high, chosen) + dot(middle, chosen) + dot(low, chosen)
        weights[:, lanes] = mix
        x = gathered[:, lanes]
        total = jnp.zeros((quarter, span), F32)
        for c in range(0, basis_count, group):
            stop = min(c + group, basis_count)
            products = dot(bases[c * quarter : stop * quarter, :], x)
            for b in range(c, stop):
                part = products[(b - c) * quarter : (b - c + 1) * quarter]
                total = total + mix[b : b + 1, :] * part
        total = total.astype(BF)
        for k in range(span // rows):
            send[where[t * (span // rows) + k]] = total[:, k * rows : (k + 1) * rows]


def owner_kernel(
    slot_cap, block_cap, arrived, received, gathered, weight, cotangent, output, back, grad_pre, hots, flat
):
    slots, quarter, rows = received.shape
    entities = cotangent.shape[1]
    chunks = slot_cap // LANES
    width = slots * rows
    for s in range(slots):
        lanes = slice(s * rows, (s + 1) * rows)
        target = arrived[s // block_cap, chunks + s % block_cap : chunks + s % block_cap + 1, :]
        hots[:, lanes] = hot(iota((entities, rows), 0) == target)
        flat[:quarter, lanes] = received[s]
    flat[quarter:, :] = jnp.ones((16, width), BF)
    own = gathered[:, gathered.shape[1] - entities :]
    own_part = lax.dot_general(
        weight[...], own, (((0,), (0,)), ((), ())), preferred_element_type=F32
    )
    sums = dot(flat[...], hots[...], NT)
    inverse = 1.0 / jnp.maximum(sums[quarter : quarter + 1], 1.0)
    preact = own_part + inverse * sums[:quarter]
    gate = jax.nn.sigmoid(preact)
    output[...] = (preact * gate).astype(BF)
    pre = (cotangent[...].astype(F32) * gate * (1.0 + preact * (1.0 - gate))).astype(BF)
    grad_pre[...] = pre
    scaled = (inverse * pre.astype(F32)).astype(BF)
    for s in range(slots):
        back[s] = dot(scaled, hots[:, s * rows : (s + 1) * rows]).astype(BF)


def fill_combined(where, returned, weights, combined, basis_count):
    quarter, rows = returned.shape[1:]
    for j, slot in enumerate(where):
        lanes = slice(j * rows, (j + 1) * rows)
        grad = returned[slot].astype(F32)
        for b in range(basis_count):
            combined[b * quarter : (b + 1) * quarter, lanes] = (
                weights[b : b + 1, lanes] * grad
            ).astype(BF)


def bases_kernel(block_cap, owners, returned, gathered, weights, grad_pre, out, combined):
    quarter, rows = returned.shape[1:]
    edge_count = weights.shape[1]
    total = combined.shape[0]
    where = block_slots(owners, edge_count // rows, block_cap)
    fill_combined(where, returned, weights, combined, total // quarter)
    x = gathered[:, :edge_count]
    chunk = 5 * quarter
    for start in range(0, total, chunk):
        stop = min(start + chunk, total)
        out[start:stop, :] = dot(combined[start:stop, :], x, NT).astype(BF)
    own = gathered[:, edge_count:]
    out[total : total + quarter, :] = dot(grad_pre[...], own, NT).astype(BF)
    out[total + quarter :, :] = jnp.zeros((out.shape[0] - total - quarter, out.shape[1]), BF)


def edges_kernel(
    block_cap, owners, returned, gathered, weights, grad_pre, bases, bases_t, weight, rel, out, combined, scaled
):
    quarter, rows = returned.shape[1:]
    edge_count = weights.shape[1]
    entities = grad_pre.shape[1]
    total = combined.shape[0]
    basis_count = total // quarter
    padded = weights.shape[0]
    relations = 2 * LANES
    where = block_slots(owners, edge_count // rows, block_cap)
    fill_combined(where, returned, weights, combined, basis_count)
    peers = out.shape[0]
    share = out.shape[1]
    span = 2 * rows if (edge_count // rows) % 2 == 0 else rows
    scaled[...] = jnp.zeros_like(scaled)
    for t in range(edge_count // span):
        lanes = slice(t * span, (t + 1) * span)
        partial = dot(bases_t[...], combined[:, lanes]).astype(BF)
        for f in range(peers):
            out[f, :, lanes] = partial[f * share : (f + 1) * share]
        x = gathered[:, lanes]
        count = span // rows
        grad = [returned[where[t * count + k]].astype(F32) for k in range(count)]
        grad = grad[0] if count == 1 else jnp.concatenate(grad, axis=1)
        group = 5
        for c in range(0, basis_count, group):
            stop = min(c + group, basis_count)
            products = dot(bases[c * quarter : stop * quarter, :], x)
            for b in range(c, stop):
                part = products[(b - c) * quarter : (b - c + 1) * quarter]
                scaled[b : b + 1, lanes] = jnp.sum(part * grad, axis=0, keepdims=True)
    high = scaled[...].astype(BF)
    low = (scaled[...] - high.astype(F32)).astype(BF)
    chosen = rel_hot(rel[...], relations)
    coef = (dot(high, chosen, NT) + dot(low, chosen, NT)).astype(BF)
    own = dot(weight[...], grad_pre[...]).astype(BF)
    tail = edge_count + entities
    for f in range(peers):
        out[f, :, edge_count:tail] = own[f * share : (f + 1) * share]
        out[f, :padded, tail:] = coef[:, :LANES]
        out[f, padded : 2 * padded, tail:] = coef[:, LANES:]


def slots_kernel(padded, arrived, slot, out, own):
    peers, share, width = arrived.shape
    dom_count, height, slot_cap = out.shape
    edge_count = slot.shape[1]
    entities = own.shape[1]
    sums = arrived[0].astype(F32)
    for f in range(1, peers):
        sums = sums + arrived[f].astype(F32)
    own[...] = sums[:, edge_count : edge_count + entities]
    edges = sums[:, :edge_count].astype(BF)
    coef = sums[: 2 * padded, edge_count + entities :].astype(BF)

    def step(p):
        near = slot[...] - p * slot_cap
        chosen = hot(iota((slot_cap, edge_count), 0) == near)
        out[p, :share, :] = dot(edges, chosen, NT).astype(BF)
        if slot_cap >= 2 * LANES:
            out[p, share:, :LANES] = coef[:padded]
            out[p, share:, LANES : 2 * LANES] = coef[padded:]
        else:
            out[p, share:, :] = coef

    each(dom_count, step)


def feats_kernel(slot_cap, padded, scale, arrived, asked, own, out, coef, total):
    dom_count, height, _ = arrived.shape
    share, entities = own.shape
    chunks = slot_cap // LANES
    total[...] = own[...]
    coef[...] = jnp.zeros_like(coef)

    def step(g):
        chosen = hot(iota((entities, slot_cap), 0) == asked_row(asked, g, chunks))
        total[...] += dot(arrived[g, :share, :], chosen, NT)
        if slot_cap >= 2 * LANES:
            coef[...] += arrived[g, share:, : 2 * LANES].astype(F32)
        else:
            coef[:, :LANES] += arrived[g, share : share + padded, :].astype(F32)
            coef[:, LANES:] += arrived[g, share + padded :, :].astype(F32)

    each(dom_count, step)
    out[...] = total[...].astype(BF)
    coef[...] = coef[...] * scale


def reduce_kernel(scale, parts, out):
    sums = parts[0].astype(F32)
    for k in range(1, parts.shape[0]):
        sums = sums + parts[k].astype(F32)
    out[...] = (sums * scale).astype(BF)


def body(
    feats,
    self_weight,
    bases,
    coef,
    src_part,
    src_row,
    edge_dst,
    edge_rel,
    block_owner,
    block_valid,
    cotangent,
):
    dom_count = lax.axis_size("dom")
    feat_count = lax.axis_size("feat")
    quarter, entities = feats.shape
    edge_count = src_row.shape[0]
    block_count = block_valid.shape[1]
    rows = edge_count // block_count
    slot_cap = LANES * ((2 * edge_count + LANES * dom_count - 1) // (LANES * dom_count))
    block_cap = (2 * block_count + dom_count - 1) // dom_count
    basis_count, _, model = bases.shape
    relation_count = coef.shape[0]
    flat = basis_count * quarter
    padded = 8 * ((basis_count + 7) // 8)
    padded = 16 * ((padded + 15) // 16)
    shape = jax.ShapeDtypeStruct
    scale = float(edge_count * dom_count) ** (-0.5)

    owners = block_owner[:, 0]
    valid = block_valid[0]
    rel = edge_rel.reshape(1, edge_count)
    bases_flat = bases.reshape(flat, model)
    coef_t = jnp.zeros((padded, 2 * LANES), F32).at[:basis_count, :relation_count].set(coef.T)

    height = slot_cap // LANES + block_cap
    send, slot = call(
        functools.partial(plan_kernel, entities, slot_cap, block_cap),
        (shape((dom_count, height, LANES), I32), shape((1, edge_count), I32)),
        smem=(0, 1),
        scratch=[pltpu.VMEM((slot_cap, edge_count), BF)],
        count=5,
    )(
        owners,
        valid,
        src_part.reshape(1, edge_count),
        src_row.reshape(1, edge_count),
        edge_dst.reshape(block_count, rows),
    )
    arrived = lax.all_to_all(send, "dom", split_axis=0, concat_axis=0, tiled=True)
    served = call(
        functools.partial(serve_kernel, slot_cap),
        shape((dom_count, quarter, slot_cap), BF),
        count=2,
    )(arrived, feats)
    fetched = lax.all_to_all(served, "dom", split_axis=0, concat_axis=0, tiled=True)
    mine = call(
        unslot_kernel,
        shape((quarter, edge_count + entities), BF),
        scratch=[pltpu.VMEM((quarter, edge_count), F32)],
        count=3,
    )(fetched, slot, feats)
    gathered = lax.all_gather(mine, "feat", axis=0, tiled=True)

    messages, weights = call(
        functools.partial(forward_kernel, block_cap),
        (shape((dom_count * block_cap, quarter, rows), BF), shape((padded, edge_count), F32)),
        smem=(0,),
        count=5,
    )(owners, gathered, bases_flat, coef_t, rel)
    received = lax.all_to_all(messages, "dom", split_axis=0, concat_axis=0, tiled=True)
    total_slots = dom_count * block_cap * rows
    output, back, grad_pre = call(
        functools.partial(owner_kernel, slot_cap, block_cap),
        (
            shape((quarter, entities), BF),
            shape((dom_count * block_cap, quarter, rows), BF),
            shape((quarter, entities), BF),
        ),
        scratch=[pltpu.VMEM((entities, total_slots), BF), pltpu.VMEM((quarter + 16, total_slots), BF)],
        count=5,
    )(arrived, received, gathered, self_weight, cotangent)
    returned = lax.all_to_all(back, "dom", split_axis=0, concat_axis=0, tiled=True)

    unit = 16 * dom_count
    tall = unit * ((flat + quarter + unit - 1) // unit)
    bases_part = call(
        functools.partial(bases_kernel, block_cap),
        shape((tall, model), BF),
        smem=(0,),
        scratch=[pltpu.VMEM((flat, edge_count), BF)],
        count=5,
    )(owners, returned, gathered, weights, grad_pre)
    parts = lax.all_to_all(
        bases_part.reshape(dom_count, tall // dom_count, model),
        "dom",
        split_axis=0,
        concat_axis=0,
        tiled=True,
    )
    edge_part = call(
        functools.partial(edges_kernel, block_cap),
        shape((feat_count, quarter, edge_count + entities + LANES), BF),
        smem=(0,),
        scratch=[pltpu.VMEM((flat, edge_count), BF), pltpu.VMEM((padded, edge_count), F32)],
        count=9,
    )(owners, returned, gathered, weights, grad_pre, bases_flat, bases_flat.T, self_weight, rel)
    edge_sum = lax.all_to_all(edge_part, "feat", split_axis=0, concat_axis=0, tiled=True)
    extra = padded * 2 * LANES // min(slot_cap, 2 * LANES)
    slot_grads, own_grads = call(
        functools.partial(slots_kernel, padded),
        (shape((dom_count, quarter + extra, slot_cap), BF), shape((quarter, entities), F32)),
        count=2,
    )(edge_sum, slot)
    arrived_grads = lax.all_to_all(slot_grads, "dom", split_axis=0, concat_axis=0, tiled=True)
    reduced = call(
        functools.partial(reduce_kernel, scale), shape((tall // dom_count, model), BF), count=1
    )(parts)
    near = [[2 * k, 2 * k + 1] for k in range(dom_count // 2)]
    far = [[2 * k + side for k in range(dom_count // 2)] for side in range(2)]
    pair = lax.all_gather(reduced, "dom", axis=0, tiled=True, axis_index_groups=near)
    whole = lax.all_gather(pair, "dom", axis=0, tiled=True, axis_index_groups=far)
    grad_feats, coef_total = call(
        functools.partial(feats_kernel, slot_cap, padded, scale),
        (shape((quarter, entities), BF), shape((padded, 2 * LANES), F32)),
        scratch=[pltpu.VMEM((quarter, entities), F32)],
        count=3,
    )(arrived_grads, arrived, own_grads)
    return (
        output,
        grad_feats,
        whole[:flat].astype(F32).reshape(basis_count, quarter, model),
        whole[flat : flat + quarter].astype(F32).T,
        coef_total[:basis_count, :relation_count].T,
    )


def solution(mesh):
    return jax.shard_map(
        body,
        mesh=mesh,
        in_specs=(
            P("feat", "dom"),
            P(None, "feat"),
            P(None, "feat", None),
            P(),
            P("dom", None),
            P("dom"),
            P("dom"),
            P("dom"),
            P("dom", None),
            P("dom", None),
            P("feat", "dom"),
        ),
        out_specs=(P("feat", "dom"), P("feat", "dom"), P(None, "feat", None), P(None, "feat"), P()),
        check_vma=False,
    )
```

```python
import functools

import jax
import jax.numpy as jnp
from jax import lax
from jax.experimental import pallas as pl
from jax.experimental.pallas import tpu as pltpu
from jax.sharding import PartitionSpec as P


BF = jnp.bfloat16
F32 = jnp.float32
I32 = jnp.int32
LANES = 128
NN = (((1,), (0,)), ((), ()))
NT = (((1,), (1,)), ((), ()))


def iota(shape, dim):
    return lax.broadcasted_iota(I32, shape, dim)


def hot(mask):
    return jnp.where(mask, 1.0, 0.0).astype(BF)


def dot(left, right, dims=NN):
    return lax.dot_general(left, right, dims, preferred_element_type=F32)


def call(kernel, out_shape, smem=(), scratch=(), count=0, us=4):
    specs = [
        pl.BlockSpec(memory_space=pltpu.SMEM if k in smem else pltpu.VMEM) for k in range(count)
    ]
    single = not isinstance(out_shape, (tuple, list))
    outs = pl.BlockSpec(memory_space=pltpu.VMEM)
    return pl.pallas_call(
        kernel,
        out_shape=out_shape,
        in_specs=specs,
        out_specs=outs if single else tuple(outs for _ in out_shape),
        scratch_shapes=scratch,
        cost_estimate=pl.CostEstimate(
            flops=us * 1_000_000_000, bytes_accessed=1 << 20, transcendentals=0
        ),
    )


def block_slots(owners, block_count, block_cap):
    slots = []
    for j in range(block_count):
        rank = jnp.int32(0)
        for k in range(j):
            rank = rank + jnp.where(owners[k] == owners[j], 1, 0)
        slots.append(owners[j] * block_cap + rank)
    return slots


def each(count, step):
    if count <= 8:
        for k in range(count):
            step(k)
    else:
        lax.fori_loop(0, count, lambda k, c: (step(k), c)[1], 0)


def plan_kernel(
    entities, slot_cap, block_cap, owners, valid, part, row, dst, send, slot_out, hot_scratch
):
    dom_count = send.shape[0]
    edge_count = part.shape[1]
    block_count = dst.shape[0]
    chunks = slot_cap // LANES
    before = hot(iota((LANES, LANES), 0) < iota((LANES, LANES), 1))
    ones = jnp.ones((LANES, LANES), BF)
    offset = jnp.zeros((dom_count, LANES), F32)
    for c in range(edge_count // LANES):
        lanes = slice(c * LANES, (c + 1) * LANES)
        here = part[:, lanes]
        mask = iota((dom_count, LANES), 0) == here
        chosen = hot(mask)
        rank = jnp.sum(jnp.where(mask, dot(chosen, before) + offset, 0.0), axis=0, keepdims=True)
        offset = offset + dot(chosen, ones)
        slot_out[:, lanes] = here * slot_cap + rank.astype(I32)
    rows = row[...]
    digits = jnp.concatenate(
        [
            (rows >> 8).astype(F32),
            (rows & 255).astype(F32),
            jnp.ones((1, edge_count), F32),
            jnp.zeros((13, edge_count), F32),
        ],
        axis=0,
    ).astype(BF)

    def ask(p):
        near = slot_out[...] - p * slot_cap
        hot_scratch[...] = hot(iota((slot_cap, edge_count), 0) == near)
        found = dot(digits, hot_scratch[...], NT)
        wanted = found[0:1] * 256.0 + found[1:2] + (1.0 - found[2:3]) * float(entities)
        wanted = wanted.astype(I32)
        for k in range(chunks):
            send[p, k : k + 1, :] = wanted[:, k * LANES : (k + 1) * LANES]
        for t in range(block_cap):
            send[p, chunks + t : chunks + t + 1, :] = jnp.full((1, LANES), entities, I32)

    each(dom_count, ask)
    for j in range(block_count):
        rank = jnp.int32(0)
        for k in range(j):
            rank = rank + jnp.where(owners[k] == owners[j], 1, 0)
        live = iota((1, LANES), 1) < valid[j]
        send[owners[j], pl.ds(chunks + rank, 1), :] = jnp.where(live, dst[j : j + 1, :], entities)


def asked_row(arrived, g, chunks):
    rows = [arrived[g, k : k + 1, :] for k in range(chunks)]
    return rows[0] if chunks == 1 else jnp.concatenate(rows, axis=1)


def serve_kernel(slot_cap, arrived, feats, served):
    chunks = slot_cap // LANES
    entities = feats.shape[1]

    def step(g):
        asked = asked_row(arrived, g, chunks)
        chosen = hot(iota((entities, slot_cap), 0) == asked)
        served[g] = dot(feats[...], chosen).astype(BF)

    each(served.shape[0], step)


def unslot_kernel(fetched, slot, feats, out, total):
    dom_count, _, slot_cap = fetched.shape
    edge_count = slot.shape[1]
    total[...] = jnp.zeros_like(total)

    def step(p):
        near = slot[...] - p * slot_cap
        chosen = hot(iota((slot_cap, edge_count), 0) == near)
        total[...] += dot(fetched[p], chosen)

    each(dom_count, step)
    out[:, :edge_count] = total[...].astype(BF)
    out[:, edge_count:] = feats[...]


def rel_hot(rel, width):
    return hot(iota((width, rel.shape[1]), 0) == rel)


def forward_kernel(block_cap, owners, gathered, bases, coef, rel, send, weights):
    _, quarter, rows = send.shape
    edge_count = rel.shape[1]
    block_count = edge_count // rows
    basis_count = bases.shape[0] // quarter
    span = 2 * rows if block_count % 2 == 0 else rows
    group = 5
    send[...] = jnp.zeros_like(send)
    table = coef[...]
    high = table.astype(BF)
    rest = table - high.astype(F32)
    middle = rest.astype(BF)
    low = (rest - middle.astype(F32)).astype(BF)
    where = block_slots(owners, block_count, block_cap)
    for t in range(edge_count // span):
        lanes = slice(t * span, (t + 1) * span)
        chosen = rel_hot(rel[:, lanes], coef.shape[1])
        mix = dot(high, chosen) + dot(middle, chosen) + dot(low, chosen)
        weights[:, lanes] = mix
        x = gathered[:, lanes]
        total = jnp.zeros((quarter, span), F32)
        for c in range(0, basis_count, group):
            stop = min(c + group, basis_count)
            products = dot(bases[c * quarter : stop * quarter, :], x)
            for b in range(c, stop):
                part = products[(b - c) * quarter : (b - c + 1) * quarter]
                total = total + mix[b : b + 1, :] * part
        total = total.astype(BF)
        for k in range(span // rows):
            send[where[t * (span // rows) + k]] = total[:, k * rows : (k + 1) * rows]


def owner_kernel(
    slot_cap, block_cap, arrived, received, gathered, weight, cotangent, output, back, grad_pre, hots, flat
):
    slots, quarter, rows = received.shape
    entities = cotangent.shape[1]
    chunks = slot_cap // LANES
    width = slots * rows
    for s in range(slots):
        lanes = slice(s * rows, (s + 1) * rows)
        target = arrived[s // block_cap, chunks + s % block_cap : chunks + s % block_cap + 1, :]
        hots[:, lanes] = hot(iota((entities, rows), 0) == target)
        flat[:quarter, lanes] = received[s]
    flat[quarter:, :] = jnp.ones((16, width), BF)
    own = gathered[:, gathered.shape[1] - entities :]
    own_part = lax.dot_general(
        weight[...], own, (((0,), (0,)), ((), ())), preferred_element_type=F32
    )
    sums = dot(flat[...], hots[...], NT)
    inverse = 1.0 / jnp.maximum(sums[quarter : quarter + 1], 1.0)
    preact = own_part + inverse * sums[:quarter]
    gate = jax.nn.sigmoid(preact)
    output[...] = (preact * gate).astype(BF)
    pre = (cotangent[...].astype(F32) * gate * (1.0 + preact * (1.0 - gate))).astype(BF)
    grad_pre[...] = pre
    scaled = (inverse * pre.astype(F32)).astype(BF)
    for s in range(slots):
        back[s] = dot(scaled, hots[:, s * rows : (s + 1) * rows]).astype(BF)


def fill_combined(where, returned, weights, combined, basis_count):
    quarter, rows = returned.shape[1:]
    for j, slot in enumerate(where):
        lanes = slice(j * rows, (j + 1) * rows)
        grad = returned[slot].astype(F32)
        for b in range(basis_count):
            combined[b * quarter : (b + 1) * quarter, lanes] = (
                weights[b : b + 1, lanes] * grad
            ).astype(BF)


def bases_kernel(block_cap, owners, returned, gathered, weights, grad_pre, out, combined):
    quarter, rows = returned.shape[1:]
    edge_count = weights.shape[1]
    total = combined.shape[0]
    where = block_slots(owners, edge_count // rows, block_cap)
    fill_combined(where, returned, weights, combined, total // quarter)
    x = gathered[:, :edge_count]
    chunk = 5 * quarter
    for start in range(0, total, chunk):
        stop = min(start + chunk, total)
        out[start:stop, :] = dot(combined[start:stop, :], x, NT).astype(BF)
    own = gathered[:, edge_count:]
    out[total : total + quarter, :] = dot(grad_pre[...], own, NT).astype(BF)
    out[total + quarter :, :] = jnp.zeros((out.shape[0] - total - quarter, out.shape[1]), BF)


def edges_kernel(
    block_cap, owners, returned, gathered, weights, grad_pre, bases, bases_t, weight, rel, out, combined, scaled
):
    quarter, rows = returned.shape[1:]
    edge_count = weights.shape[1]
    entities = grad_pre.shape[1]
    total = combined.shape[0]
    basis_count = total // quarter
    padded = weights.shape[0]
    relations = 2 * LANES
    where = block_slots(owners, edge_count // rows, block_cap)
    fill_combined(where, returned, weights, combined, basis_count)
    peers = out.shape[0]
    share = out.shape[1]
    span = 2 * rows if (edge_count // rows) % 2 == 0 else rows
    scaled[...] = jnp.zeros_like(scaled)
    for t in range(edge_count // span):
        lanes = slice(t * span, (t + 1) * span)
        partial = dot(bases_t[...], combined[:, lanes]).astype(BF)
        for f in range(peers):
            out[f, :, lanes] = partial[f * share : (f + 1) * share]
        x = gathered[:, lanes]
        count = span // rows
        grad = [returned[where[t * count + k]].astype(F32) for k in range(count)]
        grad = grad[0] if count == 1 else jnp.concatenate(grad, axis=1)
        group = 5
        for c in range(0, basis_count, group):
            stop = min(c + group, basis_count)
            products = dot(bases[c * quarter : stop * quarter, :], x)
            for b in range(c, stop):
                part = products[(b - c) * quarter : (b - c + 1) * quarter]
                scaled[b : b + 1, lanes] = jnp.sum(part * grad, axis=0, keepdims=True)
    high = scaled[...].astype(BF)
    low = (scaled[...] - high.astype(F32)).astype(BF)
    chosen = rel_hot(rel[...], relations)
    coef = (dot(high, chosen, NT) + dot(low, chosen, NT)).astype(BF)
    own = dot(weight[...], grad_pre[...]).astype(BF)
    tail = edge_count + entities
    for f in range(peers):
        out[f, :, edge_count:tail] = own[f * share : (f + 1) * share]
        out[f, :padded, tail:] = coef[:, :LANES]
        out[f, padded : 2 * padded, tail:] = coef[:, LANES:]


def slots_kernel(padded, arrived, slot, out, own):
    peers, share, _ = arrived.shape
    dom_count, _, slot_cap = out.shape
    edge_count = slot.shape[1]
    entities = own.shape[1]
    sums = arrived[0].astype(F32)
    for f in range(1, peers):
        sums = sums + arrived[f].astype(F32)
    own[...] = sums[:, edge_count : edge_count + entities]
    edges = sums[:, :edge_count].astype(BF)
    coef = sums[: 2 * padded, edge_count + entities :].astype(BF)

    def step(p):
        near = slot[...] - p * slot_cap
        chosen = hot(iota((slot_cap, edge_count), 0) == near)
        out[p, :share, :] = dot(edges, chosen, NT).astype(BF)
        if slot_cap >= 2 * LANES:
            out[p, share:, :LANES] = coef[:padded]
            out[p, share:, LANES : 2 * LANES] = coef[padded:]
        else:
            out[p, share:, :] = coef

    each(dom_count, step)


def feats_kernel(slot_cap, padded, scale, arrived, asked, own, out, coef, total):
    dom_count, _, _ = arrived.shape
    share, entities = own.shape
    chunks = slot_cap // LANES
    total[...] = own[...]
    coef[...] = jnp.zeros_like(coef)

    def step(g):
        chosen = hot(iota((entities, slot_cap), 0) == asked_row(asked, g, chunks))
        total[...] += dot(arrived[g, :share, :], chosen, NT)
        if slot_cap >= 2 * LANES:
            coef[...] += arrived[g, share:, : 2 * LANES].astype(F32)
        else:
            coef[:, :LANES] += arrived[g, share : share + padded, :].astype(F32)
            coef[:, LANES:] += arrived[g, share + padded :, :].astype(F32)

    each(dom_count, step)
    out[...] = total[...].astype(BF)
    coef[...] = coef[...] * scale


def reduce_kernel(scale, parts, out):
    sums = parts[0].astype(F32)
    for k in range(1, parts.shape[0]):
        sums = sums + parts[k].astype(F32)
    out[...] = (sums * scale).astype(BF)


def body_many(
    feats,
    self_weight,
    bases,
    coef,
    src_part,
    src_row,
    edge_dst,
    edge_rel,
    block_owner,
    block_valid,
    cotangent,
):
    dom_count = lax.axis_size("dom")
    feat_count = lax.axis_size("feat")
    quarter, entities = feats.shape
    edge_count = src_row.shape[0]
    block_count = block_valid.shape[1]
    rows = edge_count // block_count
    slot_cap = LANES * ((2 * edge_count + LANES * dom_count - 1) // (LANES * dom_count))
    block_cap = (2 * block_count + dom_count - 1) // dom_count
    basis_count, _, model = bases.shape
    relation_count = coef.shape[0]
    flat = basis_count * quarter
    padded = 8 * ((basis_count + 7) // 8)
    padded = 16 * ((padded + 15) // 16)
    shape = jax.ShapeDtypeStruct
    scale = float(edge_count * dom_count) ** (-0.5)

    owners = block_owner[:, 0]
    valid = block_valid[0]
    rel = edge_rel.reshape(1, edge_count)
    bases_flat = bases.reshape(flat, model)
    coef_t = jnp.zeros((padded, 2 * LANES), F32).at[:basis_count, :relation_count].set(coef.T)

    height = slot_cap // LANES + block_cap
    send, slot = call(
        functools.partial(plan_kernel, entities, slot_cap, block_cap),
        (shape((dom_count, height, LANES), I32), shape((1, edge_count), I32)),
        smem=(0, 1),
        scratch=[pltpu.VMEM((slot_cap, edge_count), BF)],
        count=5,
    )(
        owners,
        valid,
        src_part.reshape(1, edge_count),
        src_row.reshape(1, edge_count),
        edge_dst.reshape(block_count, rows),
    )
    arrived = lax.all_to_all(send, "dom", split_axis=0, concat_axis=0, tiled=True)
    served = call(
        functools.partial(serve_kernel, slot_cap),
        shape((dom_count, quarter, slot_cap), BF),
        count=2,
    )(arrived, feats)
    fetched = lax.all_to_all(served, "dom", split_axis=0, concat_axis=0, tiled=True)
    mine = call(
        unslot_kernel,
        shape((quarter, edge_count + entities), BF),
        scratch=[pltpu.VMEM((quarter, edge_count), F32)],
        count=3,
    )(fetched, slot, feats)
    gathered = lax.all_gather(mine, "feat", axis=0, tiled=True)

    messages, weights = call(
        functools.partial(forward_kernel, block_cap),
        (shape((dom_count * block_cap, quarter, rows), BF), shape((padded, edge_count), F32)),
        smem=(0,),
        count=5,
    )(owners, gathered, bases_flat, coef_t, rel)
    received = lax.all_to_all(messages, "dom", split_axis=0, concat_axis=0, tiled=True)
    total_slots = dom_count * block_cap * rows
    output, back, grad_pre = call(
        functools.partial(owner_kernel, slot_cap, block_cap),
        (
            shape((quarter, entities), BF),
            shape((dom_count * block_cap, quarter, rows), BF),
            shape((quarter, entities), BF),
        ),
        scratch=[pltpu.VMEM((entities, total_slots), BF), pltpu.VMEM((quarter + 16, total_slots), BF)],
        count=5,
    )(arrived, received, gathered, self_weight, cotangent)
    returned = lax.all_to_all(back, "dom", split_axis=0, concat_axis=0, tiled=True)

    unit = 16 * dom_count
    tall = unit * ((flat + quarter + unit - 1) // unit)
    bases_part = call(
        functools.partial(bases_kernel, block_cap),
        shape((tall, model), BF),
        smem=(0,),
        scratch=[pltpu.VMEM((flat, edge_count), BF)],
        count=5,
    )(owners, returned, gathered, weights, grad_pre)
    parts = lax.all_to_all(
        bases_part.reshape(dom_count, tall // dom_count, model),
        "dom",
        split_axis=0,
        concat_axis=0,
        tiled=True,
    )
    edge_part = call(
        functools.partial(edges_kernel, block_cap),
        shape((feat_count, quarter, edge_count + entities + LANES), BF),
        smem=(0,),
        scratch=[pltpu.VMEM((flat, edge_count), BF), pltpu.VMEM((padded, edge_count), F32)],
        count=9,
    )(owners, returned, gathered, weights, grad_pre, bases_flat, bases_flat.T, self_weight, rel)
    edge_sum = lax.all_to_all(edge_part, "feat", split_axis=0, concat_axis=0, tiled=True)
    extra = padded * 2 * LANES // min(slot_cap, 2 * LANES)
    slot_grads, own_grads = call(
        functools.partial(slots_kernel, padded),
        (shape((dom_count, quarter + extra, slot_cap), BF), shape((quarter, entities), F32)),
        count=2,
    )(edge_sum, slot)
    arrived_grads = lax.all_to_all(slot_grads, "dom", split_axis=0, concat_axis=0, tiled=True)
    reduced = call(
        functools.partial(reduce_kernel, scale), shape((tall // dom_count, model), BF), count=1
    )(parts)
    near = [[2 * k, 2 * k + 1] for k in range(dom_count // 2)]
    far = [[2 * k + side for k in range(dom_count // 2)] for side in range(2)]
    pair = lax.all_gather(reduced, "dom", axis=0, tiled=True, axis_index_groups=near)
    whole = lax.all_gather(pair, "dom", axis=0, tiled=True, axis_index_groups=far)
    grad_feats, coef_total = call(
        functools.partial(feats_kernel, slot_cap, padded, scale),
        (shape((quarter, entities), BF), shape((padded, 2 * LANES), F32)),
        scratch=[pltpu.VMEM((quarter, entities), F32)],
        count=3,
    )(arrived_grads, arrived, own_grads)
    return (
        output,
        grad_feats,
        whole[:flat].astype(F32).reshape(basis_count, quarter, model),
        whole[flat : flat + quarter].astype(F32).T,
        coef_total[:basis_count, :relation_count].T,
    )


def pack_kernel(owners, valid, feats, part, row, dst, rel, out):
    copies = out.shape[0]
    quarter, entities = feats.shape
    blocks = part.shape[0]
    owner = jnp.zeros((blocks, LANES), I32)
    live = jnp.zeros((blocks, LANES), I32)
    for j in range(blocks):
        here = iota((blocks, LANES), 0) == j
        owner = jnp.where(here, owners[j], owner)
        live = jnp.where(here, valid[j], live)
    target = jnp.where(iota((blocks, LANES), 1) < live, dst[...], entities)
    digits = [
        part[...],
        row[...] >> 8,
        row[...] & 255,
        owner,
        target >> 8,
        target & 255,
        rel[...] >> 8,
        rel[...] & 255,
    ]
    digits = jnp.concatenate([d.astype(F32) for d in digits], axis=0).astype(BF)
    chunks = entities // LANES
    for k in range(copies):
        for c in range(chunks):
            out[k, c * quarter : (c + 1) * quarter, :] = feats[:, c * LANES : (c + 1) * LANES]
        out[k, chunks * quarter :, :] = digits


def source_kernel(
    shared, feats, part, row, mine, wide, ids, spans, targets, rels, owners, total, hots
):
    dom_count = shared.shape[0]
    quarter, entities = feats.shape
    blocks = part.shape[0]
    chunks = entities // LANES
    edge_count = blocks * LANES
    for g in range(dom_count):
        for c in range(chunks):
            start = g * entities + c * LANES
            wide[:, start : start + LANES] = shared[g, c * quarter : (c + 1) * quarter, :]
        digits = shared[g, chunks * quarter :, :].astype(F32).astype(I32)
        piece = [digits[d * blocks : (d + 1) * blocks] for d in range(8)]
        at = piece[0] * entities + piece[1] * 256 + piece[2]
        ids[g] = at
        for t in range(blocks // 2):
            spans[g * (blocks // 2) + t] = jnp.concatenate(
                [at[2 * t : 2 * t + 1], at[2 * t + 1 : 2 * t + 2]], axis=1
            )
        owners[g] = piece[3]
        targets[g] = piece[4] * 256 + piece[5]
        rels[g] = piece[6] * 256 + piece[7]
    total[...] = jnp.zeros_like(total)
    for p in range(dom_count):
        near = jnp.where(part[...] == p, row[...], -1)
        for j in range(blocks):
            hots[:, j * LANES : (j + 1) * LANES] = hot(
                iota((entities, LANES), 0) == near[j : j + 1, :]
            )
        total[...] += dot(wide[:, p * entities : (p + 1) * entities], hots[...])
    mine[:, :edge_count] = total[...].astype(BF)
    mine[:, edge_count:] = feats[...]


def split3(table):
    high = table.astype(BF)
    rest = table - high.astype(F32)
    middle = rest.astype(BF)
    low = (rest - middle.astype(F32)).astype(BF)
    return high, middle, low


def message_kernel(block_cap, entities, owners, valid, gathered, bases, coef, rel, dst, send):
    slots, tall, rows = send.shape
    blocks = rel.shape[0]
    quarter = tall - 16
    basis_count = bases.shape[0] // quarter
    group = 5
    first = iota((16, rows), 0)
    empty = jnp.where(first == 0, entities >> 8, jnp.where(first == 1, entities & 255, 0))
    empty = empty.astype(F32).astype(BF)
    for s in range(slots):
        send[s, :quarter, :] = jnp.zeros((quarter, rows), BF)
        send[s, quarter:, :] = empty
    parts = split3(coef[...])
    where = block_slots(owners, blocks, block_cap)
    for t in range(blocks // 2):
        lanes = slice(2 * t * rows, 2 * (t + 1) * rows)
        both = jnp.concatenate([rel[2 * t : 2 * t + 1, :], rel[2 * t + 1 : 2 * t + 2, :]], axis=1)
        chosen = rel_hot(both, coef.shape[1])
        mix = sum(dot(p, chosen) for p in parts)
        x = gathered[:, lanes]
        total = jnp.zeros((quarter, 2 * rows), F32)
        for c in range(0, basis_count, group):
            stop = min(c + group, basis_count)
            products = dot(bases[c * quarter : stop * quarter, :], x)
            for b in range(c, stop):
                part = products[(b - c) * quarter : (b - c + 1) * quarter]
                total = total + mix[b : b + 1, :] * part
        total = total.astype(BF)
        for k in range(2):
            j = 2 * t + k
            slot = where[j]
            live = iota((1, rows), 1) < valid[j]
            target = jnp.where(live, dst[j : j + 1, :], entities)
            code = jnp.where(first == 0, target >> 8, jnp.where(first == 1, target & 255, 0))
            send[slot, :quarter, :] = total[:, k * rows : (k + 1) * rows]
            send[slot, quarter:, :] = code.astype(F32).astype(BF)


def node_kernel(received, gathered, weight, cotangent, output, share, grad_pre, hots, flat):
    slots, _, rows = received.shape
    quarter, entities = cotangent.shape
    copies = share.shape[0]
    for s in range(slots):
        lanes = slice(s * rows, (s + 1) * rows)
        code = received[s, quarter:, :].astype(F32).astype(I32)
        target = code[0:1] * 256 + code[1:2]
        hots[:, lanes] = hot(iota((entities, rows), 0) == target)
        flat[:quarter, lanes] = received[s, :quarter, :]
    flat[quarter:, :] = jnp.ones((16, slots * rows), BF)
    own = gathered[:, gathered.shape[1] - entities :]
    own_part = dot(weight[...], own)
    sums = dot(flat[...], hots[...], NT)
    count = sums[quarter : quarter + 1]
    inverse = 1.0 / jnp.maximum(count, 1.0)
    preact = own_part + inverse * sums[:quarter]
    gate = jax.nn.sigmoid(preact)
    output[...] = (preact * gate).astype(BF)
    pre = (cotangent[...].astype(F32) * gate * (1.0 + preact * (1.0 - gate))).astype(BF)
    grad_pre[...] = pre
    whole = count.astype(I32)
    first = iota((16, entities), 0)
    code = jnp.where(first == 0, whole >> 8, jnp.where(first == 1, whole & 255, 0))
    code = code.astype(F32).astype(BF)
    for k in range(copies):
        share[k, :quarter, :] = pre
        share[k, quarter:, :] = code


def scaled_grad(shared, q, quarter):
    code = shared[q, quarter:, :].astype(F32)
    count = code[0:1] * 256.0 + code[1:2]
    inverse = 1.0 / jnp.maximum(count, 1.0)
    return (inverse * shared[q, :quarter, :].astype(F32)).astype(BF)


def rows_of_edges_kernel(entities, place, spans, *refs):
    pieces, out, full = refs[:-2], refs[-2], refs[-1]
    count, width, model = out.shape
    quarter = pieces[0].shape[0]
    for k, piece in enumerate(pieces):
        full[pl.ds(pl.multiple_of(place[k] * quarter, quarter), quarter), :] = piece[...]

    def step(n, carry):
        row = spans[place[0] * count + n]
        total = jnp.zeros((model, width), F32)
        for start in range(0, full.shape[1], entities):
            chosen = hot(iota((entities, width), 0) == row - start)
            total = total + dot(full[:, start : start + entities], chosen)
        out[n] = total.T.astype(BF)
        return carry

    lax.fori_loop(0, count, step, 0)


def rank_kernel(
    slot_cap, entities, me, ids, rels, coef, ranks, slot_rows, slot_mix, mix, comp, digits, hots
):
    dom_count, blocks, _ = ids.shape
    before = hot(iota((LANES, LANES), 0) < iota((LANES, LANES), 1))
    ones = jnp.ones((LANES, LANES), BF)
    table = coef[...].astype(BF)

    def step(g, carry):
        near = ids[g] - me[0] * entities
        mask = (near >= 0) & (near < entities)
        chosen = jnp.where(mask, 1.0, 0.0)
        chosen = jnp.concatenate([chosen, jnp.zeros_like(chosen)], axis=0).astype(BF)
        inside = dot(chosen, before)[:blocks]
        totals = dot(chosen, ones)[:blocks]
        offset = jnp.zeros((1, LANES), F32)
        offsets = []
        for j in range(blocks):
            offsets.append(offset)
            offset = offset + totals[j : j + 1]
        rank = inside + jnp.concatenate(offsets, axis=0)
        rank = jnp.where(mask, rank.astype(I32), -1)
        ranks[g] = rank
        rel = rels[g]
        rows = jnp.where(mask, near, 0)
        first = iota((16, LANES), 0)
        for j in range(blocks):
            lanes = slice(j * LANES, (j + 1) * LANES)
            comp[:, lanes] = hot(iota((slot_cap, LANES), 0) == rank[j : j + 1, :])
            at, kind = rows[j : j + 1, :], rel[j : j + 1, :]
            code = jnp.where(first == 0, at >> 8, jnp.where(first == 1, at & 255, 0))
            code = code + jnp.where(first == 2, kind >> 8, jnp.where(first == 3, kind & 255, 0))
            digits[:, lanes] = code.astype(F32).astype(BF)
            hots[:, lanes] = rel_hot(kind, coef.shape[1])
        mix[g] = dot(table, hots[...])
        found = dot(digits[...], comp[...], NT)
        slot_rows[g] = (found[0:1] * 256.0 + found[1:2]).astype(I32)
        kind = (found[2:3] * 256.0 + found[3:4]).astype(I32)
        slot_mix[g] = dot(table, rel_hot(kind, coef.shape[1]))
        return carry

    lax.fori_loop(0, dom_count, step, 0)


def coef_kernel(owners, valid, shared, gathered, bases, rel, dst, out, scaled, grads):
    blocks = rel.shape[0]
    copies, padded, relations = out.shape
    entities = shared.shape[2]
    quarter = shared.shape[1] - 16
    basis_count = bases.shape[0] // quarter
    group = 5
    scaled[...] = jnp.zeros_like(scaled)
    total = jnp.zeros((padded, relations), F32)
    for j in range(blocks):
        live = iota((1, LANES), 1) < valid[j]
        target = jnp.where(live, dst[j : j + 1, :], entities)
        chosen = hot(iota((entities, LANES), 0) == target)
        grads[:, j * LANES : (j + 1) * LANES] = dot(scaled_grad(shared, owners[j], quarter), chosen)
    for t in range(blocks // 2):
        lanes = slice(2 * t * LANES, 2 * (t + 1) * LANES)
        both = jnp.concatenate([rel[2 * t : 2 * t + 1, :], rel[2 * t + 1 : 2 * t + 2, :]], axis=1)
        x = gathered[:, lanes]
        grad = grads[:, lanes]
        for c in range(0, basis_count, group):
            stop = min(c + group, basis_count)
            products = dot(bases[c * quarter : stop * quarter, :], x)
            for b in range(c, stop):
                part = products[(b - c) * quarter : (b - c + 1) * quarter]
                scaled[b : b + 1, :] = jnp.sum(part * grad, axis=0, keepdims=True)
        high = scaled[...].astype(BF)
        low = (scaled[...] - high.astype(F32)).astype(BF)
        chosen = rel_hot(both, relations)
        total = total + dot(high, chosen, NT) + dot(low, chosen, NT)
    total = total.astype(BF)
    for k in range(copies):
        out[k] = total


def grads_kernel(owners, targets, ranks, shared, grads, slot_grads, scaled, comp):
    dom_count, blocks, _ = targets.shape
    slot_cap = comp.shape[1]
    entities = shared.shape[2]
    quarter = shared.shape[1] - 16
    for q in range(dom_count):
        scaled[q] = scaled_grad(shared, q, quarter)

    def step(g, carry):
        rows = targets[g]
        rank = ranks[g]
        for j in range(blocks):
            lanes = slice(j * LANES, (j + 1) * LANES)
            chosen = hot(iota((entities, LANES), 0) == rows[j : j + 1, :])
            grads[g, :, lanes] = dot(scaled[owners[g * blocks + j]], chosen).astype(BF)
            comp[g % 2, :, lanes] = hot(iota((slot_cap, LANES), 0) == rank[j : j + 1, :])
        slot_grads[g] = dot(grads[g], comp[g % 2], NT).astype(BF)
        return carry

    for g in range(dom_count):
        step(g, 0)


def mix_rows(mix, grad, quarter):
    pieces = []
    for b in range(mix.shape[0]):
        wide = jnp.broadcast_to(mix[b : b + 1, :], (16, mix.shape[1])).astype(BF)
        for r in range(0, quarter, 16):
            pieces.append(wide * grad[r : r + 16])
    return jnp.concatenate(pieces, axis=0)


def scatter_kernel(slot_grads, slot_rows, slot_mix, bases_t, weight, grad_pre, coefs, out, total):
    dom_count, quarter, slot_cap = slot_grads.shape
    padded = slot_mix.shape[1]
    basis_count = bases_t.shape[1] // quarter
    entities = grad_pre.shape[1]
    peers = out.shape[0]
    total[...] = lax.dot_general(
        weight[...], grad_pre[...], (((0,), (0,)), ((), ())), preferred_element_type=F32
    )

    def step(g, carry):
        combined = mix_rows(slot_mix[g][:basis_count], slot_grads[g], quarter)
        partial = dot(bases_t[...], combined).astype(BF)
        chosen = hot(iota((entities, slot_cap), 0) == slot_rows[g])
        total[...] += dot(partial, chosen, NT)
        return carry

    for g in range(dom_count):
        step(g, 0)
    coef = coefs[0].astype(F32)
    for g in range(1, dom_count):
        coef = coef + coefs[g].astype(F32)
    coef = coef.astype(BF)
    for f in range(peers):
        out[f, :, :entities] = total[f * quarter : (f + 1) * quarter].astype(BF)
        out[f, :padded, entities:] = coef[:, :LANES]
        out[f, padded : 2 * padded, entities:] = coef[:, LANES:]


def weights_kernel(scale, place, mix, grads, full, shared, *refs):
    rows, out, own_out = refs[:-2], refs[-2], refs[-1]
    dom_count, quarter, _ = grads.shape
    entities = shared.shape[2]
    basis_count = out.shape[0] // quarter
    group = 5
    own = jnp.zeros(own_out.shape, F32)
    for q in range(dom_count):
        lanes = slice(q * entities, (q + 1) * entities)
        own = own + dot(shared[q, :quarter, :], full[:, lanes], NT)
    own_out[...] = own * scale
    out[...] = jnp.zeros_like(out)
    for part, piece in enumerate(rows):
        count = piece.shape[0]

        def step(k, carry):
            g = place[part] * count + k
            grad = grads[g]
            for c in range(0, basis_count, group):
                stop = min(c + group, basis_count)
                combined = mix_rows(mix[g, c:stop, :], grad, quarter)
                out[c * quarter : stop * quarter, :] += dot(combined, piece[k])
            return carry

        lax.fori_loop(0, count, step, 0)
    out[...] = out[...] * scale


def finish_kernel(padded, scale, arrived, after, grad_feats, coef_out):
    peers, _, _ = arrived.shape
    entities = grad_feats.shape[1]
    sums = arrived[0].astype(F32)
    for f in range(1, peers):
        sums = sums + arrived[f].astype(F32)
    grad_feats[...] = sums[:, :entities].astype(BF)
    coef = jnp.concatenate([sums[:padded, entities:], sums[padded : 2 * padded, entities:]], axis=1)
    coef_out[...] = coef[: coef_out.shape[0], : coef_out.shape[1]] * scale


def body_few(
    feats,
    self_weight,
    bases,
    coef,
    src_part,
    src_row,
    edge_dst,
    edge_rel,
    block_owner,
    block_valid,
    cotangent,
):
    dom_count = lax.axis_size("dom")
    feat_count = lax.axis_size("feat")
    quarter, entities = feats.shape
    edge_count = src_row.shape[0]
    blocks = block_valid.shape[1]
    slot_cap = LANES * ((2 * edge_count + LANES * dom_count - 1) // (LANES * dom_count))
    block_cap = (2 * blocks + dom_count - 1) // dom_count
    basis_count, _, model = bases.shape
    relation_count = coef.shape[0]
    flat = basis_count * quarter
    padded = 16 * ((basis_count + 15) // 16)
    relations = 2 * LANES
    shape = jax.ShapeDtypeStruct
    scale = float(edge_count * dom_count) ** (-0.5)
    owners = block_owner[:, 0]
    valid = block_valid[0]
    part = src_part.reshape(blocks, LANES)
    row = src_row.reshape(blocks, LANES)
    dst = edge_dst.reshape(blocks, LANES)
    rel = edge_rel.reshape(blocks, LANES)
    bases_flat = bases.reshape(flat, model)
    bases_t = bases_flat.T
    weight_t = self_weight.T
    coef_t = jnp.zeros((padded, relations), F32).at[:basis_count, :relation_count].set(coef.T)
    feat_place = lax.axis_index("feat").astype(I32)

    tall = (entities // LANES) * quarter + 8 * blocks
    packed = call(pack_kernel, shape((dom_count, tall, LANES), BF), smem=(0, 1), count=7, us=1)(
        owners, valid, feats, part, row, dst, rel
    )
    shared = lax.all_to_all(packed, "dom", split_axis=0, concat_axis=0, tiled=True)
    ints = shape((dom_count, blocks, LANES), I32)
    mine, wide, ids, spans, targets, rels, all_owners = call(
        source_kernel,
        (
            shape((quarter, edge_count + entities), BF),
            shape((quarter, dom_count * entities), BF),
            ints,
            shape((dom_count * blocks // 2, 1, 2 * LANES), I32),
            ints,
            ints,
            ints,
        ),
        scratch=[pltpu.VMEM((quarter, edge_count), F32), pltpu.VMEM((entities, edge_count), BF)],
        count=4,
        us=4,
    )(shared, feats, part, row)
    gathered = lax.all_gather(mine, "feat", axis=0, tiled=True)
    owner_list = all_owners[:, :, 0].reshape(dom_count * blocks)

    def doubled(piece):
        pieces, bit, stage = [piece], feat_count // 2, 0
        while bit >= 1:
            links = [(f, f ^ bit) for f in range(feat_count)]
            pieces = pieces + [lax.ppermute(piece, "feat", links) for piece in pieces]
            bit //= 2
            stage += 1
        return pieces

    places, bit = [0], feat_count // 2
    while bit >= 1:
        places = places + [place ^ bit for place in places]
        bit //= 2
    place = jnp.stack([feat_place ^ k for k in places])
    wide, gathered = lax.optimization_barrier((wide, gathered))
    part_count = dom_count // feat_count
    rows, full = call(
        functools.partial(rows_of_edges_kernel, entities),
        (
            shape((part_count * blocks // 2, 2 * LANES, model), BF),
            shape((model, dom_count * entities), BF),
        ),
        smem=(0,),
        count=2 + feat_count,
        us=10,
    )(place, spans, *doubled(wide))
    rows = doubled(rows.reshape(part_count, edge_count, model))
    ranks, slot_rows, slot_mix, mix = call(
        functools.partial(rank_kernel, slot_cap, entities),
        (
            ints,
            shape((dom_count, 1, slot_cap), I32),
            shape((dom_count, padded, slot_cap), F32),
            shape((dom_count, padded, edge_count), F32),
        ),
        smem=(0,),
        scratch=[
            pltpu.VMEM((slot_cap, edge_count), BF),
            pltpu.VMEM((16, edge_count), BF),
            pltpu.VMEM((relations, edge_count), BF),
        ],
        count=4,
        us=4,
    )(lax.axis_index("dom").astype(I32).reshape(1), ids, rels, coef_t)

    messages = call(
        functools.partial(message_kernel, block_cap, entities),
        shape((dom_count * block_cap, quarter + 16, LANES), BF),
        smem=(0, 1),
        count=7,
        us=4,
    )(owners, valid, gathered, bases_flat, coef_t, rel, dst)
    received = lax.all_to_all(messages, "dom", split_axis=0, concat_axis=0, tiled=True)
    slots = dom_count * block_cap
    output, share, grad_pre = call(
        node_kernel,
        (
            shape((quarter, entities), BF),
            shape((dom_count, quarter + 16, entities), BF),
            shape((quarter, entities), BF),
        ),
        scratch=[
            pltpu.VMEM((entities, slots * LANES), BF),
            pltpu.VMEM((quarter + 16, slots * LANES), BF),
        ],
        count=4,
        us=4,
    )(received, gathered, weight_t, cotangent)
    nodes = lax.all_to_all(share, "dom", split_axis=0, concat_axis=0, tiled=True)

    coef_part = call(
        coef_kernel,
        shape((dom_count, padded, relations), BF),
        smem=(0, 1),
        scratch=[pltpu.VMEM((padded, 2 * LANES), F32), pltpu.VMEM((quarter, edge_count), F32)],
        count=7,
        us=4,
    )(owners, valid, nodes, gathered, bases_flat, rel, dst)
    coefs = lax.all_to_all(coef_part, "dom", split_axis=0, concat_axis=0, tiled=True)
    grads, slot_grads = call(
        grads_kernel,
        (shape((dom_count, quarter, edge_count), BF), shape((dom_count, quarter, slot_cap), BF)),
        smem=(0,),
        scratch=[
            pltpu.VMEM((dom_count, quarter, entities), BF),
            pltpu.VMEM((2, slot_cap, edge_count), BF),
        ],
        count=4,
        us=6,
    )(owner_list, targets, ranks, nodes)
    sent = call(
        scatter_kernel,
        shape((feat_count, quarter, entities + LANES), BF),
        scratch=[pltpu.VMEM((model, entities), F32)],
        count=7,
        us=5,
    )(slot_grads, slot_rows, slot_mix, bases_t, weight_t, grad_pre, coefs)
    arrived = lax.all_to_all(sent, "feat", split_axis=0, concat_axis=0, tiled=True)
    grad_bases, grad_self = call(
        functools.partial(weights_kernel, scale),
        (shape((flat, model), F32), shape((quarter, model), F32)),
        smem=(0,),
        count=5 + feat_count,
        us=12,
    )(place, mix, grads, full, nodes, *rows)
    grad_feats, coef_total = call(
        functools.partial(finish_kernel, padded, scale),
        (shape((quarter, entities), BF), shape((basis_count, relation_count), F32)),
        count=2,
        us=1,
    )(arrived, grad_self)
    return (
        output,
        grad_feats,
        grad_bases.reshape(basis_count, quarter, model),
        grad_self.T,
        coef_total.T,
    )


def solution(mesh):
    def body(*arrays):
        dom_count = lax.axis_size("dom")
        edge_count = arrays[5].shape[0]
        feat_count = lax.axis_size("feat")
        few = dom_count * edge_count <= 1 << 14 and dom_count % feat_count == 0
        if not few:
            return body_many(*arrays)
        return body_few(*arrays)

    return jax.shard_map(
        body,
        mesh=mesh,
        in_specs=(
            P("feat", "dom"),
            P(None, "feat"),
            P(None, "feat", None),
            P(),
            P("dom", None),
            P("dom"),
            P("dom"),
            P("dom"),
            P("dom", None),
            P("dom", None),
            P("feat", "dom"),
        ),
        out_specs=(P("feat", "dom"), P("feat", "dom"), P(None, "feat", None), P(None, "feat"), P()),
        check_vma=False,
    )
```

```python
import functools

import jax
import jax.numpy as jnp
from jax import lax
from jax.experimental import pallas as pl
from jax.experimental.pallas import tpu as pltpu
from jax.sharding import PartitionSpec as P


BF = jnp.bfloat16
F32 = jnp.float32
I32 = jnp.int32
LANES = 128
NN = (((1,), (0,)), ((), ()))
NT = (((1,), (1,)), ((), ()))


def iota(shape, dim):
    return lax.broadcasted_iota(I32, shape, dim)


def hot(mask):
    return jnp.where(mask, 1.0, 0.0).astype(BF)


def dot(left, right, dims=NN):
    return lax.dot_general(left, right, dims, preferred_element_type=F32)


def call(
    kernel, out_shape, smem=(), scratch=(), count=0, us=4, far=(), far_out=(), raw=()
):
    specs = [
        pl.BlockSpec(
            memory_space=pltpu.SMEM if k in smem else pltpu.HBM if k in raw else pltpu.VMEM
        )
        for k in range(count)
    ]
    single = not isinstance(out_shape, (tuple, list))
    shapes = (out_shape,) if single else tuple(out_shape)
    shapes = tuple(
        pltpu.HBM(o.shape, o.dtype) if k in far_out else o for k, o in enumerate(shapes)
    )
    outs = pl.BlockSpec(memory_space=pltpu.VMEM)
    run = pl.pallas_call(
        kernel,
        out_shape=shapes[0] if single else shapes,
        in_specs=specs,
        out_specs=outs if single else tuple(outs for _ in shapes),
        scratch_shapes=scratch,
        compiler_params=pltpu.CompilerParams(vmem_limit_bytes=24 << 20),
        cost_estimate=pl.CostEstimate(
            flops=us * 1_000_000_000, bytes_accessed=1 << 20, transcendentals=0
        ),
    )

    def apply(*arrays):
        return run(
            *(
                pltpu.with_memory_space_constraint(a, pltpu.HBM) if k in far or k in raw else a
                for k, a in enumerate(arrays)
            )
        )

    return apply


def block_slots(owners, block_count, block_cap):
    slots = []
    for j in range(block_count):
        rank = jnp.int32(0)
        for k in range(j):
            rank = rank + jnp.where(owners[k] == owners[j], 1, 0)
        slots.append(owners[j] * block_cap + rank)
    return slots


def each(count, step):
    if count <= 8:
        for k in range(count):
            step(k)
    else:
        lax.fori_loop(0, count, lambda k, c: (step(k), c)[1], 0)


def plan_kernel(
    entities, slot_cap, block_cap, owners, valid, part, row, dst, send, slot_out, hot_scratch
):
    dom_count = send.shape[0]
    edge_count = part.shape[1]
    block_count = dst.shape[0]
    chunks = slot_cap // LANES
    before = hot(iota((LANES, LANES), 0) < iota((LANES, LANES), 1))
    ones = jnp.ones((LANES, LANES), BF)
    offset = jnp.zeros((dom_count, LANES), F32)
    for c in range(edge_count // LANES):
        lanes = slice(c * LANES, (c + 1) * LANES)
        here = part[:, lanes]
        mask = iota((dom_count, LANES), 0) == here
        chosen = hot(mask)
        rank = jnp.sum(jnp.where(mask, dot(chosen, before) + offset, 0.0), axis=0, keepdims=True)
        offset = offset + dot(chosen, ones)
        slot_out[:, lanes] = here * slot_cap + rank.astype(I32)
    rows = row[...]
    digits = jnp.concatenate(
        [
            (rows >> 8).astype(F32),
            (rows & 255).astype(F32),
            jnp.ones((1, edge_count), F32),
            jnp.zeros((13, edge_count), F32),
        ],
        axis=0,
    ).astype(BF)

    def ask(p):
        near = slot_out[...] - p * slot_cap
        hot_scratch[...] = hot(iota((slot_cap, edge_count), 0) == near)
        found = dot(digits, hot_scratch[...], NT)
        wanted = found[0:1] * 256.0 + found[1:2] + (1.0 - found[2:3]) * float(entities)
        wanted = wanted.astype(I32)
        for k in range(chunks):
            send[p, k : k + 1, :] = wanted[:, k * LANES : (k + 1) * LANES]
        for t in range(block_cap):
            send[p, chunks + t : chunks + t + 1, :] = jnp.full((1, LANES), entities, I32)

    each(dom_count, ask)
    for j in range(block_count):
        rank = jnp.int32(0)
        for k in range(j):
            rank = rank + jnp.where(owners[k] == owners[j], 1, 0)
        live = iota((1, LANES), 1) < valid[j]
        send[owners[j], pl.ds(chunks + rank, 1), :] = jnp.where(live, dst[j : j + 1, :], entities)


def asked_row(arrived, g, chunks):
    rows = [arrived[g, k : k + 1, :] for k in range(chunks)]
    return rows[0] if chunks == 1 else jnp.concatenate(rows, axis=1)


def serve_kernel(slot_cap, arrived, feats, served):
    chunks = slot_cap // LANES
    entities = feats.shape[1]

    def step(g):
        asked = asked_row(arrived, g, chunks)
        chosen = hot(iota((entities, slot_cap), 0) == asked)
        served[g] = dot(feats[...], chosen).astype(BF)

    each(served.shape[0], step)


def unslot_kernel(fetched, slot, feats, out, total):
    dom_count, _, slot_cap = fetched.shape
    edge_count = slot.shape[1]
    total[...] = jnp.zeros_like(total)

    def step(p):
        near = slot[...] - p * slot_cap
        chosen = hot(iota((slot_cap, edge_count), 0) == near)
        total[...] += dot(fetched[p], chosen)

    each(dom_count, step)
    out[:, :edge_count] = total[...].astype(BF)
    out[:, edge_count:] = feats[...]


def rel_hot(rel, width):
    return hot(iota((width, rel.shape[1]), 0) == rel)


def forward_kernel(block_cap, owners, gathered, bases, coef, rel, send, weights):
    _, quarter, rows = send.shape
    edge_count = rel.shape[1]
    block_count = edge_count // rows
    basis_count = bases.shape[0] // quarter
    span = 2 * rows if block_count % 2 == 0 else rows
    group = 5
    send[...] = jnp.zeros_like(send)
    table = coef[...]
    high = table.astype(BF)
    rest = table - high.astype(F32)
    middle = rest.astype(BF)
    low = (rest - middle.astype(F32)).astype(BF)
    where = block_slots(owners, block_count, block_cap)
    for t in range(edge_count // span):
        lanes = slice(t * span, (t + 1) * span)
        chosen = rel_hot(rel[:, lanes], coef.shape[1])
        mix = dot(high, chosen) + dot(middle, chosen) + dot(low, chosen)
        weights[:, lanes] = mix
        x = gathered[:, lanes]
        total = jnp.zeros((quarter, span), F32)
        for c in range(0, basis_count, group):
            stop = min(c + group, basis_count)
            products = dot(bases[c * quarter : stop * quarter, :], x)
            for b in range(c, stop):
                part = products[(b - c) * quarter : (b - c + 1) * quarter]
                total = total + mix[b : b + 1, :] * part
        total = total.astype(BF)
        for k in range(span // rows):
            send[where[t * (span // rows) + k]] = total[:, k * rows : (k + 1) * rows]


def owner_kernel(
    slot_cap, block_cap, arrived, received, gathered, weight, cotangent, output, back, grad_pre, hots, flat
):
    slots, quarter, rows = received.shape
    entities = cotangent.shape[1]
    chunks = slot_cap // LANES
    width = slots * rows
    for s in range(slots):
        lanes = slice(s * rows, (s + 1) * rows)
        target = arrived[s // block_cap, chunks + s % block_cap : chunks + s % block_cap + 1, :]
        hots[:, lanes] = hot(iota((entities, rows), 0) == target)
        flat[:quarter, lanes] = received[s]
    flat[quarter:, :] = jnp.ones((16, width), BF)
    own = gathered[:, gathered.shape[1] - entities :]
    own_part = lax.dot_general(
        weight[...], own, (((0,), (0,)), ((), ())), preferred_element_type=F32
    )
    sums = dot(flat[...], hots[...], NT)
    inverse = 1.0 / jnp.maximum(sums[quarter : quarter + 1], 1.0)
    preact = own_part + inverse * sums[:quarter]
    gate = jax.nn.sigmoid(preact)
    output[...] = (preact * gate).astype(BF)
    pre = (cotangent[...].astype(F32) * gate * (1.0 + preact * (1.0 - gate))).astype(BF)
    grad_pre[...] = pre
    scaled = (inverse * pre.astype(F32)).astype(BF)
    for s in range(slots):
        back[s] = dot(scaled, hots[:, s * rows : (s + 1) * rows]).astype(BF)


def fill_combined(where, returned, weights, combined, basis_count):
    quarter, rows = returned.shape[1:]
    for j, slot in enumerate(where):
        lanes = slice(j * rows, (j + 1) * rows)
        grad = returned[slot].astype(F32)
        for b in range(basis_count):
            combined[b * quarter : (b + 1) * quarter, lanes] = (
                weights[b : b + 1, lanes] * grad
            ).astype(BF)


def bases_kernel(block_cap, owners, returned, gathered, weights, grad_pre, out, combined):
    quarter, rows = returned.shape[1:]
    edge_count = weights.shape[1]
    total = combined.shape[0]
    where = block_slots(owners, edge_count // rows, block_cap)
    fill_combined(where, returned, weights, combined, total // quarter)
    x = gathered[:, :edge_count]
    chunk = 5 * quarter
    for start in range(0, total, chunk):
        stop = min(start + chunk, total)
        out[start:stop, :] = dot(combined[start:stop, :], x, NT).astype(BF)
    own = gathered[:, edge_count:]
    out[total : total + quarter, :] = dot(grad_pre[...], own, NT).astype(BF)
    out[total + quarter :, :] = jnp.zeros((out.shape[0] - total - quarter, out.shape[1]), BF)


def edges_kernel(
    block_cap, owners, returned, gathered, weights, grad_pre, bases, bases_t, weight, rel, out, combined, scaled
):
    quarter, rows = returned.shape[1:]
    edge_count = weights.shape[1]
    entities = grad_pre.shape[1]
    total = combined.shape[0]
    basis_count = total // quarter
    padded = weights.shape[0]
    relations = 2 * LANES
    where = block_slots(owners, edge_count // rows, block_cap)
    fill_combined(where, returned, weights, combined, basis_count)
    peers = out.shape[0]
    share = out.shape[1]
    span = 2 * rows if (edge_count // rows) % 2 == 0 else rows
    scaled[...] = jnp.zeros_like(scaled)
    for t in range(edge_count // span):
        lanes = slice(t * span, (t + 1) * span)
        partial = dot(bases_t[...], combined[:, lanes]).astype(BF)
        for f in range(peers):
            out[f, :, lanes] = partial[f * share : (f + 1) * share]
        x = gathered[:, lanes]
        count = span // rows
        grad = [returned[where[t * count + k]].astype(F32) for k in range(count)]
        grad = grad[0] if count == 1 else jnp.concatenate(grad, axis=1)
        group = 5
        for c in range(0, basis_count, group):
            stop = min(c + group, basis_count)
            products = dot(bases[c * quarter : stop * quarter, :], x)
            for b in range(c, stop):
                part = products[(b - c) * quarter : (b - c + 1) * quarter]
                scaled[b : b + 1, lanes] = jnp.sum(part * grad, axis=0, keepdims=True)
    high = scaled[...].astype(BF)
    low = (scaled[...] - high.astype(F32)).astype(BF)
    chosen = rel_hot(rel[...], relations)
    coef = (dot(high, chosen, NT) + dot(low, chosen, NT)).astype(BF)
    own = dot(weight[...], grad_pre[...]).astype(BF)
    tail = edge_count + entities
    for f in range(peers):
        out[f, :, edge_count:tail] = own[f * share : (f + 1) * share]
        out[f, :padded, tail:] = coef[:, :LANES]
        out[f, padded : 2 * padded, tail:] = coef[:, LANES:]


def slots_kernel(padded, arrived, slot, out, own):
    peers, share, _ = arrived.shape
    dom_count, _, slot_cap = out.shape
    edge_count = slot.shape[1]
    entities = own.shape[1]
    sums = arrived[0].astype(F32)
    for f in range(1, peers):
        sums = sums + arrived[f].astype(F32)
    own[...] = sums[:, edge_count : edge_count + entities]
    edges = sums[:, :edge_count].astype(BF)
    coef = sums[: 2 * padded, edge_count + entities :].astype(BF)

    def step(p):
        near = slot[...] - p * slot_cap
        chosen = hot(iota((slot_cap, edge_count), 0) == near)
        out[p, :share, :] = dot(edges, chosen, NT).astype(BF)
        if slot_cap >= 2 * LANES:
            out[p, share:, :LANES] = coef[:padded]
            out[p, share:, LANES : 2 * LANES] = coef[padded:]
        else:
            out[p, share:, :] = coef

    each(dom_count, step)


def feats_kernel(slot_cap, padded, scale, arrived, asked, own, out, coef, total):
    dom_count, _, _ = arrived.shape
    share, entities = own.shape
    chunks = slot_cap // LANES
    total[...] = own[...]
    coef[...] = jnp.zeros_like(coef)

    def step(g):
        chosen = hot(iota((entities, slot_cap), 0) == asked_row(asked, g, chunks))
        total[...] += dot(arrived[g, :share, :], chosen, NT)
        if slot_cap >= 2 * LANES:
            coef[...] += arrived[g, share:, : 2 * LANES].astype(F32)
        else:
            coef[:, :LANES] += arrived[g, share : share + padded, :].astype(F32)
            coef[:, LANES:] += arrived[g, share + padded :, :].astype(F32)

    each(dom_count, step)
    out[...] = total[...].astype(BF)
    coef[...] = coef[...] * scale


def reduce_kernel(scale, parts, out):
    sums = parts[0].astype(F32)
    for k in range(1, parts.shape[0]):
        sums = sums + parts[k].astype(F32)
    out[...] = (sums * scale).astype(BF)


def body_many(
    feats,
    self_weight,
    bases,
    coef,
    src_part,
    src_row,
    edge_dst,
    edge_rel,
    block_owner,
    block_valid,
    cotangent,
):
    dom_count = lax.axis_size("dom")
    feat_count = lax.axis_size("feat")
    quarter, entities = feats.shape
    edge_count = src_row.shape[0]
    block_count = block_valid.shape[1]
    rows = edge_count // block_count
    slot_cap = LANES * ((2 * edge_count + LANES * dom_count - 1) // (LANES * dom_count))
    block_cap = (2 * block_count + dom_count - 1) // dom_count
    basis_count, _, model = bases.shape
    relation_count = coef.shape[0]
    flat = basis_count * quarter
    padded = 8 * ((basis_count + 7) // 8)
    padded = 16 * ((padded + 15) // 16)
    shape = jax.ShapeDtypeStruct
    scale = float(edge_count * dom_count) ** (-0.5)

    owners = block_owner[:, 0]
    valid = block_valid[0]
    rel = edge_rel.reshape(1, edge_count)
    bases_flat = bases.reshape(flat, model)
    coef_t = jnp.zeros((padded, 2 * LANES), F32).at[:basis_count, :relation_count].set(coef.T)

    height = slot_cap // LANES + block_cap
    send, slot = call(
        functools.partial(plan_kernel, entities, slot_cap, block_cap),
        (shape((dom_count, height, LANES), I32), shape((1, edge_count), I32)),
        smem=(0, 1),
        scratch=[pltpu.VMEM((slot_cap, edge_count), BF)],
        count=5,
    )(
        owners,
        valid,
        src_part.reshape(1, edge_count),
        src_row.reshape(1, edge_count),
        edge_dst.reshape(block_count, rows),
    )
    arrived = lax.all_to_all(send, "dom", split_axis=0, concat_axis=0, tiled=True)
    served = call(
        functools.partial(serve_kernel, slot_cap),
        shape((dom_count, quarter, slot_cap), BF),
        count=2,
    )(arrived, feats)
    fetched = lax.all_to_all(served, "dom", split_axis=0, concat_axis=0, tiled=True)
    mine = call(
        unslot_kernel,
        shape((quarter, edge_count + entities), BF),
        scratch=[pltpu.VMEM((quarter, edge_count), F32)],
        count=3,
    )(fetched, slot, feats)
    gathered = lax.all_gather(mine, "feat", axis=0, tiled=True)

    messages, weights = call(
        functools.partial(forward_kernel, block_cap),
        (shape((dom_count * block_cap, quarter, rows), BF), shape((padded, edge_count), F32)),
        smem=(0,),
        count=5,
    )(owners, gathered, bases_flat, coef_t, rel)
    received = lax.all_to_all(messages, "dom", split_axis=0, concat_axis=0, tiled=True)
    total_slots = dom_count * block_cap * rows
    output, back, grad_pre = call(
        functools.partial(owner_kernel, slot_cap, block_cap),
        (
            shape((quarter, entities), BF),
            shape((dom_count * block_cap, quarter, rows), BF),
            shape((quarter, entities), BF),
        ),
        scratch=[pltpu.VMEM((entities, total_slots), BF), pltpu.VMEM((quarter + 16, total_slots), BF)],
        count=5,
    )(arrived, received, gathered, self_weight, cotangent)
    returned = lax.all_to_all(back, "dom", split_axis=0, concat_axis=0, tiled=True)

    unit = 16 * dom_count
    tall = unit * ((flat + quarter + unit - 1) // unit)
    bases_part = call(
        functools.partial(bases_kernel, block_cap),
        shape((tall, model), BF),
        smem=(0,),
        scratch=[pltpu.VMEM((flat, edge_count), BF)],
        count=5,
    )(owners, returned, gathered, weights, grad_pre)
    parts = lax.all_to_all(
        bases_part.reshape(dom_count, tall // dom_count, model),
        "dom",
        split_axis=0,
        concat_axis=0,
        tiled=True,
    )
    edge_part = call(
        functools.partial(edges_kernel, block_cap),
        shape((feat_count, quarter, edge_count + entities + LANES), BF),
        smem=(0,),
        scratch=[pltpu.VMEM((flat, edge_count), BF), pltpu.VMEM((padded, edge_count), F32)],
        count=9,
    )(owners, returned, gathered, weights, grad_pre, bases_flat, bases_flat.T, self_weight, rel)
    edge_sum = lax.all_to_all(edge_part, "feat", split_axis=0, concat_axis=0, tiled=True)
    extra = padded * 2 * LANES // min(slot_cap, 2 * LANES)
    slot_grads, own_grads = call(
        functools.partial(slots_kernel, padded),
        (shape((dom_count, quarter + extra, slot_cap), BF), shape((quarter, entities), F32)),
        count=2,
    )(edge_sum, slot)
    arrived_grads = lax.all_to_all(slot_grads, "dom", split_axis=0, concat_axis=0, tiled=True)
    reduced = call(
        functools.partial(reduce_kernel, scale), shape((tall // dom_count, model), BF), count=1
    )(parts)
    near = [[2 * k, 2 * k + 1] for k in range(dom_count // 2)]
    far = [[2 * k + side for k in range(dom_count // 2)] for side in range(2)]
    pair = lax.all_gather(reduced, "dom", axis=0, tiled=True, axis_index_groups=near)
    whole = lax.all_gather(pair, "dom", axis=0, tiled=True, axis_index_groups=far)
    grad_feats, coef_total = call(
        functools.partial(feats_kernel, slot_cap, padded, scale),
        (shape((quarter, entities), BF), shape((padded, 2 * LANES), F32)),
        scratch=[pltpu.VMEM((quarter, entities), F32)],
        count=3,
    )(arrived_grads, arrived, own_grads)
    return (
        output,
        grad_feats,
        whole[:flat].astype(F32).reshape(basis_count, quarter, model),
        whole[flat : flat + quarter].astype(F32).T,
        coef_total[:basis_count, :relation_count].T,
    )


def pack_kernel(owners, valid, feats, part, row, dst, rel, out):
    copies = out.shape[0]
    quarter, entities = feats.shape
    blocks = part.shape[0]
    owner = jnp.zeros((blocks, LANES), I32)
    live = jnp.zeros((blocks, LANES), I32)
    for j in range(blocks):
        here = iota((blocks, LANES), 0) == j
        owner = jnp.where(here, owners[j], owner)
        live = jnp.where(here, valid[j], live)
    target = jnp.where(iota((blocks, LANES), 1) < live, dst[...], entities)
    digits = [
        part[...],
        row[...] >> 8,
        row[...] & 255,
        owner,
        target >> 8,
        target & 255,
        rel[...] >> 8,
        rel[...] & 255,
    ]
    digits = jnp.concatenate([d.astype(F32) for d in digits], axis=0).astype(BF)
    chunks = entities // LANES
    for k in range(copies):
        for c in range(chunks):
            out[k, c * quarter : (c + 1) * quarter, :] = feats[:, c * LANES : (c + 1) * LANES]
        out[k, chunks * quarter :, :] = digits


def source_kernel(
    shared, feats, part, row, mine, wide, ids, spans, targets, rels, owners, total, hots
):
    dom_count = shared.shape[0]
    quarter, entities = feats.shape
    blocks = part.shape[0]
    chunks = entities // LANES
    edge_count = blocks * LANES
    for g in range(dom_count):
        for c in range(chunks):
            start = g * entities + c * LANES
            wide[:, start : start + LANES] = shared[g, c * quarter : (c + 1) * quarter, :]
        digits = shared[g, chunks * quarter :, :].astype(F32).astype(I32)
        piece = [digits[d * blocks : (d + 1) * blocks] for d in range(8)]
        at = piece[0] * entities + piece[1] * 256 + piece[2]
        ids[g] = at
        for t in range(blocks // 2):
            spans[g * (blocks // 2) + t] = jnp.concatenate(
                [at[2 * t : 2 * t + 1], at[2 * t + 1 : 2 * t + 2]], axis=1
            )
        owners[g] = piece[3]
        targets[g] = piece[4] * 256 + piece[5]
        rels[g] = piece[6] * 256 + piece[7]
    total[...] = jnp.zeros_like(total)
    for p in range(dom_count):
        near = jnp.where(part[...] == p, row[...], -1)
        for j in range(blocks):
            hots[:, j * LANES : (j + 1) * LANES] = hot(
                iota((entities, LANES), 0) == near[j : j + 1, :]
            )
        total[...] += dot(wide[:, p * entities : (p + 1) * entities], hots[...])
    mine[:, :edge_count] = total[...].astype(BF)
    mine[:, edge_count:] = feats[...]


def split3(table):
    high = table.astype(BF)
    rest = table - high.astype(F32)
    middle = rest.astype(BF)
    low = (rest - middle.astype(F32)).astype(BF)
    return high, middle, low


def message_kernel(block_cap, entities, owners, valid, gathered, bases, coef, rel, dst, send):
    slots, tall, rows = send.shape
    blocks = rel.shape[0]
    quarter = tall - 16
    basis_count = bases.shape[0] // quarter
    group = 5
    first = iota((16, rows), 0)
    empty = jnp.where(first == 0, entities >> 8, jnp.where(first == 1, entities & 255, 0))
    empty = empty.astype(F32).astype(BF)
    for s in range(slots):
        send[s, :quarter, :] = jnp.zeros((quarter, rows), BF)
        send[s, quarter:, :] = empty
    parts = split3(coef[...])
    where = block_slots(owners, blocks, block_cap)
    for t in range(blocks // 2):
        lanes = slice(2 * t * rows, 2 * (t + 1) * rows)
        both = jnp.concatenate([rel[2 * t : 2 * t + 1, :], rel[2 * t + 1 : 2 * t + 2, :]], axis=1)
        chosen = rel_hot(both, coef.shape[1])
        mix = sum(dot(p, chosen) for p in parts)
        x = gathered[:, lanes]
        total = jnp.zeros((quarter, 2 * rows), F32)
        for c in range(0, basis_count, group):
            stop = min(c + group, basis_count)
            products = dot(bases[c * quarter : stop * quarter, :], x)
            for b in range(c, stop):
                part = products[(b - c) * quarter : (b - c + 1) * quarter]
                total = total + mix[b : b + 1, :] * part
        total = total.astype(BF)
        for k in range(2):
            j = 2 * t + k
            slot = where[j]
            live = iota((1, rows), 1) < valid[j]
            target = jnp.where(live, dst[j : j + 1, :], entities)
            code = jnp.where(first == 0, target >> 8, jnp.where(first == 1, target & 255, 0))
            send[slot, :quarter, :] = total[:, k * rows : (k + 1) * rows]
            send[slot, quarter:, :] = code.astype(F32).astype(BF)


def node_kernel(received, gathered, weight, cotangent, output, share, grad_pre, hots, flat):
    slots, _, rows = received.shape
    quarter, entities = cotangent.shape
    copies = share.shape[0]
    for s in range(slots):
        lanes = slice(s * rows, (s + 1) * rows)
        code = received[s, quarter:, :].astype(F32).astype(I32)
        target = code[0:1] * 256 + code[1:2]
        hots[:, lanes] = hot(iota((entities, rows), 0) == target)
        flat[:quarter, lanes] = received[s, :quarter, :]
    flat[quarter:, :] = jnp.ones((16, slots * rows), BF)
    own = gathered[:, gathered.shape[1] - entities :]
    own_part = dot(weight[...], own)
    sums = dot(hots[...], flat[...], NT).T
    count = sums[quarter : quarter + 1]
    inverse = 1.0 / jnp.maximum(count, 1.0)
    preact = own_part + inverse * sums[:quarter]
    gate = jax.nn.sigmoid(preact)
    output[...] = (preact * gate).astype(BF)
    pre = (cotangent[...].astype(F32) * gate * (1.0 + preact * (1.0 - gate))).astype(BF)
    grad_pre[...] = pre
    whole = count.astype(I32)
    first = iota((16, entities), 0)
    code = jnp.where(first == 0, whole >> 8, jnp.where(first == 1, whole & 255, 0))
    code = code.astype(F32).astype(BF)
    for k in range(copies):
        share[k, :quarter, :] = pre
        share[k, quarter:, :] = code


def scaled_grad(shared, q, quarter):
    code = shared[q, quarter:, :].astype(F32)
    count = code[0:1] * 256.0 + code[1:2]
    inverse = 1.0 / jnp.maximum(count, 1.0)
    return (inverse * shared[q, :quarter, :].astype(F32)).astype(BF)


def rows_of_edges_kernel(entities, place, spans, *refs):
    pieces, out, full = refs[:-2], refs[-2], refs[-1]
    count, width, model = out.shape
    quarter = pieces[0].shape[0]
    for k, piece in enumerate(pieces):
        full[pl.ds(pl.multiple_of(place[k] * quarter, quarter), quarter), :] = piece[...]

    def step(n, carry):
        row = spans[place[0] * count + n]
        total = jnp.zeros((model, width), F32)
        for start in range(0, full.shape[1], entities):
            chosen = hot(iota((entities, width), 0) == row - start)
            total = total + dot(full[:, start : start + entities], chosen)
        out[n] = total.T.astype(BF)
        return carry

    lax.fori_loop(0, count, step, 0)


def rank_kernel(
    slot_cap, entities, me, ids, rels, coef, ranks, slot_rows, slot_mix, mix, comp, digits, hots
):
    dom_count, blocks, _ = ids.shape
    before = hot(iota((LANES, LANES), 0) < iota((LANES, LANES), 1))
    ones = jnp.ones((LANES, LANES), BF)
    table = coef[...].astype(BF)

    def step(g, carry):
        near = ids[g] - me[0] * entities
        mask = (near >= 0) & (near < entities)
        chosen = jnp.where(mask, 1.0, 0.0)
        chosen = jnp.concatenate([chosen, jnp.zeros_like(chosen)], axis=0).astype(BF)
        inside = dot(chosen, before)[:blocks]
        totals = dot(chosen, ones)[:blocks]
        offset = jnp.zeros((1, LANES), F32)
        offsets = []
        for j in range(blocks):
            offsets.append(offset)
            offset = offset + totals[j : j + 1]
        rank = inside + jnp.concatenate(offsets, axis=0)
        rank = jnp.where(mask, rank.astype(I32), -1)
        ranks[g] = rank
        rel = rels[g]
        rows = jnp.where(mask, near, 0)
        first = iota((16, LANES), 0)
        for j in range(blocks):
            lanes = slice(j * LANES, (j + 1) * LANES)
            comp[:, lanes] = hot(iota((slot_cap, LANES), 0) == rank[j : j + 1, :])
            at, kind = rows[j : j + 1, :], rel[j : j + 1, :]
            code = jnp.where(first == 0, at >> 8, jnp.where(first == 1, at & 255, 0))
            code = code + jnp.where(first == 2, kind >> 8, jnp.where(first == 3, kind & 255, 0))
            digits[:, lanes] = code.astype(F32).astype(BF)
            hots[:, lanes] = rel_hot(kind, coef.shape[1])
        mix[g] = dot(table, hots[...])
        found = dot(digits[...], comp[...], NT)
        slot_rows[g] = (found[0:1] * 256.0 + found[1:2]).astype(I32)
        kind = (found[2:3] * 256.0 + found[3:4]).astype(I32)
        slot_mix[g] = dot(table, rel_hot(kind, coef.shape[1]))
        return carry

    lax.fori_loop(0, dom_count, step, 0)


def products_kernel(gathered, bases, bases_t, out):
    edge_count = out.shape[1]
    bases_t[...] = bases[...].T
    step = 320
    for start in range(0, out.shape[0], step):
        stop = min(start + step, out.shape[0])
        out[start:stop, :] = dot(bases[start:stop, :], gathered[:, :edge_count]).astype(BF)


def coef_kernel(
    owners, valid, shared, products_far, rel, dst, out, scaled, grads, products, sems
):
    fetched = fetch(((products_far, products),), sems)
    blocks = rel.shape[0]
    copies, _, relations = out.shape
    entities = shared.shape[2]
    quarter = shared.shape[1] - 16
    basis_count = products.shape[0] // quarter
    scaled[...] = jnp.zeros_like(scaled)
    for j in range(blocks):
        live = iota((1, LANES), 1) < valid[j]
        target = jnp.where(live, dst[j : j + 1, :], entities)
        chosen = hot(iota((entities, LANES), 0) == target)
        grads[:, j * LANES : (j + 1) * LANES] = dot(scaled_grad(shared, owners[j], quarter), chosen)
    fetched[0].wait()
    for t in range(blocks // 2):
        lanes = slice(2 * t * LANES, 2 * (t + 1) * LANES)
        grad = grads[:, lanes]
        for b in range(basis_count):
            part = products[b * quarter : (b + 1) * quarter, lanes].astype(F32)
            scaled[b : b + 1, lanes] = jnp.sum(part * grad, axis=0, keepdims=True)
    high = scaled[...].astype(BF)
    low = (scaled[...] - high.astype(F32)).astype(BF)
    kinds = jnp.concatenate([rel[j : j + 1, :] for j in range(blocks)], axis=1)
    chosen = rel_hot(kinds, relations)
    total = (dot(chosen, high, NT) + dot(chosen, low, NT)).T.astype(BF)
    for k in range(copies):
        out[k] = total


def grads_kernel(owners, targets, ranks, shared, grads, slot_grads, scaled, comp):
    dom_count, blocks, _ = targets.shape
    slot_cap = comp.shape[1]
    entities = shared.shape[2]
    quarter = shared.shape[1] - 16
    for q in range(dom_count):
        scaled[q] = scaled_grad(shared, q, quarter)

    def step(g, carry):
        rows = targets[g]
        rank = ranks[g]
        for j in range(blocks):
            lanes = slice(j * LANES, (j + 1) * LANES)
            chosen = hot(iota((entities, LANES), 0) == rows[j : j + 1, :])
            grads[g, :, lanes] = dot(scaled[owners[g * blocks + j]], chosen).astype(BF)
            comp[g % 2, :, lanes] = hot(iota((slot_cap, LANES), 0) == rank[j : j + 1, :])
        slot_grads[g] = dot(grads[g], comp[g % 2], NT).astype(BF)
        return carry

    for g in range(dom_count):
        step(g, 0)


def mix_rows(mix, grad, quarter):
    pieces = []
    for b in range(mix.shape[0]):
        wide = jnp.broadcast_to(mix[b : b + 1, :], (16, mix.shape[1])).astype(BF)
        for r in range(0, quarter, 16):
            pieces.append(wide * grad[r : r + 16])
    return jnp.concatenate(pieces, axis=0)


def scatter_kernel(
    slot_grads, slot_rows, slot_mix, bases_far, weight, grad_pre, coefs, out, total, bases_t, sems
):
    copies = fetch(((bases_far, bases_t),), sems)
    dom_count, quarter, slot_cap = slot_grads.shape
    padded = slot_mix.shape[1]
    basis_count = bases_t.shape[1] // quarter
    entities = grad_pre.shape[1]
    peers = out.shape[0]
    total[...] = lax.dot_general(
        weight[...], grad_pre[...], (((0,), (0,)), ((), ())), preferred_element_type=F32
    )

    copies[0].wait()

    def step(g, carry):
        combined = mix_rows(slot_mix[g][:basis_count], slot_grads[g], quarter)
        partial = dot(bases_t[...], combined).astype(BF)
        chosen = hot(iota((entities, slot_cap), 0) == slot_rows[g])
        total[...] += dot(partial, chosen, NT)
        return carry

    for g in range(dom_count):
        step(g, 0)
    coef = coefs[0].astype(F32)
    for g in range(1, dom_count):
        coef = coef + coefs[g].astype(F32)
    coef = coef.astype(BF)
    for f in range(peers):
        out[f, :, :entities] = total[f * quarter : (f + 1) * quarter].astype(BF)
        out[f, :padded, entities:] = coef[:, :LANES]
        out[f, padded : 2 * padded, entities:] = coef[:, LANES:]


def fetch(pairs, sems):
    copies = [
        pltpu.make_async_copy(source, target, sems.at[k]) for k, (source, target) in enumerate(pairs)
    ]
    for copy in copies:
        copy.start()
    return copies


def weights_kernel(scale, place, mix_far, grads_far, full_far, shared, *refs):
    rows, (out, own_out, mix, grads, full, sems) = refs[:-6], refs[-6:]
    copies = fetch(((mix_far, mix), (grads_far, grads), (full_far, full)), sems)
    dom_count, quarter, _ = grads.shape
    entities = shared.shape[2]
    basis_count = out.shape[0] // quarter
    group = 5
    copies[0].wait()
    copies[1].wait()
    for part, piece in enumerate(rows):
        count = piece.shape[0]
        for k in range(count):
            g = place[part] * count + k
            grad = grads[g]
            for c in range(0, basis_count, group):
                stop = min(c + group, basis_count)
                combined = mix_rows(mix[g, c:stop, :], grad, quarter)
                total = dot(combined, piece[k])
                lanes = slice(c * quarter, stop * quarter)
                if part > 0 or k > 0:
                    total = total + out[lanes, :]
                if part == len(rows) - 1 and k == count - 1:
                    total = total * scale
                out[lanes, :] = total
    copies[2].wait()
    own = jnp.zeros(own_out.shape, F32)
    for q in range(dom_count):
        lanes = slice(q * entities, (q + 1) * entities)
        own = own + dot(shared[q, :quarter, :], full[:, lanes], NT)
    own_out[...] = own * scale


def finish_kernel(padded, scale, arrived, grad_feats, coef_out):
    peers, _, _ = arrived.shape
    entities = grad_feats.shape[1]
    sums = arrived[0].astype(F32)
    for f in range(1, peers):
        sums = sums + arrived[f].astype(F32)
    grad_feats[...] = sums[:, :entities].astype(BF)
    coef = jnp.concatenate([sums[:padded, entities:], sums[padded : 2 * padded, entities:]], axis=1)
    coef_out[...] = coef[: coef_out.shape[0], : coef_out.shape[1]] * scale


def body_few(
    feats,
    self_weight,
    bases,
    coef,
    src_part,
    src_row,
    edge_dst,
    edge_rel,
    block_owner,
    block_valid,
    cotangent,
):
    dom_count = lax.axis_size("dom")
    feat_count = lax.axis_size("feat")
    quarter, entities = feats.shape
    edge_count = src_row.shape[0]
    blocks = block_valid.shape[1]
    slot_cap = LANES * ((2 * edge_count + LANES * dom_count - 1) // (LANES * dom_count))
    block_cap = (2 * blocks + dom_count - 1) // dom_count
    basis_count, _, model = bases.shape
    relation_count = coef.shape[0]
    flat = basis_count * quarter
    padded = 16 * ((basis_count + 15) // 16)
    relations = 2 * LANES
    shape = jax.ShapeDtypeStruct
    scale = float(edge_count * dom_count) ** (-0.5)
    owners = block_owner[:, 0]
    valid = block_valid[0]
    part = src_part.reshape(blocks, LANES)
    row = src_row.reshape(blocks, LANES)
    dst = edge_dst.reshape(blocks, LANES)
    rel = edge_rel.reshape(blocks, LANES)
    bases_flat = bases.reshape(flat, model)
    weight_t = self_weight.T
    coef_t = jnp.zeros((padded, relations), F32).at[:basis_count, :relation_count].set(coef.T)
    feat_place = lax.axis_index("feat").astype(I32)

    tall = (entities // LANES) * quarter + 8 * blocks
    packed = call(
        pack_kernel,
        shape((1, tall, LANES), BF),
        smem=(0, 1),
        count=7,
        us=1,
        far=(0, 1, 2, 3, 4, 5, 6),
    )(
        owners, valid, feats, part, row, dst, rel
    )
    near = [[2 * k, 2 * k + 1] for k in range(dom_count // 2)]
    far = [[2 * k + side for k in range(dom_count // 2)] for side in range(2)]
    shared = lax.all_gather(packed, "dom", axis=0, tiled=True, axis_index_groups=near)
    shared = lax.all_gather(shared, "dom", axis=0, tiled=True, axis_index_groups=far)
    ints = shape((dom_count, blocks, LANES), I32)
    mine, wide, ids, spans, targets, rels, all_owners = call(
        source_kernel,
        (
            shape((quarter, edge_count + entities), BF),
            shape((quarter, dom_count * entities), BF),
            ints,
            shape((dom_count * blocks // 2, 1, 2 * LANES), I32),
            ints,
            ints,
            ints,
        ),
        scratch=[pltpu.VMEM((quarter, edge_count), F32), pltpu.VMEM((entities, edge_count), BF)],
        count=4,
        us=4,
        far_out=(3, 4, 6),
    )(shared, feats, part, row)
    gathered = lax.all_gather(mine, "feat", axis=0, tiled=True)
    owner_list = all_owners[:, :, 0].reshape(dom_count * blocks)

    def doubled(piece):
        pieces, bit, stage = [piece], feat_count // 2, 0
        while bit >= 1:
            links = [(f, f ^ bit) for f in range(feat_count)]
            pieces = pieces + [lax.ppermute(piece, "feat", links) for piece in pieces]
            bit //= 2
            stage += 1
        return pieces

    places, bit = [0], feat_count // 2
    while bit >= 1:
        places = places + [place ^ bit for place in places]
        bit //= 2
    place = jnp.stack([feat_place ^ k for k in places])
    wide, gathered = lax.optimization_barrier((wide, gathered))
    part_count = dom_count // feat_count
    rows, full = call(
        functools.partial(rows_of_edges_kernel, entities),
        (
            shape((part_count * blocks // 2, 2 * LANES, model), BF),
            shape((model, dom_count * entities), BF),
        ),
        smem=(0,),
        count=2 + feat_count,
        us=10,
        far=(0,),
        far_out=(1,),
    )(place, spans, *doubled(wide))
    rows = doubled(rows.reshape(part_count, edge_count, model))
    ranks, slot_rows, slot_mix, mix = call(
        functools.partial(rank_kernel, slot_cap, entities),
        (
            ints,
            shape((dom_count, 1, slot_cap), I32),
            shape((dom_count, padded, slot_cap), F32),
            shape((dom_count, padded, edge_count), F32),
        ),
        smem=(0,),
        scratch=[
            pltpu.VMEM((slot_cap, edge_count), BF),
            pltpu.VMEM((16, edge_count), BF),
            pltpu.VMEM((relations, edge_count), BF),
        ],
        count=4,
        us=4,
        far=(0,),
        far_out=(0, 1, 2, 3),
    )(lax.axis_index("dom").astype(I32).reshape(1), ids, rels, coef_t)

    messages = call(
        functools.partial(message_kernel, block_cap, entities),
        shape((dom_count * block_cap, quarter + 16, LANES), BF),
        smem=(0, 1),
        count=7,
        us=4,
        far=(0, 1),
    )(owners, valid, gathered, bases_flat, coef_t, rel, dst)
    received = lax.all_to_all(messages, "dom", split_axis=0, concat_axis=0, tiled=True)
    slots = dom_count * block_cap
    output, share, grad_pre = call(
        node_kernel,
        (
            shape((quarter, entities), BF),
            shape((dom_count, quarter + 16, entities), BF),
            shape((quarter, entities), BF),
        ),
        scratch=[
            pltpu.VMEM((entities, slots * LANES), BF),
            pltpu.VMEM((quarter + 16, slots * LANES), BF),
        ],
        count=4,
        us=4,
        far_out=(2,),
    )(received, gathered, weight_t, cotangent)
    nodes = lax.all_to_all(share, "dom", split_axis=0, concat_axis=0, tiled=True)

    bases_t, products = call(
        products_kernel,
        (shape((model, flat), BF), shape((flat, edge_count), BF)),
        count=2,
        us=4,
        far_out=(0, 1),
    )(gathered, bases_flat)
    coef_part = call(
        coef_kernel,
        shape((dom_count, padded, relations), BF),
        smem=(0, 1),
        scratch=[pltpu.VMEM((padded, edge_count), F32), pltpu.VMEM((quarter, edge_count), F32), pltpu.VMEM((flat, edge_count), BF), pltpu.SemaphoreType.DMA((1,))],
        raw=(3,),
        count=6,
        us=4,
        far=(0, 1),
    )(owners, valid, nodes, products, rel, dst)
    coefs = lax.all_to_all(coef_part, "dom", split_axis=0, concat_axis=0, tiled=True)
    grads, slot_grads = call(
        grads_kernel,
        (shape((dom_count, quarter, edge_count), BF), shape((dom_count, quarter, slot_cap), BF)),
        smem=(0,),
        scratch=[
            pltpu.VMEM((dom_count, quarter, entities), BF),
            pltpu.VMEM((2, slot_cap, edge_count), BF),
        ],
        count=4,
        us=6,
        far=(0, 1, 2),
        far_out=(0,),
    )(owner_list, targets, ranks, nodes)
    sent = call(
        scatter_kernel,
        shape((feat_count, quarter, entities + LANES), BF),
        scratch=[
            pltpu.VMEM((model, entities), F32),
            pltpu.VMEM((model, flat), BF),
            pltpu.SemaphoreType.DMA((1,)),
        ],
        raw=(3,),
        count=7,
        us=5,
    )(slot_grads, slot_rows, slot_mix, bases_t, weight_t, grad_pre, coefs)
    arrived = lax.all_to_all(sent, "feat", split_axis=0, concat_axis=0, tiled=True)
    grad_bases, grad_self = call(
        functools.partial(weights_kernel, scale),
        (shape((flat, model), F32), shape((quarter, model), F32)),
        smem=(0,),
        count=5 + feat_count,
        us=12,
        far=(0,),
        raw=(1, 2, 3),
        scratch=[
            pltpu.VMEM((dom_count, padded, edge_count), F32),
            pltpu.VMEM((dom_count, quarter, edge_count), BF),
            pltpu.VMEM((model, dom_count * entities), BF),
            pltpu.SemaphoreType.DMA((3,)),
        ],
    )(place, mix, grads, full, nodes, *rows)
    grad_feats, coef_total = call(
        functools.partial(finish_kernel, padded, scale),
        (shape((quarter, entities), BF), shape((basis_count, relation_count), F32)),
        count=1,
        us=1,
    )(arrived)
    return (
        output,
        grad_feats,
        grad_bases.reshape(basis_count, quarter, model),
        grad_self.T,
        coef_total.T,
    )


def solution(mesh):
    def body(*arrays):
        dom_count = lax.axis_size("dom")
        edge_count = arrays[5].shape[0]
        feat_count = lax.axis_size("feat")
        few = dom_count * edge_count <= 1 << 14 and dom_count % feat_count == 0
        if not few:
            return body_many(*arrays)
        return body_few(*arrays)

    return jax.shard_map(
        body,
        mesh=mesh,
        in_specs=(
            P("feat", "dom"),
            P(None, "feat"),
            P(None, "feat", None),
            P(),
            P("dom", None),
            P("dom"),
            P("dom"),
            P("dom"),
            P("dom", None),
            P("dom", None),
            P("feat", "dom"),
        ),
        out_specs=(P("feat", "dom"), P("feat", "dom"), P(None, "feat", None), P(None, "feat"), P()),
        check_vma=False,
    )
```

```python
import functools

import jax
import jax.numpy as jnp
from jax import lax
from jax.experimental import pallas as pl
from jax.experimental.pallas import tpu as pltpu
from jax.sharding import PartitionSpec as P


BF = jnp.bfloat16
F32 = jnp.float32
I32 = jnp.int32
LANES = 128
NN = (((1,), (0,)), ((), ()))
NT = (((1,), (1,)), ((), ()))


def iota(shape, dim):
    return lax.broadcasted_iota(I32, shape, dim)


def hot(mask):
    return jnp.where(mask, 1.0, 0.0).astype(BF)


def dot(left, right, dims=NN):
    return lax.dot_general(left, right, dims, preferred_element_type=F32)


def call(
    kernel, out_shape, smem=(), scratch=(), count=0, us=4, far=(), far_out=(), raw=(), raw_out=()
):
    specs = [
        pl.BlockSpec(
            memory_space=pltpu.SMEM if k in smem else pltpu.HBM if k in raw else pltpu.VMEM
        )
        for k in range(count)
    ]
    single = not isinstance(out_shape, (tuple, list))
    shapes = (out_shape,) if single else tuple(out_shape)
    shapes = tuple(
        pltpu.HBM(o.shape, o.dtype) if k in far_out else o for k, o in enumerate(shapes)
    )
    outs = tuple(
        pl.BlockSpec(memory_space=pltpu.HBM if k in raw_out else pltpu.VMEM)
        for k in range(len(shapes))
    )
    run = pl.pallas_call(
        kernel,
        out_shape=shapes[0] if single else shapes,
        in_specs=specs,
        out_specs=outs[0] if single else outs,
        scratch_shapes=scratch,
        compiler_params=pltpu.CompilerParams(vmem_limit_bytes=24 << 20),
        cost_estimate=pl.CostEstimate(
            flops=us * 1_000_000_000, bytes_accessed=1 << 20, transcendentals=0
        ),
    )

    def apply(*arrays):
        return run(
            *(
                pltpu.with_memory_space_constraint(a, pltpu.HBM) if k in far or k in raw else a
                for k, a in enumerate(arrays)
            )
        )

    return apply


def block_slots(owners, block_count, block_cap):
    slots = []
    for j in range(block_count):
        rank = jnp.int32(0)
        for k in range(j):
            rank = rank + jnp.where(owners[k] == owners[j], 1, 0)
        slots.append(owners[j] * block_cap + rank)
    return slots


def each(count, step):
    if count <= 8:
        for k in range(count):
            step(k)
    else:
        lax.fori_loop(0, count, lambda k, c: (step(k), c)[1], 0)


def plan_kernel(
    entities, slot_cap, block_cap, owners, valid, part, row, dst, send, slot_out, hot_scratch
):
    dom_count = send.shape[0]
    edge_count = part.shape[1]
    block_count = dst.shape[0]
    chunks = slot_cap // LANES
    before = hot(iota((LANES, LANES), 0) < iota((LANES, LANES), 1))
    ones = jnp.ones((LANES, LANES), BF)
    offset = jnp.zeros((dom_count, LANES), F32)
    for c in range(edge_count // LANES):
        lanes = slice(c * LANES, (c + 1) * LANES)
        here = part[:, lanes]
        mask = iota((dom_count, LANES), 0) == here
        chosen = hot(mask)
        rank = jnp.sum(jnp.where(mask, dot(chosen, before) + offset, 0.0), axis=0, keepdims=True)
        offset = offset + dot(chosen, ones)
        slot_out[:, lanes] = here * slot_cap + rank.astype(I32)
    rows = row[...]
    digits = jnp.concatenate(
        [
            (rows >> 8).astype(F32),
            (rows & 255).astype(F32),
            jnp.ones((1, edge_count), F32),
            jnp.zeros((13, edge_count), F32),
        ],
        axis=0,
    ).astype(BF)

    def ask(p):
        near = slot_out[...] - p * slot_cap
        hot_scratch[...] = hot(iota((slot_cap, edge_count), 0) == near)
        found = dot(digits, hot_scratch[...], NT)
        wanted = found[0:1] * 256.0 + found[1:2] + (1.0 - found[2:3]) * float(entities)
        wanted = wanted.astype(I32)
        for k in range(chunks):
            send[p, k : k + 1, :] = wanted[:, k * LANES : (k + 1) * LANES]
        for t in range(block_cap):
            send[p, chunks + t : chunks + t + 1, :] = jnp.full((1, LANES), entities, I32)

    each(dom_count, ask)
    for j in range(block_count):
        rank = jnp.int32(0)
        for k in range(j):
            rank = rank + jnp.where(owners[k] == owners[j], 1, 0)
        live = iota((1, LANES), 1) < valid[j]
        send[owners[j], pl.ds(chunks + rank, 1), :] = jnp.where(live, dst[j : j + 1, :], entities)


def asked_row(arrived, g, chunks):
    rows = [arrived[g, k : k + 1, :] for k in range(chunks)]
    return rows[0] if chunks == 1 else jnp.concatenate(rows, axis=1)


def serve_kernel(slot_cap, arrived, feats, served):
    chunks = slot_cap // LANES
    entities = feats.shape[1]

    def step(g):
        asked = asked_row(arrived, g, chunks)
        chosen = hot(iota((entities, slot_cap), 0) == asked)
        served[g] = dot(feats[...], chosen).astype(BF)

    each(served.shape[0], step)


def unslot_kernel(fetched, slot, feats, out, total):
    dom_count, _, slot_cap = fetched.shape
    edge_count = slot.shape[1]
    total[...] = jnp.zeros_like(total)

    def step(p):
        near = slot[...] - p * slot_cap
        chosen = hot(iota((slot_cap, edge_count), 0) == near)
        total[...] += dot(fetched[p], chosen)

    each(dom_count, step)
    out[:, :edge_count] = total[...].astype(BF)
    out[:, edge_count:] = feats[...]


def rel_hot(rel, width):
    return hot(iota((width, rel.shape[1]), 0) == rel)


def forward_kernel(block_cap, owners, gathered, bases, coef, rel, send, weights):
    _, quarter, rows = send.shape
    edge_count = rel.shape[1]
    block_count = edge_count // rows
    basis_count = bases.shape[0] // quarter
    span = 2 * rows if block_count % 2 == 0 else rows
    group = 5
    send[...] = jnp.zeros_like(send)
    table = coef[...]
    high = table.astype(BF)
    rest = table - high.astype(F32)
    middle = rest.astype(BF)
    low = (rest - middle.astype(F32)).astype(BF)
    where = block_slots(owners, block_count, block_cap)
    for t in range(edge_count // span):
        lanes = slice(t * span, (t + 1) * span)
        chosen = rel_hot(rel[:, lanes], coef.shape[1])
        mix = dot(high, chosen) + dot(middle, chosen) + dot(low, chosen)
        weights[:, lanes] = mix
        x = gathered[:, lanes]
        total = jnp.zeros((quarter, span), F32)
        for c in range(0, basis_count, group):
            stop = min(c + group, basis_count)
            products = dot(bases[c * quarter : stop * quarter, :], x)
            for b in range(c, stop):
                part = products[(b - c) * quarter : (b - c + 1) * quarter]
                total = total + mix[b : b + 1, :] * part
        total = total.astype(BF)
        for k in range(span // rows):
            send[where[t * (span // rows) + k]] = total[:, k * rows : (k + 1) * rows]


def owner_kernel(
    slot_cap, block_cap, arrived, received, gathered, weight, cotangent, output, back, grad_pre, hots, flat
):
    slots, quarter, rows = received.shape
    entities = cotangent.shape[1]
    chunks = slot_cap // LANES
    width = slots * rows
    for s in range(slots):
        lanes = slice(s * rows, (s + 1) * rows)
        target = arrived[s // block_cap, chunks + s % block_cap : chunks + s % block_cap + 1, :]
        hots[:, lanes] = hot(iota((entities, rows), 0) == target)
        flat[:quarter, lanes] = received[s]
    flat[quarter:, :] = jnp.ones((16, width), BF)
    own = gathered[:, gathered.shape[1] - entities :]
    own_part = lax.dot_general(
        weight[...], own, (((0,), (0,)), ((), ())), preferred_element_type=F32
    )
    sums = dot(flat[...], hots[...], NT)
    inverse = 1.0 / jnp.maximum(sums[quarter : quarter + 1], 1.0)
    preact = own_part + inverse * sums[:quarter]
    gate = jax.nn.sigmoid(preact)
    output[...] = (preact * gate).astype(BF)
    pre = (cotangent[...].astype(F32) * gate * (1.0 + preact * (1.0 - gate))).astype(BF)
    grad_pre[...] = pre
    scaled = (inverse * pre.astype(F32)).astype(BF)
    for s in range(slots):
        back[s] = dot(scaled, hots[:, s * rows : (s + 1) * rows]).astype(BF)


def fill_combined(where, returned, weights, combined, basis_count):
    quarter, rows = returned.shape[1:]
    for j, slot in enumerate(where):
        lanes = slice(j * rows, (j + 1) * rows)
        grad = returned[slot].astype(F32)
        for b in range(basis_count):
            combined[b * quarter : (b + 1) * quarter, lanes] = (
                weights[b : b + 1, lanes] * grad
            ).astype(BF)


def bases_kernel(block_cap, owners, returned, gathered, weights, grad_pre, out, combined):
    quarter, rows = returned.shape[1:]
    edge_count = weights.shape[1]
    total = combined.shape[0]
    where = block_slots(owners, edge_count // rows, block_cap)
    fill_combined(where, returned, weights, combined, total // quarter)
    x = gathered[:, :edge_count]
    chunk = 5 * quarter
    for start in range(0, total, chunk):
        stop = min(start + chunk, total)
        out[start:stop, :] = dot(combined[start:stop, :], x, NT).astype(BF)
    own = gathered[:, edge_count:]
    out[total : total + quarter, :] = dot(grad_pre[...], own, NT).astype(BF)
    out[total + quarter :, :] = jnp.zeros((out.shape[0] - total - quarter, out.shape[1]), BF)


def edges_kernel(
    block_cap, owners, returned, gathered, weights, grad_pre, bases, bases_t, weight, rel, out, combined, scaled
):
    quarter, rows = returned.shape[1:]
    edge_count = weights.shape[1]
    entities = grad_pre.shape[1]
    total = combined.shape[0]
    basis_count = total // quarter
    padded = weights.shape[0]
    relations = 2 * LANES
    where = block_slots(owners, edge_count // rows, block_cap)
    fill_combined(where, returned, weights, combined, basis_count)
    peers = out.shape[0]
    share = out.shape[1]
    span = 2 * rows if (edge_count // rows) % 2 == 0 else rows
    scaled[...] = jnp.zeros_like(scaled)
    for t in range(edge_count // span):
        lanes = slice(t * span, (t + 1) * span)
        partial = dot(bases_t[...], combined[:, lanes]).astype(BF)
        for f in range(peers):
            out[f, :, lanes] = partial[f * share : (f + 1) * share]
        x = gathered[:, lanes]
        count = span // rows
        grad = [returned[where[t * count + k]].astype(F32) for k in range(count)]
        grad = grad[0] if count == 1 else jnp.concatenate(grad, axis=1)
        group = 5
        for c in range(0, basis_count, group):
            stop = min(c + group, basis_count)
            products = dot(bases[c * quarter : stop * quarter, :], x)
            for b in range(c, stop):
                part = products[(b - c) * quarter : (b - c + 1) * quarter]
                scaled[b : b + 1, lanes] = jnp.sum(part * grad, axis=0, keepdims=True)
    high = scaled[...].astype(BF)
    low = (scaled[...] - high.astype(F32)).astype(BF)
    chosen = rel_hot(rel[...], relations)
    coef = (dot(high, chosen, NT) + dot(low, chosen, NT)).astype(BF)
    own = dot(weight[...], grad_pre[...]).astype(BF)
    tail = edge_count + entities
    for f in range(peers):
        out[f, :, edge_count:tail] = own[f * share : (f + 1) * share]
        out[f, :padded, tail:] = coef[:, :LANES]
        out[f, padded : 2 * padded, tail:] = coef[:, LANES:]


def slots_kernel(padded, arrived, slot, out, own):
    peers, share, _ = arrived.shape
    dom_count, _, slot_cap = out.shape
    edge_count = slot.shape[1]
    entities = own.shape[1]
    sums = arrived[0].astype(F32)
    for f in range(1, peers):
        sums = sums + arrived[f].astype(F32)
    own[...] = sums[:, edge_count : edge_count + entities]
    edges = sums[:, :edge_count].astype(BF)
    coef = sums[: 2 * padded, edge_count + entities :].astype(BF)

    def step(p):
        near = slot[...] - p * slot_cap
        chosen = hot(iota((slot_cap, edge_count), 0) == near)
        out[p, :share, :] = dot(edges, chosen, NT).astype(BF)
        if slot_cap >= 2 * LANES:
            out[p, share:, :LANES] = coef[:padded]
            out[p, share:, LANES : 2 * LANES] = coef[padded:]
        else:
            out[p, share:, :] = coef

    each(dom_count, step)


def feats_kernel(slot_cap, padded, scale, arrived, asked, own, out, coef, total):
    dom_count, _, _ = arrived.shape
    share, entities = own.shape
    chunks = slot_cap // LANES
    total[...] = own[...]
    coef[...] = jnp.zeros_like(coef)

    def step(g):
        chosen = hot(iota((entities, slot_cap), 0) == asked_row(asked, g, chunks))
        total[...] += dot(arrived[g, :share, :], chosen, NT)
        if slot_cap >= 2 * LANES:
            coef[...] += arrived[g, share:, : 2 * LANES].astype(F32)
        else:
            coef[:, :LANES] += arrived[g, share : share + padded, :].astype(F32)
            coef[:, LANES:] += arrived[g, share + padded :, :].astype(F32)

    each(dom_count, step)
    out[...] = total[...].astype(BF)
    coef[...] = coef[...] * scale


def reduce_kernel(scale, parts, out):
    sums = parts[0].astype(F32)
    for k in range(1, parts.shape[0]):
        sums = sums + parts[k].astype(F32)
    out[...] = (sums * scale).astype(BF)


def body_many(
    feats,
    self_weight,
    bases,
    coef,
    src_part,
    src_row,
    edge_dst,
    edge_rel,
    block_owner,
    block_valid,
    cotangent,
):
    dom_count = lax.axis_size("dom")
    feat_count = lax.axis_size("feat")
    quarter, entities = feats.shape
    edge_count = src_row.shape[0]
    block_count = block_valid.shape[1]
    rows = edge_count // block_count
    slot_cap = LANES * ((2 * edge_count + LANES * dom_count - 1) // (LANES * dom_count))
    block_cap = (2 * block_count + dom_count - 1) // dom_count
    basis_count, _, model = bases.shape
    relation_count = coef.shape[0]
    flat = basis_count * quarter
    padded = 8 * ((basis_count + 7) // 8)
    padded = 16 * ((padded + 15) // 16)
    shape = jax.ShapeDtypeStruct
    scale = float(edge_count * dom_count) ** (-0.5)

    owners = block_owner[:, 0]
    valid = block_valid[0]
    rel = edge_rel.reshape(1, edge_count)
    bases_flat = bases.reshape(flat, model)
    coef_t = jnp.zeros((padded, 2 * LANES), F32).at[:basis_count, :relation_count].set(coef.T)

    height = slot_cap // LANES + block_cap
    send, slot = call(
        functools.partial(plan_kernel, entities, slot_cap, block_cap),
        (shape((dom_count, height, LANES), I32), shape((1, edge_count), I32)),
        smem=(0, 1),
        scratch=[pltpu.VMEM((slot_cap, edge_count), BF)],
        count=5,
    )(
        owners,
        valid,
        src_part.reshape(1, edge_count),
        src_row.reshape(1, edge_count),
        edge_dst.reshape(block_count, rows),
    )
    arrived = lax.all_to_all(send, "dom", split_axis=0, concat_axis=0, tiled=True)
    served = call(
        functools.partial(serve_kernel, slot_cap),
        shape((dom_count, quarter, slot_cap), BF),
        count=2,
    )(arrived, feats)
    fetched = lax.all_to_all(served, "dom", split_axis=0, concat_axis=0, tiled=True)
    mine = call(
        unslot_kernel,
        shape((quarter, edge_count + entities), BF),
        scratch=[pltpu.VMEM((quarter, edge_count), F32)],
        count=3,
    )(fetched, slot, feats)
    gathered = lax.all_gather(mine, "feat", axis=0, tiled=True)

    messages, weights = call(
        functools.partial(forward_kernel, block_cap),
        (shape((dom_count * block_cap, quarter, rows), BF), shape((padded, edge_count), F32)),
        smem=(0,),
        count=5,
    )(owners, gathered, bases_flat, coef_t, rel)
    received = lax.all_to_all(messages, "dom", split_axis=0, concat_axis=0, tiled=True)
    total_slots = dom_count * block_cap * rows
    output, back, grad_pre = call(
        functools.partial(owner_kernel, slot_cap, block_cap),
        (
            shape((quarter, entities), BF),
            shape((dom_count * block_cap, quarter, rows), BF),
            shape((quarter, entities), BF),
        ),
        scratch=[pltpu.VMEM((entities, total_slots), BF), pltpu.VMEM((quarter + 16, total_slots), BF)],
        count=5,
    )(arrived, received, gathered, self_weight, cotangent)
    returned = lax.all_to_all(back, "dom", split_axis=0, concat_axis=0, tiled=True)

    unit = 16 * dom_count
    tall = unit * ((flat + quarter + unit - 1) // unit)
    bases_part = call(
        functools.partial(bases_kernel, block_cap),
        shape((tall, model), BF),
        smem=(0,),
        scratch=[pltpu.VMEM((flat, edge_count), BF)],
        count=5,
    )(owners, returned, gathered, weights, grad_pre)
    parts = lax.all_to_all(
        bases_part.reshape(dom_count, tall // dom_count, model),
        "dom",
        split_axis=0,
        concat_axis=0,
        tiled=True,
    )
    edge_part = call(
        functools.partial(edges_kernel, block_cap),
        shape((feat_count, quarter, edge_count + entities + LANES), BF),
        smem=(0,),
        scratch=[pltpu.VMEM((flat, edge_count), BF), pltpu.VMEM((padded, edge_count), F32)],
        count=9,
    )(owners, returned, gathered, weights, grad_pre, bases_flat, bases_flat.T, self_weight, rel)
    edge_sum = lax.all_to_all(edge_part, "feat", split_axis=0, concat_axis=0, tiled=True)
    extra = padded * 2 * LANES // min(slot_cap, 2 * LANES)
    slot_grads, own_grads = call(
        functools.partial(slots_kernel, padded),
        (shape((dom_count, quarter + extra, slot_cap), BF), shape((quarter, entities), F32)),
        count=2,
    )(edge_sum, slot)
    arrived_grads = lax.all_to_all(slot_grads, "dom", split_axis=0, concat_axis=0, tiled=True)
    reduced = call(
        functools.partial(reduce_kernel, scale), shape((tall // dom_count, model), BF), count=1
    )(parts)
    near = [[2 * k, 2 * k + 1] for k in range(dom_count // 2)]
    far = [[2 * k + side for k in range(dom_count // 2)] for side in range(2)]
    pair = lax.all_gather(reduced, "dom", axis=0, tiled=True, axis_index_groups=near)
    whole = lax.all_gather(pair, "dom", axis=0, tiled=True, axis_index_groups=far)
    grad_feats, coef_total = call(
        functools.partial(feats_kernel, slot_cap, padded, scale),
        (shape((quarter, entities), BF), shape((padded, 2 * LANES), F32)),
        scratch=[pltpu.VMEM((quarter, entities), F32)],
        count=3,
    )(arrived_grads, arrived, own_grads)
    return (
        output,
        grad_feats,
        whole[:flat].astype(F32).reshape(basis_count, quarter, model),
        whole[flat : flat + quarter].astype(F32).T,
        coef_total[:basis_count, :relation_count].T,
    )


def pack_kernel(owners, valid, feats, part, row, dst, rel, out):
    copies = out.shape[0]
    quarter, entities = feats.shape
    blocks = part.shape[0]
    owner = jnp.zeros((blocks, LANES), I32)
    live = jnp.zeros((blocks, LANES), I32)
    for j in range(blocks):
        here = iota((blocks, LANES), 0) == j
        owner = jnp.where(here, owners[j], owner)
        live = jnp.where(here, valid[j], live)
    target = jnp.where(iota((blocks, LANES), 1) < live, dst[...], entities)
    digits = [
        part[...],
        row[...] >> 8,
        row[...] & 255,
        owner,
        target >> 8,
        target & 255,
        rel[...] >> 8,
        rel[...] & 255,
    ]
    digits = jnp.concatenate([d.astype(F32) for d in digits], axis=0).astype(BF)
    chunks = entities // LANES
    for k in range(copies):
        for c in range(chunks):
            out[k, c * quarter : (c + 1) * quarter, :] = feats[:, c * LANES : (c + 1) * LANES]
        out[k, chunks * quarter :, :] = digits


def source_kernel(
    shared, feats, part, row, mine, wide, ids, spans, targets, rels, owners, total, hots
):
    dom_count = shared.shape[0]
    quarter, entities = feats.shape
    blocks = part.shape[0]
    chunks = entities // LANES
    edge_count = blocks * LANES
    for g in range(dom_count):
        for c in range(chunks):
            start = g * entities + c * LANES
            wide[:, start : start + LANES] = shared[g, c * quarter : (c + 1) * quarter, :]
        digits = shared[g, chunks * quarter :, :].astype(F32).astype(I32)
        piece = [digits[d * blocks : (d + 1) * blocks] for d in range(8)]
        at = piece[0] * entities + piece[1] * 256 + piece[2]
        ids[g] = at
        for t in range(blocks // 2):
            spans[g * (blocks // 2) + t] = jnp.concatenate(
                [at[2 * t : 2 * t + 1], at[2 * t + 1 : 2 * t + 2]], axis=1
            )
        owners[g] = piece[3]
        targets[g] = piece[4] * 256 + piece[5]
        rels[g] = piece[6] * 256 + piece[7]
    total[...] = jnp.zeros_like(total)
    for p in range(dom_count):
        near = jnp.where(part[...] == p, row[...], -1)
        for j in range(blocks):
            hots[:, j * LANES : (j + 1) * LANES] = hot(
                iota((entities, LANES), 0) == near[j : j + 1, :]
            )
        total[...] += dot(wide[:, p * entities : (p + 1) * entities], hots[...])
    mine[:, :edge_count] = total[...].astype(BF)
    mine[:, edge_count:] = feats[...]


def split3(table):
    high = table.astype(BF)
    rest = table - high.astype(F32)
    middle = rest.astype(BF)
    low = (rest - middle.astype(F32)).astype(BF)
    return high, middle, low


def message_kernel(block_cap, entities, owners, valid, gathered, bases, coef, rel, dst, send):
    slots, tall, rows = send.shape
    blocks = rel.shape[0]
    quarter = tall - 16
    basis_count = bases.shape[0] // quarter
    group = 5
    first = iota((16, rows), 0)
    empty = jnp.where(first == 0, entities >> 8, jnp.where(first == 1, entities & 255, 0))
    empty = empty.astype(F32).astype(BF)
    for s in range(slots):
        send[s, :quarter, :] = jnp.zeros((quarter, rows), BF)
        send[s, quarter:, :] = empty
    parts = split3(coef[...])
    where = block_slots(owners, blocks, block_cap)
    for t in range(blocks // 2):
        lanes = slice(2 * t * rows, 2 * (t + 1) * rows)
        both = jnp.concatenate([rel[2 * t : 2 * t + 1, :], rel[2 * t + 1 : 2 * t + 2, :]], axis=1)
        chosen = rel_hot(both, coef.shape[1])
        mix = sum(dot(p, chosen) for p in parts)
        x = gathered[:, lanes]
        total = jnp.zeros((quarter, 2 * rows), F32)
        for c in range(0, basis_count, group):
            stop = min(c + group, basis_count)
            products = dot(bases[c * quarter : stop * quarter, :], x)
            for b in range(c, stop):
                part = products[(b - c) * quarter : (b - c + 1) * quarter]
                total = total + mix[b : b + 1, :] * part
        total = total.astype(BF)
        for k in range(2):
            j = 2 * t + k
            slot = where[j]
            live = iota((1, rows), 1) < valid[j]
            target = jnp.where(live, dst[j : j + 1, :], entities)
            code = jnp.where(first == 0, target >> 8, jnp.where(first == 1, target & 255, 0))
            send[slot, :quarter, :] = total[:, k * rows : (k + 1) * rows]
            send[slot, quarter:, :] = code.astype(F32).astype(BF)


def node_kernel(received, gathered, weight, cotangent, output, share, grad_pre, hots, flat):
    slots, _, rows = received.shape
    quarter, entities = cotangent.shape
    copies = share.shape[0]
    for s in range(slots):
        lanes = slice(s * rows, (s + 1) * rows)
        code = received[s, quarter:, :].astype(F32).astype(I32)
        target = code[0:1] * 256 + code[1:2]
        hots[:, lanes] = hot(iota((entities, rows), 0) == target)
        flat[:quarter, lanes] = received[s, :quarter, :]
    flat[quarter:, :] = jnp.ones((16, slots * rows), BF)
    own = gathered[:, gathered.shape[1] - entities :]
    own_part = dot(weight[...], own)
    sums = dot(hots[...], flat[...], NT).T
    count = sums[quarter : quarter + 1]
    inverse = 1.0 / jnp.maximum(count, 1.0)
    preact = own_part + inverse * sums[:quarter]
    gate = jax.nn.sigmoid(preact)
    output[...] = (preact * gate).astype(BF)
    pre = (cotangent[...].astype(F32) * gate * (1.0 + preact * (1.0 - gate))).astype(BF)
    grad_pre[...] = pre
    whole = count.astype(I32)
    first = iota((16, entities), 0)
    code = jnp.where(first == 0, whole >> 8, jnp.where(first == 1, whole & 255, 0))
    code = code.astype(F32).astype(BF)
    for k in range(copies):
        share[k, :quarter, :] = pre
        share[k, quarter:, :] = code


def scaled_grad(shared, q, quarter):
    code = shared[q, quarter:, :].astype(F32)
    count = code[0:1] * 256.0 + code[1:2]
    inverse = 1.0 / jnp.maximum(count, 1.0)
    return (inverse * shared[q, :quarter, :].astype(F32)).astype(BF)


def rows_of_edges_kernel(entities, place, spans, *refs):
    pieces, out, full = refs[:-2], refs[-2], refs[-1]
    count, width, model = out.shape
    quarter = pieces[0].shape[0]
    for k, piece in enumerate(pieces):
        full[pl.ds(pl.multiple_of(place[k] * quarter, quarter), quarter), :] = piece[...]

    def step(n, carry):
        row = spans[place[0] * count + n]
        total = jnp.zeros((model, width), F32)
        for start in range(0, full.shape[1], entities):
            chosen = hot(iota((entities, width), 0) == row - start)
            total = total + dot(full[:, start : start + entities], chosen)
        out[n] = total.T.astype(BF)
        return carry

    lax.fori_loop(0, count, step, 0)


def rank_kernel(
    slot_cap, entities, me, ids, rels, coef, ranks, slot_rows, slot_mix, mix, comp, digits, hots
):
    dom_count, blocks, _ = ids.shape
    before = hot(iota((LANES, LANES), 0) < iota((LANES, LANES), 1))
    ones = jnp.ones((LANES, LANES), BF)
    table = coef[...].astype(BF)

    def step(g, carry):
        near = ids[g] - me[0] * entities
        mask = (near >= 0) & (near < entities)
        chosen = jnp.where(mask, 1.0, 0.0)
        chosen = jnp.concatenate([chosen, jnp.zeros_like(chosen)], axis=0).astype(BF)
        inside = dot(chosen, before)[:blocks]
        totals = dot(chosen, ones)[:blocks]
        offset = jnp.zeros((1, LANES), F32)
        offsets = []
        for j in range(blocks):
            offsets.append(offset)
            offset = offset + totals[j : j + 1]
        rank = inside + jnp.concatenate(offsets, axis=0)
        rank = jnp.where(mask, rank.astype(I32), -1)
        ranks[g] = rank
        rel = rels[g]
        rows = jnp.where(mask, near, 0)
        first = iota((16, LANES), 0)
        for j in range(blocks):
            lanes = slice(j * LANES, (j + 1) * LANES)
            comp[:, lanes] = hot(iota((slot_cap, LANES), 0) == rank[j : j + 1, :])
            at, kind = rows[j : j + 1, :], rel[j : j + 1, :]
            code = jnp.where(first == 0, at >> 8, jnp.where(first == 1, at & 255, 0))
            code = code + jnp.where(first == 2, kind >> 8, jnp.where(first == 3, kind & 255, 0))
            digits[:, lanes] = code.astype(F32).astype(BF)
            hots[:, lanes] = rel_hot(kind, coef.shape[1])
        mix[g] = dot(table, hots[...])
        found = dot(digits[...], comp[...], NT)
        slot_rows[g] = (found[0:1] * 256.0 + found[1:2]).astype(I32)
        kind = (found[2:3] * 256.0 + found[3:4]).astype(I32)
        slot_mix[g] = dot(table, rel_hot(kind, coef.shape[1]))
        return carry

    lax.fori_loop(0, dom_count, step, 0)


def products_kernel(gathered, bases, bases_t, out):
    edge_count = out.shape[1]
    bases_t[...] = bases[...].T
    step = 320
    for start in range(0, out.shape[0], step):
        stop = min(start + step, out.shape[0])
        out[start:stop, :] = dot(bases[start:stop, :], gathered[:, :edge_count]).astype(BF)


def grads_kernel(
    owners,
    me,
    targets,
    ranks,
    shared,
    products_far,
    rel,
    grads,
    slot_grads,
    coef_out,
    node,
    comp,
    scaled,
    products,
    sems,
):
    fetched = fetch(((products_far, products),), sems)
    dom_count, blocks, _ = targets.shape
    slot_cap = comp.shape[2]
    entities = shared.shape[2]
    quarter = shared.shape[1] - 16
    copies, _, relations = coef_out.shape
    basis_count = products.shape[0] // quarter
    for q in range(dom_count):
        node[q] = scaled_grad(shared, q, quarter)
    for g in range(dom_count):
        rows = targets[g]
        rank = ranks[g].astype(F32).T.astype(I32)
        for j in range(0, blocks, 2):
            both = jnp.concatenate([rows[j : j + 1, :], rows[j + 1 : j + 2, :]], axis=1)
            chosen = hot(iota((entities, 2 * LANES), 0) == both)
            first, second = owners[g * blocks + j], owners[g * blocks + j + 1]
            pair = dot(jnp.concatenate([node[first], node[second]], axis=0), chosen).astype(BF)
            middle = (j + 1) * LANES
            grads[g, :, j * LANES : middle] = pair[:quarter, :LANES]
            grads[g, :, middle : middle + LANES] = pair[quarter:, LANES:]
        for j in range(blocks):
            lanes = slice(j * LANES, (j + 1) * LANES)
            comp[g % 2, lanes, :] = hot(iota((LANES, slot_cap), 1) == rank[:, j : j + 1])
        slot_grads[g] = dot(grads[g], comp[g % 2]).astype(BF)
    scaled[...] = jnp.zeros_like(scaled)
    fetched[0].wait()
    for t in range(blocks // 2):
        lanes = slice(2 * t * LANES, 2 * (t + 1) * LANES)
        grad = grads[me[0], :, lanes].astype(F32)
        for b in range(basis_count):
            part = products[b * quarter : (b + 1) * quarter, lanes].astype(F32)
            scaled[b : b + 1, lanes] = jnp.sum(part * grad, axis=0, keepdims=True)
    high = scaled[...].astype(BF)
    low = (scaled[...] - high.astype(F32)).astype(BF)
    kinds = jnp.concatenate([rel[j : j + 1, :] for j in range(blocks)], axis=1)
    chosen = rel_hot(kinds, relations)
    total = (dot(chosen, high, NT) + dot(chosen, low, NT)).T.astype(BF)
    for k in range(copies):
        coef_out[k] = total


def mix_rows(mix, grad, quarter):
    pieces = []
    for b in range(mix.shape[0]):
        wide = jnp.broadcast_to(mix[b : b + 1, :], (16, mix.shape[1])).astype(BF)
        for r in range(0, quarter, 16):
            pieces.append(wide * grad[r : r + 16])
    return jnp.concatenate(pieces, axis=0)


def column(row):
    return jnp.broadcast_to(row.astype(F32), (8, row.shape[1])).T[:, :1].astype(I32)


def scatter_kernel(
    slot_grads, slot_rows, slot_mix, bases_far, weight, grad_pre, out, total, bases_t, rows, sems
):
    copies = fetch(((bases_far, bases_t),), sems)
    dom_count, quarter, slot_cap = slot_grads.shape
    basis_count = bases_t.shape[1] // quarter
    entities = grad_pre.shape[1]
    peers = out.shape[0]
    total[...] = lax.dot_general(
        weight[...], grad_pre[...], (((0,), (0,)), ((), ())), preferred_element_type=F32
    )

    copies[0].wait()

    group = 4 if dom_count % 4 == 0 else 1
    for start in range(0, dom_count, group):
        part = range(start, start + group)
        mix = jnp.concatenate([slot_mix[g][:basis_count] for g in part], axis=1)
        grad = jnp.concatenate([slot_grads[g] for g in part], axis=1)
        partial = dot(bases_t[...], mix_rows(mix, grad, quarter)).astype(BF)
        for n, g in enumerate(part):
            chosen = hot(iota((slot_cap, entities), 1) == column(slot_rows[g]))
            rows[n * slot_cap : (n + 1) * slot_cap, :] = chosen
        total[...] += dot(partial, rows[: group * slot_cap, :])
    for f in range(peers):
        out[f] = total[f * quarter : (f + 1) * quarter].astype(BF)


def fetch(pairs, sems):
    copies = [
        pltpu.make_async_copy(source, target, sems.at[k]) for k, (source, target) in enumerate(pairs)
    ]
    for copy in copies:
        copy.start()
    return copies


def weights_kernel(scale, place, mix_far, grads_far, full_far, shared, *refs):
    rows, (out, own_out, total, mix, grads, full, sems, done) = refs[:-8], refs[-8:]
    dom_count, quarter, _ = grads.shape
    entities = shared.shape[2]
    basis_count = out.shape[0] // quarter
    group = 5
    count = rows[0].shape[0]
    order = [place[part] * count + k for part in range(len(rows)) for k in range(count)]
    pairs = []
    for n, g in enumerate(order):
        pairs += [(mix_far.at[g], mix.at[n]), (grads_far.at[g], grads.at[n])]
    copies = fetch(pairs + [(full_far, full)], sems)
    stores = []
    for n in range(dom_count):
        copies[2 * n].wait()
        copies[2 * n + 1].wait()
        grad = grads[n]
        for c in range(0, basis_count, group):
            stop = min(c + group, basis_count)
            lanes = slice(c * quarter, stop * quarter)
            sums = dot(mix_rows(mix[n, c:stop, :], grad, quarter), rows[n // count][n % count])
            if n > 0:
                sums = sums + total[lanes, :]
            if n == dom_count - 1:
                sums = sums * scale
            total[lanes, :] = sums
            if n == dom_count - 1:
                store = pltpu.make_async_copy(
                    total.at[lanes, :], out.at[lanes, :], done.at[c // group]
                )
                store.start()
                stores.append(store)
    copies[2 * dom_count].wait()
    own = jnp.zeros((full.shape[0], quarter), F32)
    for q in range(dom_count):
        lanes = slice(q * entities, (q + 1) * entities)
        own = own + dot(full[:, lanes], shared[q, :quarter, :], NT)
    own_out[...] = own.T * scale
    for store in stores:
        store.wait()


def merge_kernel(sums, coefs, out):
    peers, _, entities = sums.shape
    padded = coefs.shape[1]
    coef = coefs[0].astype(F32)
    for g in range(1, coefs.shape[0]):
        coef = coef + coefs[g].astype(F32)
    coef = coef.astype(BF)
    for f in range(peers):
        out[f, :, :entities] = sums[f]
        out[f, :padded, entities:] = coef[:, :LANES]
        out[f, padded:, entities:] = coef[:, LANES:]


def finish_kernel(padded, scale, arrived, grad_feats, coef_out):
    entities = grad_feats.shape[1]
    sums = arrived[0].astype(F32)
    for f in range(1, arrived.shape[0]):
        sums = sums + arrived[f].astype(F32)
    grad_feats[...] = sums[:, :entities].astype(BF)
    coef = jnp.concatenate([sums[:padded, entities:], sums[padded:, entities:]], axis=1)
    coef_out[...] = coef[: coef_out.shape[0], : coef_out.shape[1]] * scale


def body_few(
    feats,
    self_weight,
    bases,
    coef,
    src_part,
    src_row,
    edge_dst,
    edge_rel,
    block_owner,
    block_valid,
    cotangent,
):
    dom_count = lax.axis_size("dom")
    feat_count = lax.axis_size("feat")
    quarter, entities = feats.shape
    edge_count = src_row.shape[0]
    blocks = block_valid.shape[1]
    slot_cap = LANES * ((2 * edge_count + LANES * dom_count - 1) // (LANES * dom_count))
    block_cap = (2 * blocks + dom_count - 1) // dom_count
    basis_count, _, model = bases.shape
    relation_count = coef.shape[0]
    flat = basis_count * quarter
    padded = 16 * ((basis_count + 15) // 16)
    relations = 2 * LANES
    shape = jax.ShapeDtypeStruct
    scale = float(edge_count * dom_count) ** (-0.5)
    owners = block_owner[:, 0]
    valid = block_valid[0]
    part = src_part.reshape(blocks, LANES)
    row = src_row.reshape(blocks, LANES)
    dst = edge_dst.reshape(blocks, LANES)
    rel = edge_rel.reshape(blocks, LANES)
    bases_flat = bases.reshape(flat, model)
    weight_t = self_weight.T
    coef_t = jnp.zeros((padded, relations), F32).at[:basis_count, :relation_count].set(coef.T)
    dom_place = lax.axis_index("dom").astype(I32).reshape(1)
    feat_place = lax.axis_index("feat").astype(I32)

    tall = (entities // LANES) * quarter + 8 * blocks
    packed = call(
        pack_kernel,
        shape((1, tall, LANES), BF),
        smem=(0, 1),
        count=7,
        us=1,
        far=(0, 1, 2, 3, 4, 5, 6),
    )(
        owners, valid, feats, part, row, dst, rel
    )
    near = [[2 * k, 2 * k + 1] for k in range(dom_count // 2)]
    far = [[2 * k + side for k in range(dom_count // 2)] for side in range(2)]
    shared = lax.all_gather(packed, "dom", axis=0, tiled=True, axis_index_groups=near)
    shared = lax.all_gather(shared, "dom", axis=0, tiled=True, axis_index_groups=far)
    ints = shape((dom_count, blocks, LANES), I32)
    mine, wide, ids, spans, targets, rels, all_owners = call(
        source_kernel,
        (
            shape((quarter, edge_count + entities), BF),
            shape((quarter, dom_count * entities), BF),
            ints,
            shape((dom_count * blocks // 2, 1, 2 * LANES), I32),
            ints,
            ints,
            ints,
        ),
        scratch=[pltpu.VMEM((quarter, edge_count), F32), pltpu.VMEM((entities, edge_count), BF)],
        count=4,
        us=4,
        far_out=(3, 4, 6),
    )(shared, feats, part, row)
    gathered = lax.all_gather(mine, "feat", axis=0, tiled=True)
    owner_list = all_owners[:, :, 0].reshape(dom_count * blocks)

    def doubled(piece):
        pieces, bit, stage = [piece], feat_count // 2, 0
        while bit >= 1:
            links = [(f, f ^ bit) for f in range(feat_count)]
            pieces = pieces + [lax.ppermute(piece, "feat", links) for piece in pieces]
            bit //= 2
            stage += 1
        return pieces

    places, bit = [0], feat_count // 2
    while bit >= 1:
        places = places + [place ^ bit for place in places]
        bit //= 2
    place = jnp.stack([feat_place ^ k for k in places])
    wide, gathered = lax.optimization_barrier((wide, gathered))
    part_count = dom_count // feat_count
    rows, full = call(
        functools.partial(rows_of_edges_kernel, entities),
        (
            shape((part_count * blocks // 2, 2 * LANES, model), BF),
            shape((model, dom_count * entities), BF),
        ),
        smem=(0,),
        count=2 + feat_count,
        us=10,
        far=tuple(range(2 + feat_count)),
        far_out=(1,),
    )(place, spans, *doubled(wide))
    rows = doubled(rows.reshape(part_count, edge_count, model))
    ranks, slot_rows, slot_mix, mix = call(
        functools.partial(rank_kernel, slot_cap, entities),
        (
            ints,
            shape((dom_count, 1, slot_cap), I32),
            shape((dom_count, padded, slot_cap), F32),
            shape((dom_count, padded, edge_count), F32),
        ),
        smem=(0,),
        scratch=[
            pltpu.VMEM((slot_cap, edge_count), BF),
            pltpu.VMEM((16, edge_count), BF),
            pltpu.VMEM((relations, edge_count), BF),
        ],
        count=4,
        us=4,
        far=(0,),
        far_out=(0, 1, 2, 3),
    )(dom_place, ids, rels, coef_t)

    messages = call(
        functools.partial(message_kernel, block_cap, entities),
        shape((dom_count * block_cap, quarter + 16, LANES), BF),
        smem=(0, 1),
        count=7,
        us=4,
        far=(0, 1),
    )(owners, valid, gathered, bases_flat, coef_t, rel, dst)
    received = lax.all_to_all(messages, "dom", split_axis=0, concat_axis=0, tiled=True)
    slots = dom_count * block_cap
    output, share, grad_pre = call(
        node_kernel,
        (
            shape((quarter, entities), BF),
            shape((dom_count, quarter + 16, entities), BF),
            shape((quarter, entities), BF),
        ),
        scratch=[
            pltpu.VMEM((entities, slots * LANES), BF),
            pltpu.VMEM((quarter + 16, slots * LANES), BF),
        ],
        count=4,
        us=4,
        far_out=(2,),
    )(received, gathered, weight_t, cotangent)
    nodes = lax.all_to_all(share, "dom", split_axis=0, concat_axis=0, tiled=True)

    bases_t, products = call(
        products_kernel,
        (shape((model, flat), BF), shape((flat, edge_count), BF)),
        count=2,
        us=4,
        far_out=(0, 1),
    )(gathered, bases_flat)
    grads, slot_grads, coef_part = call(
        grads_kernel,
        (
            shape((dom_count, quarter, edge_count), BF),
            shape((dom_count, quarter, slot_cap), BF),
            shape((dom_count, padded, relations), BF),
        ),
        smem=(0, 1),
        scratch=[
            pltpu.VMEM((dom_count, quarter, entities), BF),
            pltpu.VMEM((2, edge_count, slot_cap), BF),
            pltpu.VMEM((padded, edge_count), F32),
            pltpu.VMEM((flat, edge_count), BF),
            pltpu.SemaphoreType.DMA((1,)),
        ],
        count=7,
        us=8,
        far=(0, 1, 2, 3),
        far_out=(0,),
        raw=(5,),
    )(owner_list, dom_place, targets, ranks, nodes, products, rel)
    coefs = lax.all_to_all(
        coef_part, "dom", split_axis=0, concat_axis=0, tiled=True
    )
    sums = call(
        scatter_kernel,
        shape((feat_count, quarter, entities), BF),
        scratch=[
            pltpu.VMEM((model, entities), F32),
            pltpu.VMEM((model, flat), BF),
            pltpu.VMEM((4 * slot_cap, entities), BF),
            pltpu.SemaphoreType.DMA((1,)),
        ],
        raw=(3,),
        far=(1, 2, 5),
        count=6,
        us=5,
    )(slot_grads, slot_rows, slot_mix, bases_t, weight_t, grad_pre)
    sent = call(
        merge_kernel, shape((feat_count, quarter, entities + LANES), BF), count=2, us=1
    )(sums, coefs)
    arrived = lax.all_to_all(sent, "feat", split_axis=0, concat_axis=0, tiled=True)
    grad_bases, grad_self = call(
        functools.partial(weights_kernel, scale),
        (shape((flat, model), F32), shape((quarter, model), F32)),
        smem=(0,),
        count=5 + feat_count,
        us=12,
        far=(0,),
        raw=(1, 2, 3),
        raw_out=(0,),
        scratch=[
            pltpu.VMEM((flat, model), F32),
            pltpu.VMEM((dom_count, padded, edge_count), F32),
            pltpu.VMEM((dom_count, quarter, edge_count), BF),
            pltpu.VMEM((model, dom_count * entities), BF),
            pltpu.SemaphoreType.DMA((2 * dom_count + 1,)),
            pltpu.SemaphoreType.DMA((basis_count,)),
        ],
    )(place, mix, grads, full, nodes, *rows)
    grad_feats, coef_total = call(
        functools.partial(finish_kernel, padded, scale),
        (shape((quarter, entities), BF), shape((basis_count, relation_count), F32)),
        count=1,
        us=1,
    )(arrived)
    return (
        output,
        grad_feats,
        grad_bases.reshape(basis_count, quarter, model),
        grad_self.T,
        coef_total.T,
    )


def solution(mesh):
    def body(*arrays):
        dom_count = lax.axis_size("dom")
        edge_count = arrays[5].shape[0]
        feat_count = lax.axis_size("feat")
        few = dom_count * edge_count <= 1 << 14 and dom_count % feat_count == 0
        if not few:
            return body_many(*arrays)
        return body_few(*arrays)

    return jax.shard_map(
        body,
        mesh=mesh,
        in_specs=(
            P("feat", "dom"),
            P(None, "feat"),
            P(None, "feat", None),
            P(),
            P("dom", None),
            P("dom"),
            P("dom"),
            P("dom"),
            P("dom", None),
            P("dom", None),
            P("feat", "dom"),
        ),
        out_specs=(P("feat", "dom"), P("feat", "dom"), P(None, "feat", None), P(None, "feat"), P()),
        check_vma=False,
    )
```

```python
import functools

import jax
import jax.numpy as jnp
from jax import lax
from jax.experimental import pallas as pl
from jax.experimental.pallas import tpu as pltpu
from jax.sharding import PartitionSpec as P


BF = jnp.bfloat16
F32 = jnp.float32
I32 = jnp.int32
LANES = 128
NN = (((1,), (0,)), ((), ()))
NT = (((1,), (1,)), ((), ()))


def iota(shape, dim):
    return lax.broadcasted_iota(I32, shape, dim)


def hot(mask):
    return jnp.where(mask, 1.0, 0.0).astype(BF)


def dot(left, right, dims=NN):
    return lax.dot_general(left, right, dims, preferred_element_type=F32)


def call(
    kernel, out_shape, smem=(), scratch=(), count=0, us=4, far=(), far_out=(), raw=(), raw_out=()
):
    specs = [
        pl.BlockSpec(
            memory_space=pltpu.SMEM if k in smem else pltpu.HBM if k in raw else pltpu.VMEM
        )
        for k in range(count)
    ]
    single = not isinstance(out_shape, (tuple, list))
    shapes = (out_shape,) if single else tuple(out_shape)
    shapes = tuple(
        pltpu.HBM(o.shape, o.dtype) if k in far_out else o for k, o in enumerate(shapes)
    )
    outs = tuple(
        pl.BlockSpec(memory_space=pltpu.HBM if k in raw_out else pltpu.VMEM)
        for k in range(len(shapes))
    )
    run = pl.pallas_call(
        kernel,
        out_shape=shapes[0] if single else shapes,
        in_specs=specs,
        out_specs=outs[0] if single else outs,
        scratch_shapes=scratch,
        compiler_params=pltpu.CompilerParams(vmem_limit_bytes=24 << 20),
        cost_estimate=pl.CostEstimate(
            flops=us * 1_000_000_000, bytes_accessed=1 << 20, transcendentals=0
        ),
    )

    def apply(*arrays):
        return run(
            *(
                pltpu.with_memory_space_constraint(a, pltpu.HBM) if k in far or k in raw else a
                for k, a in enumerate(arrays)
            )
        )

    return apply


def block_slots(owners, block_count, block_cap):
    slots = []
    for j in range(block_count):
        rank = jnp.int32(0)
        for k in range(j):
            rank = rank + jnp.where(owners[k] == owners[j], 1, 0)
        slots.append(owners[j] * block_cap + rank)
    return slots


def each(count, step):
    if count <= 8:
        for k in range(count):
            step(k)
    else:
        lax.fori_loop(0, count, lambda k, c: (step(k), c)[1], 0)


def plan_kernel(
    entities, slot_cap, block_cap, owners, valid, part, row, dst, send, slot_out, hot_scratch
):
    dom_count = send.shape[0]
    edge_count = part.shape[1]
    block_count = dst.shape[0]
    chunks = slot_cap // LANES
    before = hot(iota((LANES, LANES), 0) < iota((LANES, LANES), 1))
    ones = jnp.ones((LANES, LANES), BF)
    offset = jnp.zeros((dom_count, LANES), F32)
    for c in range(edge_count // LANES):
        lanes = slice(c * LANES, (c + 1) * LANES)
        here = part[:, lanes]
        mask = iota((dom_count, LANES), 0) == here
        chosen = hot(mask)
        rank = jnp.sum(jnp.where(mask, dot(chosen, before) + offset, 0.0), axis=0, keepdims=True)
        offset = offset + dot(chosen, ones)
        slot_out[:, lanes] = here * slot_cap + rank.astype(I32)
    rows = row[...]
    digits = jnp.concatenate(
        [
            (rows >> 8).astype(F32),
            (rows & 255).astype(F32),
            jnp.ones((1, edge_count), F32),
            jnp.zeros((13, edge_count), F32),
        ],
        axis=0,
    ).astype(BF)

    def ask(p):
        near = slot_out[...] - p * slot_cap
        hot_scratch[...] = hot(iota((slot_cap, edge_count), 0) == near)
        found = dot(digits, hot_scratch[...], NT)
        wanted = found[0:1] * 256.0 + found[1:2] + (1.0 - found[2:3]) * float(entities)
        wanted = wanted.astype(I32)
        for k in range(chunks):
            send[p, k : k + 1, :] = wanted[:, k * LANES : (k + 1) * LANES]
        for t in range(block_cap):
            send[p, chunks + t : chunks + t + 1, :] = jnp.full((1, LANES), entities, I32)

    each(dom_count, ask)
    for j in range(block_count):
        rank = jnp.int32(0)
        for k in range(j):
            rank = rank + jnp.where(owners[k] == owners[j], 1, 0)
        live = iota((1, LANES), 1) < valid[j]
        send[owners[j], pl.ds(chunks + rank, 1), :] = jnp.where(live, dst[j : j + 1, :], entities)


def asked_row(arrived, g, chunks):
    rows = [arrived[g, k : k + 1, :] for k in range(chunks)]
    return rows[0] if chunks == 1 else jnp.concatenate(rows, axis=1)


def serve_kernel(slot_cap, arrived, feats, served):
    chunks = slot_cap // LANES
    entities = feats.shape[1]

    def step(g):
        asked = asked_row(arrived, g, chunks)
        chosen = hot(iota((entities, slot_cap), 0) == asked)
        served[g] = dot(feats[...], chosen).astype(BF)

    each(served.shape[0], step)


def unslot_kernel(fetched, slot, feats, out, total):
    dom_count, _, slot_cap = fetched.shape
    edge_count = slot.shape[1]
    total[...] = jnp.zeros_like(total)

    def step(p):
        near = slot[...] - p * slot_cap
        chosen = hot(iota((slot_cap, edge_count), 0) == near)
        total[...] += dot(fetched[p], chosen)

    each(dom_count, step)
    out[:, :edge_count] = total[...].astype(BF)
    out[:, edge_count:] = feats[...]


def rel_hot(rel, width):
    return hot(iota((width, rel.shape[1]), 0) == rel)


def forward_kernel(block_cap, owners, gathered, bases, coef, rel, send, weights):
    _, quarter, rows = send.shape
    edge_count = rel.shape[1]
    block_count = edge_count // rows
    basis_count = bases.shape[0] // quarter
    span = 2 * rows if block_count % 2 == 0 else rows
    group = 5
    send[...] = jnp.zeros_like(send)
    table = coef[...]
    high = table.astype(BF)
    rest = table - high.astype(F32)
    middle = rest.astype(BF)
    low = (rest - middle.astype(F32)).astype(BF)
    where = block_slots(owners, block_count, block_cap)
    for t in range(edge_count // span):
        lanes = slice(t * span, (t + 1) * span)
        chosen = rel_hot(rel[:, lanes], coef.shape[1])
        mix = dot(high, chosen) + dot(middle, chosen) + dot(low, chosen)
        weights[:, lanes] = mix
        x = gathered[:, lanes]
        total = jnp.zeros((quarter, span), F32)
        for c in range(0, basis_count, group):
            stop = min(c + group, basis_count)
            products = dot(bases[c * quarter : stop * quarter, :], x)
            for b in range(c, stop):
                part = products[(b - c) * quarter : (b - c + 1) * quarter]
                total = total + mix[b : b + 1, :] * part
        total = total.astype(BF)
        for k in range(span // rows):
            send[where[t * (span // rows) + k]] = total[:, k * rows : (k + 1) * rows]


def owner_kernel(
    slot_cap, block_cap, arrived, received, gathered, weight, cotangent, output, back, grad_pre, hots, flat
):
    slots, quarter, rows = received.shape
    entities = cotangent.shape[1]
    chunks = slot_cap // LANES
    width = slots * rows
    for s in range(slots):
        lanes = slice(s * rows, (s + 1) * rows)
        target = arrived[s // block_cap, chunks + s % block_cap : chunks + s % block_cap + 1, :]
        hots[:, lanes] = hot(iota((entities, rows), 0) == target)
        flat[:quarter, lanes] = received[s]
    flat[quarter:, :] = jnp.ones((16, width), BF)
    own = gathered[:, gathered.shape[1] - entities :]
    own_part = lax.dot_general(
        weight[...], own, (((0,), (0,)), ((), ())), preferred_element_type=F32
    )
    sums = dot(flat[...], hots[...], NT)
    inverse = 1.0 / jnp.maximum(sums[quarter : quarter + 1], 1.0)
    preact = own_part + inverse * sums[:quarter]
    gate = jax.nn.sigmoid(preact)
    output[...] = (preact * gate).astype(BF)
    pre = (cotangent[...].astype(F32) * gate * (1.0 + preact * (1.0 - gate))).astype(BF)
    grad_pre[...] = pre
    scaled = (inverse * pre.astype(F32)).astype(BF)
    for s in range(slots):
        back[s] = dot(scaled, hots[:, s * rows : (s + 1) * rows]).astype(BF)


def fill_combined(where, returned, weights, combined, basis_count):
    quarter, rows = returned.shape[1:]
    for j, slot in enumerate(where):
        lanes = slice(j * rows, (j + 1) * rows)
        grad = returned[slot].astype(F32)
        for b in range(basis_count):
            combined[b * quarter : (b + 1) * quarter, lanes] = (
                weights[b : b + 1, lanes] * grad
            ).astype(BF)


def bases_kernel(block_cap, owners, returned, gathered, weights, grad_pre, out, combined):
    quarter, rows = returned.shape[1:]
    edge_count = weights.shape[1]
    total = combined.shape[0]
    where = block_slots(owners, edge_count // rows, block_cap)
    fill_combined(where, returned, weights, combined, total // quarter)
    x = gathered[:, :edge_count]
    chunk = 5 * quarter
    for start in range(0, total, chunk):
        stop = min(start + chunk, total)
        out[start:stop, :] = dot(combined[start:stop, :], x, NT).astype(BF)
    own = gathered[:, edge_count:]
    out[total : total + quarter, :] = dot(grad_pre[...], own, NT).astype(BF)
    out[total + quarter :, :] = jnp.zeros((out.shape[0] - total - quarter, out.shape[1]), BF)


def edges_kernel(
    block_cap, owners, returned, gathered, weights, grad_pre, bases, bases_t, weight, rel, out, combined, scaled
):
    quarter, rows = returned.shape[1:]
    edge_count = weights.shape[1]
    entities = grad_pre.shape[1]
    total = combined.shape[0]
    basis_count = total // quarter
    padded = weights.shape[0]
    relations = 2 * LANES
    where = block_slots(owners, edge_count // rows, block_cap)
    fill_combined(where, returned, weights, combined, basis_count)
    peers = out.shape[0]
    share = out.shape[1]
    span = 2 * rows if (edge_count // rows) % 2 == 0 else rows
    scaled[...] = jnp.zeros_like(scaled)
    for t in range(edge_count // span):
        lanes = slice(t * span, (t + 1) * span)
        partial = dot(bases_t[...], combined[:, lanes]).astype(BF)
        for f in range(peers):
            out[f, :, lanes] = partial[f * share : (f + 1) * share]
        x = gathered[:, lanes]
        count = span // rows
        grad = [returned[where[t * count + k]].astype(F32) for k in range(count)]
        grad = grad[0] if count == 1 else jnp.concatenate(grad, axis=1)
        group = 5
        for c in range(0, basis_count, group):
            stop = min(c + group, basis_count)
            products = dot(bases[c * quarter : stop * quarter, :], x)
            for b in range(c, stop):
                part = products[(b - c) * quarter : (b - c + 1) * quarter]
                scaled[b : b + 1, lanes] = jnp.sum(part * grad, axis=0, keepdims=True)
    high = scaled[...].astype(BF)
    low = (scaled[...] - high.astype(F32)).astype(BF)
    chosen = rel_hot(rel[...], relations)
    coef = (dot(high, chosen, NT) + dot(low, chosen, NT)).astype(BF)
    own = dot(weight[...], grad_pre[...]).astype(BF)
    tail = edge_count + entities
    for f in range(peers):
        out[f, :, edge_count:tail] = own[f * share : (f + 1) * share]
        out[f, :padded, tail:] = coef[:, :LANES]
        out[f, padded : 2 * padded, tail:] = coef[:, LANES:]


def slots_kernel(padded, arrived, slot, out, own):
    peers, share, _ = arrived.shape
    dom_count, _, slot_cap = out.shape
    edge_count = slot.shape[1]
    entities = own.shape[1]
    sums = arrived[0].astype(F32)
    for f in range(1, peers):
        sums = sums + arrived[f].astype(F32)
    own[...] = sums[:, edge_count : edge_count + entities]
    edges = sums[:, :edge_count].astype(BF)
    coef = sums[: 2 * padded, edge_count + entities :].astype(BF)

    def step(p):
        near = slot[...] - p * slot_cap
        chosen = hot(iota((slot_cap, edge_count), 0) == near)
        out[p, :share, :] = dot(edges, chosen, NT).astype(BF)
        if slot_cap >= 2 * LANES:
            out[p, share:, :LANES] = coef[:padded]
            out[p, share:, LANES : 2 * LANES] = coef[padded:]
        else:
            out[p, share:, :] = coef

    each(dom_count, step)


def feats_kernel(slot_cap, padded, scale, arrived, asked, own, out, coef, total):
    dom_count, _, _ = arrived.shape
    share, entities = own.shape
    chunks = slot_cap // LANES
    total[...] = own[...]
    coef[...] = jnp.zeros_like(coef)

    def step(g):
        chosen = hot(iota((entities, slot_cap), 0) == asked_row(asked, g, chunks))
        total[...] += dot(arrived[g, :share, :], chosen, NT)
        if slot_cap >= 2 * LANES:
            coef[...] += arrived[g, share:, : 2 * LANES].astype(F32)
        else:
            coef[:, :LANES] += arrived[g, share : share + padded, :].astype(F32)
            coef[:, LANES:] += arrived[g, share + padded :, :].astype(F32)

    each(dom_count, step)
    out[...] = total[...].astype(BF)
    coef[...] = coef[...] * scale


def reduce_kernel(scale, parts, out):
    sums = parts[0].astype(F32)
    for k in range(1, parts.shape[0]):
        sums = sums + parts[k].astype(F32)
    out[...] = (sums * scale).astype(BF)


def body_many(
    feats,
    self_weight,
    bases,
    coef,
    src_part,
    src_row,
    edge_dst,
    edge_rel,
    block_owner,
    block_valid,
    cotangent,
):
    dom_count = lax.axis_size("dom")
    feat_count = lax.axis_size("feat")
    quarter, entities = feats.shape
    edge_count = src_row.shape[0]
    block_count = block_valid.shape[1]
    rows = edge_count // block_count
    slot_cap = LANES * ((2 * edge_count + LANES * dom_count - 1) // (LANES * dom_count))
    block_cap = (2 * block_count + dom_count - 1) // dom_count
    basis_count, _, model = bases.shape
    relation_count = coef.shape[0]
    flat = basis_count * quarter
    padded = 8 * ((basis_count + 7) // 8)
    padded = 16 * ((padded + 15) // 16)
    shape = jax.ShapeDtypeStruct
    scale = float(edge_count * dom_count) ** (-0.5)

    owners = block_owner[:, 0]
    valid = block_valid[0]
    rel = edge_rel.reshape(1, edge_count)
    bases_flat = bases.reshape(flat, model)
    coef_t = jnp.zeros((padded, 2 * LANES), F32).at[:basis_count, :relation_count].set(coef.T)

    height = slot_cap // LANES + block_cap
    send, slot = call(
        functools.partial(plan_kernel, entities, slot_cap, block_cap),
        (shape((dom_count, height, LANES), I32), shape((1, edge_count), I32)),
        smem=(0, 1),
        scratch=[pltpu.VMEM((slot_cap, edge_count), BF)],
        count=5,
    )(
        owners,
        valid,
        src_part.reshape(1, edge_count),
        src_row.reshape(1, edge_count),
        edge_dst.reshape(block_count, rows),
    )
    arrived = lax.all_to_all(send, "dom", split_axis=0, concat_axis=0, tiled=True)
    served = call(
        functools.partial(serve_kernel, slot_cap),
        shape((dom_count, quarter, slot_cap), BF),
        count=2,
    )(arrived, feats)
    fetched = lax.all_to_all(served, "dom", split_axis=0, concat_axis=0, tiled=True)
    mine = call(
        unslot_kernel,
        shape((quarter, edge_count + entities), BF),
        scratch=[pltpu.VMEM((quarter, edge_count), F32)],
        count=3,
    )(fetched, slot, feats)
    gathered = lax.all_gather(mine, "feat", axis=0, tiled=True)

    messages, weights = call(
        functools.partial(forward_kernel, block_cap),
        (shape((dom_count * block_cap, quarter, rows), BF), shape((padded, edge_count), F32)),
        smem=(0,),
        count=5,
    )(owners, gathered, bases_flat, coef_t, rel)
    received = lax.all_to_all(messages, "dom", split_axis=0, concat_axis=0, tiled=True)
    total_slots = dom_count * block_cap * rows
    output, back, grad_pre = call(
        functools.partial(owner_kernel, slot_cap, block_cap),
        (
            shape((quarter, entities), BF),
            shape((dom_count * block_cap, quarter, rows), BF),
            shape((quarter, entities), BF),
        ),
        scratch=[pltpu.VMEM((entities, total_slots), BF), pltpu.VMEM((quarter + 16, total_slots), BF)],
        count=5,
    )(arrived, received, gathered, self_weight, cotangent)
    returned = lax.all_to_all(back, "dom", split_axis=0, concat_axis=0, tiled=True)

    unit = 16 * dom_count
    tall = unit * ((flat + quarter + unit - 1) // unit)
    bases_part = call(
        functools.partial(bases_kernel, block_cap),
        shape((tall, model), BF),
        smem=(0,),
        scratch=[pltpu.VMEM((flat, edge_count), BF)],
        count=5,
    )(owners, returned, gathered, weights, grad_pre)
    parts = lax.all_to_all(
        bases_part.reshape(dom_count, tall // dom_count, model),
        "dom",
        split_axis=0,
        concat_axis=0,
        tiled=True,
    )
    edge_part = call(
        functools.partial(edges_kernel, block_cap),
        shape((feat_count, quarter, edge_count + entities + LANES), BF),
        smem=(0,),
        scratch=[pltpu.VMEM((flat, edge_count), BF), pltpu.VMEM((padded, edge_count), F32)],
        count=9,
    )(owners, returned, gathered, weights, grad_pre, bases_flat, bases_flat.T, self_weight, rel)
    edge_sum = lax.all_to_all(edge_part, "feat", split_axis=0, concat_axis=0, tiled=True)
    extra = padded * 2 * LANES // min(slot_cap, 2 * LANES)
    slot_grads, own_grads = call(
        functools.partial(slots_kernel, padded),
        (shape((dom_count, quarter + extra, slot_cap), BF), shape((quarter, entities), F32)),
        count=2,
    )(edge_sum, slot)
    arrived_grads = lax.all_to_all(slot_grads, "dom", split_axis=0, concat_axis=0, tiled=True)
    reduced = call(
        functools.partial(reduce_kernel, scale), shape((tall // dom_count, model), BF), count=1
    )(parts)
    near = [[2 * k, 2 * k + 1] for k in range(dom_count // 2)]
    far = [[2 * k + side for k in range(dom_count // 2)] for side in range(2)]
    pair = lax.all_gather(reduced, "dom", axis=0, tiled=True, axis_index_groups=near)
    whole = lax.all_gather(pair, "dom", axis=0, tiled=True, axis_index_groups=far)
    grad_feats, coef_total = call(
        functools.partial(feats_kernel, slot_cap, padded, scale),
        (shape((quarter, entities), BF), shape((padded, 2 * LANES), F32)),
        scratch=[pltpu.VMEM((quarter, entities), F32)],
        count=3,
    )(arrived_grads, arrived, own_grads)
    return (
        output,
        grad_feats,
        whole[:flat].astype(F32).reshape(basis_count, quarter, model),
        whole[flat : flat + quarter].astype(F32).T,
        coef_total[:basis_count, :relation_count].T,
    )


def pack_kernel(owners, valid, feats, part, row, dst, rel, out):
    copies = out.shape[0]
    quarter, entities = feats.shape
    blocks = part.shape[0]
    owner = jnp.zeros((blocks, LANES), I32)
    live = jnp.zeros((blocks, LANES), I32)
    for j in range(blocks):
        here = iota((blocks, LANES), 0) == j
        owner = jnp.where(here, owners[j], owner)
        live = jnp.where(here, valid[j], live)
    target = jnp.where(iota((blocks, LANES), 1) < live, dst[...], entities)
    digits = [
        part[...],
        row[...] >> 8,
        row[...] & 255,
        owner,
        target >> 8,
        target & 255,
        rel[...] >> 8,
        rel[...] & 255,
    ]
    digits = jnp.concatenate([d.astype(F32) for d in digits], axis=0).astype(BF)
    chunks = entities // LANES
    for k in range(copies):
        for c in range(chunks):
            out[k, c * quarter : (c + 1) * quarter, :] = feats[:, c * LANES : (c + 1) * LANES]
        out[k, chunks * quarter :, :] = digits


def source_kernel(
    shared, feats, part, row, mine, wide, ids, spans, targets, rels, owners, total, hots
):
    dom_count = shared.shape[0]
    quarter, entities = feats.shape
    blocks = part.shape[0]
    chunks = entities // LANES
    edge_count = blocks * LANES
    for g in range(dom_count):
        for c in range(chunks):
            start = g * entities + c * LANES
            wide[:, start : start + LANES] = shared[g, c * quarter : (c + 1) * quarter, :]
        digits = shared[g, chunks * quarter :, :].astype(F32).astype(I32)
        piece = [digits[d * blocks : (d + 1) * blocks] for d in range(8)]
        at = piece[0] * entities + piece[1] * 256 + piece[2]
        ids[g] = at
        for t in range(blocks // 2):
            spans[g * (blocks // 2) + t] = jnp.concatenate(
                [at[2 * t : 2 * t + 1], at[2 * t + 1 : 2 * t + 2]], axis=1
            )
        owners[g] = piece[3]
        targets[g] = piece[4] * 256 + piece[5]
        rels[g] = piece[6] * 256 + piece[7]
    total[...] = jnp.zeros_like(total)
    for p in range(dom_count):
        near = jnp.where(part[...] == p, row[...], -1)
        for j in range(blocks):
            hots[:, j * LANES : (j + 1) * LANES] = hot(
                iota((entities, LANES), 0) == near[j : j + 1, :]
            )
        total[...] += dot(wide[:, p * entities : (p + 1) * entities], hots[...])
    mine[:, :edge_count] = total[...].astype(BF)
    mine[:, edge_count:] = feats[...]


def split3(table):
    high = table.astype(BF)
    rest = table - high.astype(F32)
    middle = rest.astype(BF)
    low = (rest - middle.astype(F32)).astype(BF)
    return high, middle, low


def message_kernel(block_cap, entities, owners, valid, gathered, bases, coef, rel, dst, send):
    slots, tall, rows = send.shape
    blocks = rel.shape[0]
    quarter = tall - 8
    basis_count = bases.shape[0] // quarter
    group = 5
    first = iota((8, rows), 0)
    empty = jnp.where(first == 0, entities >> 8, jnp.where(first == 1, entities & 255, 0))
    empty = empty.astype(F32).astype(BF)
    for s in range(slots):
        send[s, :quarter, :] = jnp.zeros((quarter, rows), BF)
        send[s, quarter:, :] = empty
    parts = split3(coef[...])
    where = block_slots(owners, blocks, block_cap)
    for t in range(blocks // 2):
        lanes = slice(2 * t * rows, 2 * (t + 1) * rows)
        both = jnp.concatenate([rel[2 * t : 2 * t + 1, :], rel[2 * t + 1 : 2 * t + 2, :]], axis=1)
        chosen = rel_hot(both, coef.shape[1])
        mix = sum(dot(p, chosen) for p in parts)
        x = gathered[:, lanes]
        total = jnp.zeros((quarter, 2 * rows), F32)
        for c in range(0, basis_count, group):
            stop = min(c + group, basis_count)
            products = dot(bases[c * quarter : stop * quarter, :], x)
            for b in range(c, stop):
                part = products[(b - c) * quarter : (b - c + 1) * quarter]
                total = total + mix[b : b + 1, :] * part
        total = total.astype(BF)
        for k in range(2):
            j = 2 * t + k
            slot = where[j]
            live = iota((1, rows), 1) < valid[j]
            target = jnp.where(live, dst[j : j + 1, :], entities)
            code = jnp.where(first == 0, target >> 8, jnp.where(first == 1, target & 255, 0))
            send[slot, :quarter, :] = total[:, k * rows : (k + 1) * rows]
            send[slot, quarter:, :] = code.astype(F32).astype(BF)


def node_kernel(received, gathered, weight, cotangent, output, share, grad_pre, hots, flat):
    slots, _, rows = received.shape
    quarter, entities = cotangent.shape
    copies = share.shape[0]
    for s in range(slots):
        lanes = slice(s * rows, (s + 1) * rows)
        code = received[s, quarter:, :].astype(F32).astype(I32)
        target = code[0:1] * 256 + code[1:2]
        hots[:, lanes] = hot(iota((entities, rows), 0) == target)
        flat[:quarter, lanes] = received[s, :quarter, :]
    flat[quarter:, :] = jnp.ones((16, slots * rows), BF)
    own = gathered[:, gathered.shape[1] - entities :]
    own_part = dot(weight[...], own)
    sums = dot(hots[...], flat[...], NT).T
    count = sums[quarter : quarter + 1]
    inverse = 1.0 / jnp.maximum(count, 1.0)
    preact = own_part + inverse * sums[:quarter]
    gate = jax.nn.sigmoid(preact)
    output[...] = (preact * gate).astype(BF)
    pre = (cotangent[...].astype(F32) * gate * (1.0 + preact * (1.0 - gate))).astype(BF)
    grad_pre[...] = pre
    whole = count.astype(I32)
    first = iota((8, entities), 0)
    code = jnp.where(first == 0, whole >> 8, jnp.where(first == 1, whole & 255, 0))
    code = code.astype(F32).astype(BF)
    for k in range(copies):
        share[k, :quarter, :] = pre
        share[k, quarter:, :] = code


def scaled_grad(shared, q, quarter):
    code = shared[q, quarter:, :].astype(F32)
    count = code[0:1] * 256.0 + code[1:2]
    inverse = 1.0 / jnp.maximum(count, 1.0)
    return (inverse * shared[q, :quarter, :].astype(F32)).astype(BF)


def rows_of_edges_kernel(entities, place, spans, *refs):
    pieces, out, full = refs[:-2], refs[-2], refs[-1]
    count, width, model = out.shape
    quarter = pieces[0].shape[0]
    for k, piece in enumerate(pieces):
        full[pl.ds(pl.multiple_of(place[k] * quarter, quarter), quarter), :] = piece[...]

    def step(n, carry):
        row = spans[place[0] * count + n]
        total = jnp.zeros((model, width), F32)
        for start in range(0, full.shape[1], entities):
            chosen = hot(iota((entities, width), 0) == row - start)
            total = total + dot(full[:, start : start + entities], chosen)
        out[n] = total.T.astype(BF)
        return carry

    lax.fori_loop(0, count, step, 0)


def rank_kernel(
    slot_cap, entities, me, ids, rels, coef, ranks, slot_rows, slot_mix, mix, comp, digits, hots
):
    dom_count, blocks, _ = ids.shape
    before = hot(iota((LANES, LANES), 0) < iota((LANES, LANES), 1))
    ones = jnp.ones((LANES, LANES), BF)
    table = coef[...].astype(BF)

    def step(g, carry):
        near = ids[g] - me[0] * entities
        mask = (near >= 0) & (near < entities)
        chosen = jnp.where(mask, 1.0, 0.0)
        chosen = jnp.concatenate([chosen, jnp.zeros_like(chosen)], axis=0).astype(BF)
        inside = dot(chosen, before)[:blocks]
        totals = dot(chosen, ones)[:blocks]
        offset = jnp.zeros((1, LANES), F32)
        offsets = []
        for j in range(blocks):
            offsets.append(offset)
            offset = offset + totals[j : j + 1]
        rank = inside + jnp.concatenate(offsets, axis=0)
        rank = jnp.where(mask, rank.astype(I32), -1)
        ranks[g] = rank
        rel = rels[g]
        rows = jnp.where(mask, near, 0)
        first = iota((16, LANES), 0)
        for j in range(blocks):
            lanes = slice(j * LANES, (j + 1) * LANES)
            comp[:, lanes] = hot(iota((slot_cap, LANES), 0) == rank[j : j + 1, :])
            at, kind = rows[j : j + 1, :], rel[j : j + 1, :]
            code = jnp.where(first == 0, at >> 8, jnp.where(first == 1, at & 255, 0))
            code = code + jnp.where(first == 2, kind >> 8, jnp.where(first == 3, kind & 255, 0))
            digits[:, lanes] = code.astype(F32).astype(BF)
            hots[:, lanes] = rel_hot(kind, coef.shape[1])
        mix[g] = dot(table, hots[...])
        found = dot(digits[...], comp[...], NT)
        slot_rows[g] = (found[0:1] * 256.0 + found[1:2]).astype(I32)
        kind = (found[2:3] * 256.0 + found[3:4]).astype(I32)
        slot_mix[g] = dot(table, rel_hot(kind, coef.shape[1]))
        return carry

    lax.fori_loop(0, dom_count, step, 0)


def products_kernel(gathered, bases, bases_t, out):
    edge_count = out.shape[1]
    bases_t[...] = bases[...].T
    step = 320
    for start in range(0, out.shape[0], step):
        stop = min(start + step, out.shape[0])
        out[start:stop, :] = dot(bases[start:stop, :], gathered[:, :edge_count]).astype(BF)


def grads_kernel(
    owners,
    me,
    targets,
    ranks,
    shared,
    products_far,
    rel,
    grads,
    slot_grads,
    coef_out,
    node,
    comp,
    scaled,
    products,
    sems,
):
    fetched = fetch(((products_far, products),), sems)
    dom_count, blocks, _ = targets.shape
    slot_cap = comp.shape[2]
    entities = shared.shape[2]
    quarter = shared.shape[1] - 8
    copies, _, relations = coef_out.shape
    basis_count = products.shape[0] // quarter
    for q in range(dom_count):
        node[q] = scaled_grad(shared, q, quarter)
    for g in range(dom_count):
        rows = targets[g]
        rank = ranks[g].astype(F32).T.astype(I32)
        for j in range(0, blocks, 2):
            both = jnp.concatenate([rows[j : j + 1, :], rows[j + 1 : j + 2, :]], axis=1)
            chosen = hot(iota((entities, 2 * LANES), 0) == both)
            first, second = owners[g * blocks + j], owners[g * blocks + j + 1]
            pair = dot(jnp.concatenate([node[first], node[second]], axis=0), chosen).astype(BF)
            middle = (j + 1) * LANES
            grads[g, :, j * LANES : middle] = pair[:quarter, :LANES]
            grads[g, :, middle : middle + LANES] = pair[quarter:, LANES:]
        for j in range(blocks):
            lanes = slice(j * LANES, (j + 1) * LANES)
            comp[g % 2, lanes, :] = hot(iota((LANES, slot_cap), 1) == rank[:, j : j + 1])
        slot_grads[g] = dot(grads[g], comp[g % 2]).astype(BF)
    scaled[...] = jnp.zeros_like(scaled)
    fetched[0].wait()
    for t in range(blocks // 2):
        lanes = slice(2 * t * LANES, 2 * (t + 1) * LANES)
        grad = grads[me[0], :, lanes].astype(F32)
        for b in range(basis_count):
            part = products[b * quarter : (b + 1) * quarter, lanes].astype(F32)
            scaled[b : b + 1, lanes] = jnp.sum(part * grad, axis=0, keepdims=True)
    high = scaled[...].astype(BF)
    low = (scaled[...] - high.astype(F32)).astype(BF)
    kinds = jnp.concatenate([rel[j : j + 1, :] for j in range(blocks)], axis=1)
    chosen = rel_hot(kinds, relations)
    total = (dot(chosen, high, NT) + dot(chosen, low, NT)).T.astype(BF)
    for k in range(copies):
        coef_out[k] = total


def mix_rows(mix, grad, quarter):
    pieces = []
    for b in range(mix.shape[0]):
        wide = jnp.broadcast_to(mix[b : b + 1, :], (16, mix.shape[1])).astype(BF)
        for r in range(0, quarter, 16):
            pieces.append(wide * grad[r : r + 16])
    return jnp.concatenate(pieces, axis=0)


def column(row):
    return jnp.broadcast_to(row.astype(F32), (8, row.shape[1])).T[:, :1].astype(I32)


def scatter_kernel(
    slot_grads, slot_rows, slot_mix, bases_far, weight, grad_pre, out, total, bases_t, rows, sems
):
    copies = fetch(((bases_far, bases_t),), sems)
    dom_count, quarter, slot_cap = slot_grads.shape
    basis_count = bases_t.shape[1] // quarter
    entities = grad_pre.shape[1]
    peers = out.shape[0]
    total[...] = lax.dot_general(
        weight[...], grad_pre[...], (((0,), (0,)), ((), ())), preferred_element_type=F32
    )

    copies[0].wait()

    group = 4 if dom_count % 4 == 0 else 1
    for start in range(0, dom_count, group):
        part = range(start, start + group)
        mix = jnp.concatenate([slot_mix[g][:basis_count] for g in part], axis=1)
        grad = jnp.concatenate([slot_grads[g] for g in part], axis=1)
        partial = dot(bases_t[...], mix_rows(mix, grad, quarter)).astype(BF)
        for n, g in enumerate(part):
            chosen = hot(iota((slot_cap, entities), 1) == column(slot_rows[g]))
            rows[n * slot_cap : (n + 1) * slot_cap, :] = chosen
        total[...] += dot(partial, rows[: group * slot_cap, :])
    for f in range(peers):
        out[f] = total[f * quarter : (f + 1) * quarter].astype(BF)


def fetch(pairs, sems):
    copies = [
        pltpu.make_async_copy(source, target, sems.at[k]) for k, (source, target) in enumerate(pairs)
    ]
    for copy in copies:
        copy.start()
    return copies


def weights_kernel(scale, place, mix_far, grads_far, full_far, shared, *refs):
    rows, (out, own_out, total, mix, grads, full, sems, done) = refs[:-8], refs[-8:]
    dom_count, quarter, _ = grads.shape
    entities = shared.shape[2]
    basis_count = out.shape[0] // quarter
    group = 5
    count = rows[0].shape[0]
    order = [place[part] * count + k for part in range(len(rows)) for k in range(count)]
    pairs = []
    for n, g in enumerate(order):
        pairs += [(mix_far.at[g], mix.at[n]), (grads_far.at[g], grads.at[n])]
    copies = fetch(pairs + [(full_far, full)], sems)
    stores = []
    for n in range(dom_count):
        copies[2 * n].wait()
        copies[2 * n + 1].wait()
        grad = grads[n]
        for c in range(0, basis_count, group):
            stop = min(c + group, basis_count)
            lanes = slice(c * quarter, stop * quarter)
            sums = dot(mix_rows(mix[n, c:stop, :], grad, quarter), rows[n // count][n % count])
            if n > 0:
                sums = sums + total[lanes, :]
            if n == dom_count - 1:
                sums = sums * scale
            total[lanes, :] = sums
            if n == dom_count - 1:
                store = pltpu.make_async_copy(
                    total.at[lanes, :], out.at[lanes, :], done.at[c // group]
                )
                store.start()
                stores.append(store)
    copies[2 * dom_count].wait()
    own = jnp.zeros((full.shape[0], quarter), F32)
    for q in range(dom_count):
        lanes = slice(q * entities, (q + 1) * entities)
        own = own + dot(full[:, lanes], shared[q, :quarter, :], NT)
    own_out[...] = own.T * scale
    for store in stores:
        store.wait()


def merge_kernel(sums, coefs, out):
    peers, _, entities = sums.shape
    padded = coefs.shape[1]
    coef = coefs[0].astype(F32)
    for g in range(1, coefs.shape[0]):
        coef = coef + coefs[g].astype(F32)
    coef = coef.astype(BF)
    for f in range(peers):
        out[f, :, :entities] = sums[f]
        out[f, :padded, entities:] = coef[:, :LANES]
        out[f, padded:, entities:] = coef[:, LANES:]


def finish_kernel(padded, scale, arrived, grad_feats, coef_out):
    entities = grad_feats.shape[1]
    sums = arrived[0].astype(F32)
    for f in range(1, arrived.shape[0]):
        sums = sums + arrived[f].astype(F32)
    grad_feats[...] = sums[:, :entities].astype(BF)
    coef = jnp.concatenate([sums[:padded, entities:], sums[padded:, entities:]], axis=1)
    coef_out[...] = coef[: coef_out.shape[0], : coef_out.shape[1]] * scale


def body_few(
    feats,
    self_weight,
    bases,
    coef,
    src_part,
    src_row,
    edge_dst,
    edge_rel,
    block_owner,
    block_valid,
    cotangent,
):
    dom_count = lax.axis_size("dom")
    feat_count = lax.axis_size("feat")
    quarter, entities = feats.shape
    edge_count = src_row.shape[0]
    blocks = block_valid.shape[1]
    slot_cap = LANES * ((2 * edge_count + LANES * dom_count - 1) // (LANES * dom_count))
    block_cap = (2 * blocks + dom_count - 1) // dom_count
    basis_count, _, model = bases.shape
    relation_count = coef.shape[0]
    flat = basis_count * quarter
    padded = 16 * ((basis_count + 15) // 16)
    relations = 2 * LANES
    shape = jax.ShapeDtypeStruct
    scale = float(edge_count * dom_count) ** (-0.5)
    owners = block_owner[:, 0]
    valid = block_valid[0]
    part = src_part.reshape(blocks, LANES)
    row = src_row.reshape(blocks, LANES)
    dst = edge_dst.reshape(blocks, LANES)
    rel = edge_rel.reshape(blocks, LANES)
    bases_flat = bases.reshape(flat, model)
    weight_t = self_weight.T
    coef_t = jnp.zeros((padded, relations), F32).at[:basis_count, :relation_count].set(coef.T)
    dom_place = lax.axis_index("dom").astype(I32).reshape(1)
    feat_place = lax.axis_index("feat").astype(I32)

    tall = (entities // LANES) * quarter + 8 * blocks
    packed = call(
        pack_kernel,
        shape((1, tall, LANES), BF),
        smem=(0, 1),
        count=7,
        us=1,
        far=(0, 1, 2, 3, 4, 5, 6),
    )(
        owners, valid, feats, part, row, dst, rel
    )
    near = [[2 * k, 2 * k + 1] for k in range(dom_count // 2)]
    far = [[2 * k + side for k in range(dom_count // 2)] for side in range(2)]
    shared = lax.all_gather(packed, "dom", axis=0, tiled=True, axis_index_groups=near)
    shared = lax.all_gather(shared, "dom", axis=0, tiled=True, axis_index_groups=far)
    ints = shape((dom_count, blocks, LANES), I32)
    mine, wide, ids, spans, targets, rels, all_owners = call(
        source_kernel,
        (
            shape((quarter, edge_count + entities), BF),
            shape((quarter, dom_count * entities), BF),
            ints,
            shape((dom_count * blocks // 2, 1, 2 * LANES), I32),
            ints,
            ints,
            ints,
        ),
        scratch=[pltpu.VMEM((quarter, edge_count), F32), pltpu.VMEM((entities, edge_count), BF)],
        count=4,
        us=4,
        far_out=(3, 4, 6),
    )(shared, feats, part, row)
    gathered = lax.all_gather(mine, "feat", axis=0, tiled=True)
    owner_list = all_owners[:, :, 0].reshape(dom_count * blocks)

    def doubled(piece):
        pieces, bit, stage = [piece], feat_count // 2, 0
        while bit >= 1:
            links = [(f, f ^ bit) for f in range(feat_count)]
            pieces = pieces + [lax.ppermute(piece, "feat", links) for piece in pieces]
            bit //= 2
            stage += 1
        return pieces

    places, bit = [0], feat_count // 2
    while bit >= 1:
        places = places + [place ^ bit for place in places]
        bit //= 2
    place = jnp.stack([feat_place ^ k for k in places])
    wide, gathered = lax.optimization_barrier((wide, gathered))
    part_count = dom_count // feat_count
    rows, full = call(
        functools.partial(rows_of_edges_kernel, entities),
        (
            shape((part_count * blocks // 2, 2 * LANES, model), BF),
            shape((model, dom_count * entities), BF),
        ),
        smem=(0,),
        count=2 + feat_count,
        us=10,
        far=tuple(range(2 + feat_count)),
        far_out=(1,),
    )(place, spans, *doubled(wide))
    rows = doubled(rows.reshape(part_count, edge_count, model))
    ranks, slot_rows, slot_mix, mix = call(
        functools.partial(rank_kernel, slot_cap, entities),
        (
            ints,
            shape((dom_count, 1, slot_cap), I32),
            shape((dom_count, padded, slot_cap), F32),
            shape((dom_count, padded, edge_count), F32),
        ),
        smem=(0,),
        scratch=[
            pltpu.VMEM((slot_cap, edge_count), BF),
            pltpu.VMEM((16, edge_count), BF),
            pltpu.VMEM((relations, edge_count), BF),
        ],
        count=4,
        us=4,
        far=(0,),
        far_out=(0, 1, 2, 3),
    )(dom_place, ids, rels, coef_t)

    messages = call(
        functools.partial(message_kernel, block_cap, entities),
        shape((dom_count * block_cap, quarter + 8, LANES), BF),
        smem=(0, 1),
        count=7,
        us=4,
        far=(0, 1),
    )(owners, valid, gathered, bases_flat, coef_t, rel, dst)
    received = lax.all_to_all(messages, "dom", split_axis=0, concat_axis=0, tiled=True)
    slots = dom_count * block_cap
    output, share, grad_pre = call(
        node_kernel,
        (
            shape((quarter, entities), BF),
            shape((dom_count, quarter + 8, entities), BF),
            shape((quarter, entities), BF),
        ),
        scratch=[
            pltpu.VMEM((entities, slots * LANES), BF),
            pltpu.VMEM((quarter + 16, slots * LANES), BF),
        ],
        count=4,
        us=4,
        far_out=(2,),
    )(received, gathered, weight_t, cotangent)
    nodes = lax.all_to_all(share, "dom", split_axis=0, concat_axis=0, tiled=True)

    bases_t, products = call(
        products_kernel,
        (shape((model, flat), BF), shape((flat, edge_count), BF)),
        count=2,
        us=4,
        far_out=(0, 1),
    )(gathered, bases_flat)
    grads, slot_grads, coef_part = call(
        grads_kernel,
        (
            shape((dom_count, quarter, edge_count), BF),
            shape((dom_count, quarter, slot_cap), BF),
            shape((dom_count, padded, relations), BF),
        ),
        smem=(0, 1),
        scratch=[
            pltpu.VMEM((dom_count, quarter, entities), BF),
            pltpu.VMEM((2, edge_count, slot_cap), BF),
            pltpu.VMEM((padded, edge_count), F32),
            pltpu.VMEM((flat, edge_count), BF),
            pltpu.SemaphoreType.DMA((1,)),
        ],
        count=7,
        us=8,
        far=(0, 1, 2, 3),
        far_out=(0,),
        raw=(5,),
    )(owner_list, dom_place, targets, ranks, nodes, products, rel)
    coefs = lax.all_to_all(
        coef_part, "dom", split_axis=0, concat_axis=0, tiled=True
    )
    sums = call(
        scatter_kernel,
        shape((feat_count, quarter, entities), BF),
        scratch=[
            pltpu.VMEM((model, entities), F32),
            pltpu.VMEM((model, flat), BF),
            pltpu.VMEM((4 * slot_cap, entities), BF),
            pltpu.SemaphoreType.DMA((1,)),
        ],
        raw=(3,),
        far=(1, 2, 5),
        count=6,
        us=5,
    )(slot_grads, slot_rows, slot_mix, bases_t, weight_t, grad_pre)
    sent = call(
        merge_kernel, shape((feat_count, quarter, entities + LANES), BF), count=2, us=1
    )(sums, coefs)
    arrived = lax.all_to_all(sent, "feat", split_axis=0, concat_axis=0, tiled=True)
    grad_bases, grad_self = call(
        functools.partial(weights_kernel, scale),
        (shape((flat, model), F32), shape((quarter, model), F32)),
        smem=(0,),
        count=5 + feat_count,
        us=12,
        far=(0,),
        raw=(1, 2, 3),
        raw_out=(0,),
        scratch=[
            pltpu.VMEM((flat, model), F32),
            pltpu.VMEM((dom_count, padded, edge_count), F32),
            pltpu.VMEM((dom_count, quarter, edge_count), BF),
            pltpu.VMEM((model, dom_count * entities), BF),
            pltpu.SemaphoreType.DMA((2 * dom_count + 1,)),
            pltpu.SemaphoreType.DMA((basis_count,)),
        ],
    )(place, mix, grads, full, nodes, *rows)
    grad_feats, coef_total = call(
        functools.partial(finish_kernel, padded, scale),
        (shape((quarter, entities), BF), shape((basis_count, relation_count), F32)),
        count=1,
        us=1,
    )(arrived)
    return (
        output,
        grad_feats,
        grad_bases.reshape(basis_count, quarter, model),
        grad_self.T,
        coef_total.T,
    )


def solution(mesh):
    def body(*arrays):
        dom_count = lax.axis_size("dom")
        edge_count = arrays[5].shape[0]
        feat_count = lax.axis_size("feat")
        few = dom_count * edge_count <= 1 << 14 and dom_count % feat_count == 0
        if not few:
            return body_many(*arrays)
        return body_few(*arrays)

    return jax.shard_map(
        body,
        mesh=mesh,
        in_specs=(
            P("feat", "dom"),
            P(None, "feat"),
            P(None, "feat", None),
            P(),
            P("dom", None),
            P("dom"),
            P("dom"),
            P("dom"),
            P("dom", None),
            P("dom", None),
            P("feat", "dom"),
        ),
        out_specs=(P("feat", "dom"), P("feat", "dom"), P(None, "feat", None), P(None, "feat"), P()),
        check_vma=False,
    )
```
